16 devices in a mesh: w: 4 (over z, y), h: 4 (over x, core).
Axes of the slice: x: 2, y: 2, z: 2, core: 2. Of those that a mesh axis runs over, the one named last changes fastest.
Arguments:
- image: bfloat16 [1, 96, 192, 640], P(None, 'h', 'w')
- w_first: bfloat16 [3, 3, 640, 640], replicated
- w_down: bfloat16 [3, 3, 640, 640], replicated
- grad_out: bfloat16 [1, 48, 96, 640], P(None, 'h', 'w')
Outputs:
- output 1: bfloat16 [1, 48, 96, 640], P(None, 'h', 'w')
- output 2: bfloat16 [1, 96, 192, 640], P(None, 'h', 'w')
- output 3: float32 [3, 3, 640, 640], replicated
- output 4: float32 [3, 3, 640, 640], replicated
All inputs are finite; a program needn't handle non-finite values.
Results may differ from the reference program's by a relative error of at most 0.0115483.
Values are sent between devices in bfloat16 or wider.
A program may use at most 1 GiB of HBM per device.

```python
import jax
import jax.numpy as jnp
from jax import lax

NUM_IMAGES = 1
HEIGHT = 96
WIDTH = 192
CHANNELS = 640

CONV_DIMS = ('NHWC', 'HWIO', 'NHWC')


def gelu_tanh(values):
    return jax.nn.gelu(values, approximate=True)


def conv_first(lhs_in, kernel):
    return lax.conv_general_dilated(lhs_in, kernel, (1, 1), ((1, 1), (1, 1)), dimension_numbers=CONV_DIMS, precision=lax.Precision.HIGHEST)


def conv_down(lhs_in, kernel):
    return lax.conv_general_dilated(lhs_in, kernel, (2, 2), ((0, 1), (0, 1)), dimension_numbers=CONV_DIMS, precision=lax.Precision.HIGHEST)


def setup_inputs(seed: int = 0) -> dict:
    root_key = jax.random.key(seed)
    key_image, key_first, key_down, key_grad = jax.random.split(root_key, 4)
    w_scale = (9 * CHANNELS) ** -0.5
    image = jax.random.normal(key_image, (NUM_IMAGES, HEIGHT, WIDTH, CHANNELS), jnp.float32)
    w_first = jax.random.normal(key_first, (3, 3, CHANNELS, CHANNELS), jnp.float32) * w_scale
    w_down = jax.random.normal(key_down, (3, 3, CHANNELS, CHANNELS), jnp.float32) * w_scale
    grad_out = jax.random.normal(key_grad, (NUM_IMAGES, HEIGHT // 2, WIDTH // 2, CHANNELS), jnp.float32)
    return {'image': image.astype(jnp.bfloat16), 'w_first': w_first.astype(jnp.bfloat16), 'w_down': w_down.astype(jnp.bfloat16), 'grad_out': grad_out.astype(jnp.bfloat16)}


def reference(image, w_first, w_down, grad_out):
    pre_full, first_vjp = jax.vjp(conv_first, image.astype(jnp.float32), w_first.astype(jnp.float32))
    pre_act = pre_full.astype(jnp.bfloat16)
    pre_f32 = pre_act.astype(jnp.float32)
    gelu_out, gelu_vjp = jax.vjp(gelu_tanh, pre_f32)
    hidden = gelu_out.astype(jnp.bfloat16)
    out_full, down_vjp = jax.vjp(conv_down, hidden.astype(jnp.float32), w_down.astype(jnp.float32))
    block_out = out_full.astype(jnp.bfloat16)
    grad_hidden, grad_w_down = down_vjp(grad_out.astype(jnp.float32))
    grad_pre = gelu_vjp(grad_hidden)[0].astype(jnp.bfloat16)
    grad_full, grad_w_first = first_vjp(grad_pre.astype(jnp.float32))
    return block_out, grad_full.astype(jnp.bfloat16), grad_w_first, grad_w_down
```

```python
import jax
import jax.numpy as jnp
from jax import lax
from jax.sharding import PartitionSpec as P
from jax.experimental import pallas as pl
from jax.experimental.pallas import tpu as pltpu

MESH = pl.DeviceIdType.MESH
F32, BF16 = jnp.float32, jnp.bfloat16
C = 640
ROWS, COLS = 24, 48
OUT_R, OUT_C = 12, 24
PIX, OPIX = ROWS * COLS, OUT_R * OUT_C
HALF = 320
MIB = 2 ** 20
ORDERS = (('x', 'y', 'z'), ('y', 'z', 'x'), ('z', 'x', 'y'))
R1, R2, R3, A1, A2, A3A, A3B, DA, DB, DC, LA, LB, LC = range(13)


def gelu_tanh(values):
    return jax.nn.gelu(values, approximate=True)


def dot(lhs, rhs):
    return lax.dot_general(lhs, rhs, (((1,), (0,)), ((), ())), preferred_element_type=F32)


def dot_rhs_t(lhs, rhs):
    return lax.dot_general(lhs, rhs, (((1,), (1,)), ((), ())), preferred_element_type=F32)


def dot_lhs_t(lhs, rhs):
    return lax.dot_general(lhs, rhs, (((0,), (0,)), ((), ())), preferred_element_type=F32)


VM = pl.BlockSpec(memory_space=pltpu.VMEM)
ANY = pl.BlockSpec(memory_space=pl.ANY)


def shift_columns(ext_ref, out_ref):
    def one_row(r, _):
        for c in range(3):
            out_ref[c, pl.ds(pl.multiple_of(r * COLS, COLS), COLS), :] = ext_ref[r, c:c + COLS, :]
        return 0
    lax.fori_loop(0, ROWS + 2, one_row, 0)


def conv_first_kernel(ext_ref, w_ref, a_ref, z_ref, cat, sa, sz):
    step = pl.program_id(0)

    @pl.when(step == 0)
    def _():
        def one_row(r, _):
            for c in range(3):
                cat[pl.ds(pl.multiple_of(r * COLS, COLS), COLS), c * C:(c + 1) * C] = ext_ref[r, c:c + COLS, :]
            return 0
        lax.fori_loop(0, ROWS + 2, one_row, 0)

    block = 8 * COLS
    acc = None
    for a in range(3):
        rows = pl.ds(pl.multiple_of(step * block + a * COLS, COLS), block)
        part = dot(cat[rows, :], w_ref[a])
        acc = part if acc is None else acc + part
    pre = acc.astype(BF16).astype(F32)
    act = gelu_tanh(pre).astype(BF16).astype(F32)
    for lane in range(5):
        sa[lane] = pre[:, lane * 128:(lane + 1) * 128]
        sz[lane] = act[:, lane * 128:(lane + 1) * 128]
    for r in range(8):
        for cp in range(2):
            for lane in range(5):
                rows, lanes = pl.ds(r * COLS + cp, OUT_C, stride=2), pl.ds(lane * 128, 128)
                a_ref[r % 2, cp, r // 2, :, lanes] = sa[lane, rows, :]
                z_ref[r % 2, cp, r // 2, :, lanes] = sz[lane, rows, :]


def conv_first(image_ext, w_first):
    shape = jax.ShapeDtypeStruct((2, 2, OUT_R, OUT_C, C), F32)
    spec = pl.BlockSpec((2, 2, 4, OUT_C, C), lambda i: (0, 0, i, 0, 0))
    return pl.pallas_call(
        conv_first_kernel, grid=(3,), out_shape=[shape, shape],
        in_specs=[pl.BlockSpec(image_ext.shape, lambda i: (0, 0, 0)), pl.BlockSpec((3, 3 * C, C), lambda i: (0, 0, 0))],
        out_specs=[spec, spec],
        scratch_shapes=[pltpu.VMEM(((ROWS + 2) * COLS, 3 * C), BF16), pltpu.VMEM((5, 8 * COLS, 128), F32), pltpu.VMEM((5, 8 * COLS, 128), F32)],
        compiler_params=pltpu.CompilerParams(vmem_limit_bytes=56 * MIB),
        cost_estimate=pl.CostEstimate(flops=2 * PIX * 9 * C * C, bytes_accessed=16 * MIB, transcendentals=PIX * C),
    )(image_ext, w_first.reshape(3, 3 * C, C))


def weight_down_kernel(z_ref, zp_ref, g_ref, gp_ref, out_ref, taps, gs):
    core = lax.axis_index('h') % 2
    for src, (zr, gr) in enumerate(((z_ref, g_ref), (zp_ref, gp_ref))):
        gs[src * OPIX:(src + 1) * OPIX, :] = gr[1:, 1:, :].reshape(OPIX, C).astype(BF16)
        for t in range(9):
            a, c = t // 3, t % 3
            tap = zr[a % 2, c % 2, a // 2:a // 2 + OUT_R, c // 2:c // 2 + OUT_C, :]
            taps[t, src * OPIX:(src + 1) * OPIX, :] = tap.reshape(OPIX, C).astype(BF16)

    def one(j, _):
        res = dot_lhs_t(taps[4 * core + j], gs[...])
        out_ref[2 * j] = res[:HALF]
        out_ref[2 * j + 1] = res[HALF:]
        return 0
    lax.fori_loop(0, 5, one, 0)


def weight_down(z_own, z_pair, g_own, g_pair):
    return pl.pallas_call(
        weight_down_kernel, out_shape=jax.ShapeDtypeStruct((10, HALF, C), F32), in_specs=[VM] * 4, out_specs=VM,
        scratch_shapes=[pltpu.VMEM((9, 2 * OPIX, C), BF16), pltpu.VMEM((2 * OPIX, C), BF16)],
        compiler_params=pltpu.CompilerParams(vmem_limit_bytes=56 * MIB),
        cost_estimate=pl.CostEstimate(flops=2 * OPIX * 9 * C * C, bytes_accessed=16 * MIB, transcendentals=0),
    )(z_own, z_pair, g_own, g_pair)


def conv_down_kernel(z_ref, w_ref, y_ref, acc):
    for t in range(9):
        a, c = t // 3, t % 3
        tap = z_ref[a % 2, c % 2, a // 2:a // 2 + OUT_R, c // 2:c // 2 + OUT_C, :].reshape(OPIX, C).astype(BF16)
        part = dot(tap, w_ref[t])
        acc[...] = part if t == 0 else acc[...] + part
    y_ref[...] = acc[...].astype(BF16)


def conv_down(z_own, w_down):
    return pl.pallas_call(
        conv_down_kernel, out_shape=jax.ShapeDtypeStruct((OPIX, C), BF16), in_specs=[VM] * 2, out_specs=VM,
        scratch_shapes=[pltpu.VMEM((OPIX, C), F32)],
        compiler_params=pltpu.CompilerParams(vmem_limit_bytes=56 * MIB),
        cost_estimate=pl.CostEstimate(flops=2 * OPIX * 9 * C * C, bytes_accessed=12 * MIB, transcendentals=0),
    )(z_own, w_down)


def grad_pre_kernel(g_ref, a_ref, w_ref, out_ref, gs, sd):
    for di in range(2):
        for dj in range(2):
            gs[di, dj] = g_ref[di:di + OUT_R, dj:dj + OUT_C, :].reshape(OPIX, C).astype(BF16)
    for rp in range(2):
        for cp in range(2):
            acc = None
            for a in ((0, 2), (1,))[rp]:
                for c in ((0, 2), (1,))[cp]:
                    part = dot_rhs_t(gs[1 - a // 2, 1 - c // 2], w_ref[3 * a + c])
                    acc = part if acc is None else acc + part
            pre = a_ref[rp, cp].reshape(OPIX, C)
            grad = jax.vjp(gelu_tanh, pre)[1](acc)[0].astype(BF16).astype(F32)
            for i in range(OUT_R):
                for lane in range(5):
                    rows = pl.ds((2 * i + rp) * COLS + cp, OUT_C, stride=2)
                    sd[lane, rows, :] = grad[i * OUT_C:(i + 1) * OUT_C, lane * 128:(lane + 1) * 128]
    for lane in range(5):
        out_ref[:, lane * 128:(lane + 1) * 128] = sd[lane].astype(BF16)


def grad_pre_call(g_ext, a_own, w_down):
    return pl.pallas_call(
        grad_pre_kernel, out_shape=jax.ShapeDtypeStruct((PIX, C), BF16), in_specs=[VM] * 3, out_specs=VM,
        scratch_shapes=[pltpu.VMEM((2, 2, OPIX, C), BF16), pltpu.VMEM((5, PIX, 128), F32)],
        compiler_params=pltpu.CompilerParams(vmem_limit_bytes=56 * MIB),
        cost_estimate=pl.CostEstimate(flops=2 * OPIX * 9 * C * C, bytes_accessed=12 * MIB, transcendentals=PIX * C),
    )(g_ext, a_own, w_down)


def weight_first_kernel(x_ref, xp_ref, d_ref, dp_ref, out_ref, xs):
    core = lax.axis_index('h') % 2
    for src, ref in enumerate((x_ref, xp_ref)):
        shift_columns(ref, xs.at[src])

    def one(j, _):
        t = 4 * core + j
        a, c = t // 3, t % 3
        rows = pl.ds(pl.multiple_of(a * COLS, COLS), PIX)
        res = dot_lhs_t(xs[0, c, rows, :], d_ref[...]) + dot_lhs_t(xs[1, c, rows, :], dp_ref[...])
        out_ref[2 * j] = res[:HALF]
        out_ref[2 * j + 1] = res[HALF:]
        return 0
    lax.fori_loop(0, 5, one, 0)


def weight_first(x_own, x_pair, d_own, d_pair):
    return pl.pallas_call(
        weight_first_kernel, out_shape=jax.ShapeDtypeStruct((10, HALF, C), F32), in_specs=[VM] * 4, out_specs=VM,
        scratch_shapes=[pltpu.VMEM((2, 3, (ROWS + 2) * COLS, C), BF16)],
        compiler_params=pltpu.CompilerParams(vmem_limit_bytes=56 * MIB),
        cost_estimate=pl.CostEstimate(flops=2 * PIX * 9 * C * C, bytes_accessed=16 * MIB, transcendentals=0),
    )(x_own, x_pair, d_own, d_pair)


def grad_image_kernel(d_ref, w_ref, out_ref, ds, acc):
    shift_columns(d_ref, ds)
    block = 8 * COLS

    def one(i, _):
        for t in range(9):
            a, c = t // 3, t % 3
            rows = pl.ds(pl.multiple_of(i * block + (2 - a) * COLS, COLS), block)
            part = dot_rhs_t(ds[2 - c, rows, :], w_ref[t])
            acc[...] = part if t == 0 else acc[...] + part
        out_ref[pl.ds(pl.multiple_of(i * block, block), block), :] = acc[...].astype(BF16)
        return 0
    lax.fori_loop(0, 3, one, 0)


def grad_image_call(d_ext, w_first):
    return pl.pallas_call(
        grad_image_kernel, out_shape=jax.ShapeDtypeStruct((PIX, C), BF16), in_specs=[VM] * 2, out_specs=VM,
        scratch_shapes=[pltpu.VMEM((3, (ROWS + 2) * COLS, C), BF16), pltpu.VMEM((8 * COLS, C), F32)],
        compiler_params=pltpu.CompilerParams(vmem_limit_bytes=56 * MIB),
        cost_estimate=pl.CostEstimate(flops=2 * PIX * 9 * C * C, bytes_accessed=16 * MIB, transcendentals=0),
    )(d_ext, w_first)


def place():
    w, h = lax.axis_index('w'), lax.axis_index('h')
    bit = {'x': h // 2, 'c': h % 2, 'y': w % 2, 'z': w // 2}
    dev = {'x': (w, (h + 2) % 4), 'c': (w, h + 1 - 2 * (h % 2)), 'y': (w + 1 - 2 * (w % 2), h), 'z': ((w + 2) % 4, h)}
    return bit, dev


class Reducer:
    def __init__(self, index, own, land, out, sems, grants, bit, dev):
        self.index, self.own, self.land, self.out, self.sems, self.grants, self.bit, self.dev = index, own, land, out, sems, grants, bit, dev

    def starts(self, third):
        b = [self.bit[axis] for axis in ORDERS[third]]
        base2 = b[0] * 160
        base3 = base2 + b[1] * 80
        return b, base2, base3, base3 + b[2] * 40

    def copy(self, third, kind):
        b, base2, base3, base4 = self.starts(third)
        core = self.bit['c']
        far = (1 - b[0]) * 160
        src, size, axis = {
            R1: (far, 160, 0), R2: (base2 + (1 - b[1]) * 80, 80, 1), R3: (base3 + (1 - b[2]) * 40, 40, 2),
            A1: (base4, 40, 2), A2: (base3, 80, 1), A3A: (base3, 80, 0), A3B: (base2 + (1 - b[1]) * 80, 80, 0),
            DA: (base2, 160, 'c'), DB: (far + b[1] * 80, 80, 'c'), DC: (far + (1 - b[1]) * 80, 80, 'c'),
            LA: (base2, 160, None), LB: (far + b[1] * 80, 80, None), LC: (far + (1 - b[1]) * 80, 80, None),
        }[kind]
        rows = pl.ds(pl.multiple_of(src, 8), size)
        source = self.own.at[pl.ds(core + 3 * third, 3), rows]
        send, recv = (s.at[self.index, third, kind] for s in self.sems)
        if kind <= R3:
            target = self.land.at[pl.ds(3 * third, 3), pl.ds((0, 160, 240)[kind], size)]
        elif kind <= A3B:
            target = source
        else:
            target = self.out.at[pl.ds(9 * core + 3 * third, 3), rows]
        if axis is None:
            return pltpu.make_async_copy(source, target, recv)
        peer = self.dev[axis if axis == 'c' else ORDERS[third][axis]]
        return pltpu.make_async_remote_copy(src_ref=source, dst_ref=target, send_sem=send, recv_sem=recv, device_id=peer, device_id_type=MESH)

    def add(self, third, kind):
        _, base2, base3, base4 = self.starts(third)
        keep, size = ((base2, 160), (base3, 80), (base4, 40))[kind]
        land_at = (0, 160, 240)[kind]
        steps = size // 40

        def body(j, _):
            unit, row = 3 * third + j // steps, (j % steps) * 40
            rows = pl.ds(pl.multiple_of(keep + row, 8), 40)
            where = self.bit['c'] + unit
            self.own[where, rows, :] += self.land[unit, pl.ds(pl.multiple_of(land_at + row, 8), 40), :]
            return 0
        lax.fori_loop(0, 3 * steps, body, 0)

    def begin(self):
        for third in range(3):
            self.copy(third, R1).start()

    def move(self, wait_for, then, add=False):
        for third in range(3):
            self.copy(third, wait_for).wait()
            if add:
                pl.semaphore_signal(self.grants.at[self.index, third, wait_for], inc=1, device_id=self.dev[ORDERS[third][wait_for]], device_id_type=MESH)
                self.add(third, wait_for)
            for kind in then:
                if kind in (A1, A2, A3A):
                    pl.semaphore_wait(self.grants.at[self.index, third, {A1: R3, A2: R2, A3A: R1}[kind]], 1)
                self.copy(third, kind).start()

    def finish(self):
        for kind in (DA, DB, DC, LA, LB, LC):
            self.move(kind, ())


def reduce_kernel(p_down, p_first, o_down, o_first, own_d, own_f, land_d, land_f, local_sems, send_sems, recv_sems, grants):
    bit, dev = place()
    loads = [pltpu.make_async_copy(p, o, local_sems.at[i]) for i, (p, o) in enumerate(((p_down, own_d), (p_first, own_f)))]
    for load in loads:
        load.start()
    barrier = pltpu.get_barrier_semaphore()
    for axis in 'xyzc':
        pl.semaphore_signal(barrier, inc=1, device_id=dev[axis], device_id_type=MESH)
    pl.semaphore_wait(barrier, 4)
    sems = (send_sems, recv_sems)
    both = [Reducer(0, own_d, land_d, o_down, sems, grants, bit, dev), Reducer(1, own_f, land_f, o_first, sems, grants, bit, dev)]
    for load, one in zip(loads, both):
        load.wait()
        one.begin()
    for kind in (R1, R2, R3):
        for one in both:
            one.move(kind, (kind + 1,), add=True)
    for one in both:
        one.move(A1, (A2, A3A))
    for one in both:
        one.move(A2, (A3B, DA, LA))
    for one in both:
        one.move(A3A, (DB, LB))
    for one in both:
        one.move(A3B, (DC, LC))
    for one in both:
        one.finish()


def reduce_all(p_down, p_first):
    shape = jax.ShapeDtypeStruct((18, HALF, C), F32)
    return pl.pallas_call(
        reduce_kernel, out_shape=[shape, shape], in_specs=[ANY] * 2, out_specs=[ANY] * 2,
        scratch_shapes=[pltpu.VMEM((10, HALF, C), F32)] * 2 + [pltpu.VMEM((9, 280, C), F32)] * 2
        + [pltpu.SemaphoreType.DMA((2,)), pltpu.SemaphoreType.DMA((2, 3, 13)), pltpu.SemaphoreType.DMA((2, 3, 13)), pltpu.SemaphoreType.REGULAR((2, 3, 3))],
        compiler_params=pltpu.CompilerParams(collective_id=1, has_side_effects=True, vmem_limit_bytes=56 * MIB),
        cost_estimate=pl.CostEstimate(flops=2 * PIX * 90 * C * C, bytes_accessed=64 * MIB, transcendentals=0),
    )(p_down, p_first)


def settle_kernel(in_a, in_b, out_a, out_b, buf, load_sems, store_sems):
    loads, stores = [], []
    for i, (src, dst) in enumerate(((in_a, out_a), (in_b, out_b))):
        for part in range(9):
            span = pl.ds(2 * part, 2)
            loads.append(pltpu.make_async_copy(src.at[span], buf.at[i, span], load_sems.at[i, part]))
            stores.append(pltpu.make_async_copy(buf.at[i, span], dst.at[span], store_sems.at[i, part]))
    for load in loads:
        load.start()
    for load, store in zip(loads, stores):
        load.wait()
        store.start()
    for store in stores:
        store.wait()


def settle(sum_a, sum_b):
    shape = jax.ShapeDtypeStruct((18, HALF, C), F32)
    return pl.pallas_call(
        settle_kernel, out_shape=[shape, shape], in_specs=[ANY] * 2, out_specs=[ANY] * 2,
        scratch_shapes=[pltpu.VMEM((2, 18, HALF, C), F32), pltpu.SemaphoreType.DMA((2, 9)), pltpu.SemaphoreType.DMA((2, 9))],
        compiler_params=pltpu.CompilerParams(vmem_limit_bytes=56 * MIB),
    )(sum_a, sum_b)


def solution(mesh):
    axis_len = {'h': mesh.shape['h'], 'w': mesh.shape['w']}

    def from_prev(edge, axis):
        return lax.ppermute(edge, axis, [(i, i + 1) for i in range(axis_len[axis] - 1)])

    def from_next(edge, axis):
        return lax.ppermute(edge, axis, [(i + 1, i) for i in range(axis_len[axis] - 1)])

    def swap_core(value):
        return lax.ppermute(value, 'h', [(i, i ^ 1) for i in range(axis_len['h'])])

    def frame(tile):
        rows = jnp.concatenate([from_prev(tile[-1:], 'h'), tile, from_next(tile[:1], 'h')], 0)
        return jnp.concatenate([from_prev(rows[:, -1:], 'w'), rows, from_next(rows[:, :1], 'w')], 1)

    def block_step(image, w_first, w_down, grad_out):
        image, grad_out = image[0], grad_out[0]
        x_own = frame(image)
        g_rows = jnp.concatenate([from_prev(grad_out[-1:], 'h'), grad_out], 0)
        g_own = jnp.concatenate([from_prev(g_rows[:, -1:], 'w'), g_rows], 1)
        x_pair, g_pair = swap_core(x_own), swap_core(g_own)
        a_own, z_tile = conv_first(x_own, w_first)
        z_rows = jnp.concatenate([z_tile, jnp.pad(from_next(z_tile[:1, :, :1], 'h'), ((0, 1),) + ((0, 0),) * 4)], 2)
        z_own = jnp.concatenate([z_rows, jnp.pad(from_next(z_rows[:, :1, :, :1], 'w'), ((0, 0), (0, 1)) + ((0, 0),) * 3)], 3)
        z_pair = swap_core(z_own)
        g_f32, gp_f32 = g_own.astype(F32), g_pair.astype(F32)
        p_down = weight_down(z_own, z_pair, g_f32, gp_f32)
        w_taps = w_down.reshape(9, C, C)
        grad_pre = grad_pre_call(g_f32, a_own, w_taps)
        d_pair = swap_core(grad_pre)
        p_first = weight_first(x_own, x_pair, grad_pre, d_pair)
        block_out = conv_down(z_own, w_taps)
        grad_image = grad_image_call(frame(grad_pre.reshape(ROWS, COLS, C)), w_first.reshape(9, C, C))
        grad_w_down, grad_w_first = settle(*reduce_all(p_down, p_first))
        return (block_out.reshape(1, OUT_R, OUT_C, C), grad_image.reshape(1, ROWS, COLS, C),
                grad_w_first.reshape(3, 3, C, C), grad_w_down.reshape(3, 3, C, C))

    img_spec = P(None, 'h', 'w', None)
    return jax.shard_map(block_step, mesh=mesh, in_specs=(img_spec, P(), P(), img_spec), out_specs=(img_spec, img_spec, P(), P()), check_vma=False)
```

```python
import jax
import jax.numpy as jnp
from jax import lax
from jax.sharding import PartitionSpec as P
from jax.experimental import pallas as pl
from jax.experimental.pallas import tpu as pltpu

MESH = pl.DeviceIdType.MESH
F32, BF16 = jnp.float32, jnp.bfloat16
C = 640
ROWS, COLS = 24, 48
OUT_R, OUT_C = 12, 24
PIX, OPIX = ROWS * COLS, OUT_R * OUT_C
HALF = 320
MIB = 2 ** 20
ORDERS = (('x', 'y', 'z'), ('y', 'z', 'x'), ('z', 'x', 'y'))
R1, R2, R3, A1, A2, A3A, A3B, DA, DB, DC, LA, LB, LC = range(13)


def gelu_tanh(values):
    return jax.nn.gelu(values, approximate=True)


def dot(lhs, rhs):
    return lax.dot_general(lhs, rhs, (((1,), (0,)), ((), ())), preferred_element_type=F32)


def dot_rhs_t(lhs, rhs):
    return lax.dot_general(lhs, rhs, (((1,), (1,)), ((), ())), preferred_element_type=F32)


def dot_lhs_t(lhs, rhs):
    return lax.dot_general(lhs, rhs, (((0,), (0,)), ((), ())), preferred_element_type=F32)


VM = pl.BlockSpec(memory_space=pltpu.VMEM)
ANY = pl.BlockSpec(memory_space=pl.ANY)


def shift_columns(ext_ref, out_ref):
    def one_row(r, _):
        for c in range(3):
            out_ref[c, pl.ds(pl.multiple_of(r * COLS, COLS), COLS), :] = ext_ref[r, c:c + COLS, :]
        return 0
    lax.fori_loop(0, ROWS + 2, one_row, 0)


def conv_first_kernel(ext_ref, w_ref, a_ref, z_ref, cat, sa, sz):
    step = pl.program_id(0)

    @pl.when(step == 0)
    def _():
        def one_row(r, _):
            for c in range(3):
                cat[pl.ds(pl.multiple_of(r * COLS, COLS), COLS), c * C:(c + 1) * C] = ext_ref[r, c:c + COLS, :]
            return 0
        lax.fori_loop(0, ROWS + 2, one_row, 0)

    block = 8 * COLS
    acc = None
    for a in range(3):
        rows = pl.ds(pl.multiple_of(step * block + a * COLS, COLS), block)
        part = dot(cat[rows, :], w_ref[a])
        acc = part if acc is None else acc + part
    pre = acc.astype(BF16).astype(F32)
    act = gelu_tanh(pre).astype(BF16).astype(F32)
    for lane in range(5):
        sa[lane] = pre[:, lane * 128:(lane + 1) * 128]
        sz[lane] = act[:, lane * 128:(lane + 1) * 128]
    for r in range(8):
        for cp in range(2):
            for lane in range(5):
                rows, lanes = pl.ds(r * COLS + cp, OUT_C, stride=2), pl.ds(lane * 128, 128)
                a_ref[r % 2, cp, r // 2, :, lanes] = sa[lane, rows, :]
                z_ref[r % 2, cp, r // 2, :, lanes] = sz[lane, rows, :]


def conv_first(image_ext, w_first):
    shape = jax.ShapeDtypeStruct((2, 2, OUT_R, OUT_C, C), F32)
    spec = pl.BlockSpec((2, 2, 4, OUT_C, C), lambda i: (0, 0, i, 0, 0))
    return pl.pallas_call(
        conv_first_kernel, grid=(3,), out_shape=[shape, shape],
        in_specs=[pl.BlockSpec(image_ext.shape, lambda i: (0, 0, 0)), pl.BlockSpec((3, 3 * C, C), lambda i: (0, 0, 0))],
        out_specs=[spec, spec],
        scratch_shapes=[pltpu.VMEM(((ROWS + 2) * COLS, 3 * C), BF16), pltpu.VMEM((5, 8 * COLS, 128), F32), pltpu.VMEM((5, 8 * COLS, 128), F32)],
        compiler_params=pltpu.CompilerParams(vmem_limit_bytes=56 * MIB),
        cost_estimate=pl.CostEstimate(flops=2 * PIX * 9 * C * C, bytes_accessed=16 * MIB, transcendentals=PIX * C),
    )(image_ext, w_first.reshape(3, 3 * C, C))


def weight_down_kernel(z_ref, zp_ref, g_ref, gp_ref, out_ref, tap_ref, taps, gs):
    core = lax.axis_index('h') % 2
    for src, (zr, gr) in enumerate(((z_ref, g_ref), (zp_ref, gp_ref))):
        gs[src * OPIX:(src + 1) * OPIX, :] = gr[1:, 1:, :].reshape(OPIX, C).astype(BF16)
        for t in range(9):
            a, c = t // 3, t % 3
            tap = zr[a % 2, c % 2, a // 2:a // 2 + OUT_R, c // 2:c // 2 + OUT_C, :].reshape(OPIX, C).astype(BF16)
            taps[t, src * OPIX:(src + 1) * OPIX, :] = tap
            if src == 0:
                tap_ref[t] = tap

    def one(j, _):
        res = dot_lhs_t(taps[4 * core + j], gs[...])
        out_ref[2 * j] = res[:HALF]
        out_ref[2 * j + 1] = res[HALF:]
        return 0
    lax.fori_loop(0, 5, one, 0)


def weight_down(z_own, z_pair, g_own, g_pair):
    return pl.pallas_call(
        weight_down_kernel, out_shape=[jax.ShapeDtypeStruct((10, HALF, C), F32), jax.ShapeDtypeStruct((9, OPIX, C), BF16)], in_specs=[VM] * 4, out_specs=[VM] * 2,
        scratch_shapes=[pltpu.VMEM((9, 2 * OPIX, C), BF16), pltpu.VMEM((2 * OPIX, C), BF16)],
        compiler_params=pltpu.CompilerParams(vmem_limit_bytes=56 * MIB),
        cost_estimate=pl.CostEstimate(flops=2 * OPIX * 9 * C * C, bytes_accessed=16 * MIB, transcendentals=0),
    )(z_own, z_pair, g_own, g_pair)


def place():
    w, h = lax.axis_index('w'), lax.axis_index('h')
    bit = {'x': h // 2, 'c': h % 2, 'y': w % 2, 'z': w // 2}
    dev = {'x': (w, (h + 2) % 4), 'c': (w, h + 1 - 2 * (h % 2)), 'y': (w + 1 - 2 * (w % 2), h), 'z': ((w + 2) % 4, h)}
    return bit, dev


class Reducer:
    def __init__(self, index, own, land, out, sems, grants, bit, dev):
        self.index, self.own, self.land, self.out, self.sems, self.grants, self.bit, self.dev = index, own, land, out, sems, grants, bit, dev

    def starts(self, third):
        b = [self.bit[axis] for axis in ORDERS[third]]
        base2 = b[0] * 160
        base3 = base2 + b[1] * 80
        return b, base2, base3, base3 + b[2] * 40

    def copy(self, third, kind):
        b, base2, base3, base4 = self.starts(third)
        core = self.bit['c']
        far = (1 - b[0]) * 160
        src, size, axis = {
            R1: (far, 160, 0), R2: (base2 + (1 - b[1]) * 80, 80, 1), R3: (base3 + (1 - b[2]) * 40, 40, 2),
            A1: (base4, 40, 2), A2: (base3, 80, 1), A3A: (base3, 80, 0), A3B: (base2 + (1 - b[1]) * 80, 80, 0),
            DA: (base2, 160, 'c'), DB: (far + b[1] * 80, 80, 'c'), DC: (far + (1 - b[1]) * 80, 80, 'c'),
            LA: (base2, 160, None), LB: (far + b[1] * 80, 80, None), LC: (far + (1 - b[1]) * 80, 80, None),
        }[kind]
        rows = pl.ds(pl.multiple_of(src, 8), size)
        source = self.own.at[pl.ds(core + 3 * third, 3), rows]
        send, recv = (s.at[self.index, third, kind] for s in self.sems)
        if kind <= R3:
            target = self.land.at[pl.ds(3 * third, 3), pl.ds((0, 160, 240)[kind], size)]
        elif kind <= A3B:
            target = source
        else:
            target = self.out.at[pl.ds(9 * core + 3 * third, 3), rows]
        if axis is None:
            return pltpu.make_async_copy(source, target, recv)
        peer = self.dev[axis if axis == 'c' else ORDERS[third][axis]]
        return pltpu.make_async_remote_copy(src_ref=source, dst_ref=target, send_sem=send, recv_sem=recv, device_id=peer, device_id_type=MESH)

    def add(self, third, kind):
        _, base2, base3, base4 = self.starts(third)
        keep, size = ((base2, 160), (base3, 80), (base4, 40))[kind]
        land_at = (0, 160, 240)[kind]
        steps = size // 40

        def body(j, _):
            unit, row = 3 * third + j // steps, (j % steps) * 40
            rows = pl.ds(pl.multiple_of(keep + row, 8), 40)
            where = self.bit['c'] + unit
            self.own[where, rows, :] += self.land[unit, pl.ds(pl.multiple_of(land_at + row, 8), 40), :]
            return 0
        lax.fori_loop(0, 3 * steps, body, 0)

    def begin(self):
        for third in range(3):
            self.copy(third, R1).start()

    def move(self, wait_for, then, add=False):
        for third in range(3):
            self.copy(third, wait_for).wait()
            if add:
                pl.semaphore_signal(self.grants.at[self.index, third, wait_for], inc=1, device_id=self.dev[ORDERS[third][wait_for]], device_id_type=MESH)
                self.add(third, wait_for)
            for kind in then:
                if kind in (A1, A2, A3A):
                    pl.semaphore_wait(self.grants.at[self.index, third, {A1: R3, A2: R2, A3A: R1}[kind]], 1)
                self.copy(third, kind).start()

    def finish(self):
        for kind in (DA, DB, DC, LA, LB, LC):
            self.move(kind, ())


NEAR = [(dw, dh) for dw in (-1, 0, 1) for dh in (-1, 0, 1) if (dw, dh) != (0, 0)]
EDGE = 8


def lane(k):
    return pl.ds(k * 128, 128)


def back_kernel(p_down, taps_in, g_in, a_in, w_down, w_first, x_in, xp_in, y_out, dx_out, o_down, o_first,
                own_d, own_f, land_d, land_f, wbuf, xs, ext, taps, g_ext, da, da_pair, grid, acc,
                row_send, col_send, cor_send, row_land, col_land, cor_land,
                load_sems, pair_sems, near_sems, out_sems, send_sems, recv_sems, grants):
    bit, dev = place()
    w, h = lax.axis_index('w'), lax.axis_index('h')
    core = bit['c']
    flat_a = own_f.at[pl.ds(0, 4), pl.ds(0, OPIX)]
    loads = {}
    for i, (name, src, dst) in enumerate((('p', p_down, own_d), ('w', w_down, wbuf), ('g', g_in, g_ext), ('a', a_in, flat_a),
                                          ('x', x_in, ext), ('t', taps_in, taps))):
        loads[name] = pltpu.make_async_copy(src, dst, load_sems.at[i])
        loads[name].start()
    barrier = pltpu.get_barrier_semaphore()
    for axis in 'xyzc':
        pl.semaphore_signal(barrier, inc=1, device_id=dev[axis], device_id_type=MESH)
    for dw, dh in NEAR:
        pl.semaphore_signal(barrier, inc=1, device_id=((w + dw + 4) % 4, (h + dh + 4) % 4), device_id_type=MESH)
    pl.semaphore_wait(barrier, 12)
    sems = (send_sems, recv_sems)
    down = Reducer(0, own_d, land_d, o_down, sems, grants, bit, dev)
    first = Reducer(1, own_f, land_f, o_first, sems, grants, bit, dev)
    both = (down, first)
    loads['p'].wait()
    down.begin()

    loads['g'].wait()
    for di in range(2):
        for dj in range(2):
            at = (2 * di + dj) * OPIX
            xs[1, 0, at:at + OPIX, :] = g_ext[di:di + OUT_R, dj:dj + OUT_C, :].reshape(OPIX, C).astype(BF16)
    loads['a'].wait()
    loads['w'].wait()
    for rp in range(2):
        for cp in range(2):
            total = None
            for a in ((0, 2), (1,))[rp]:
                for c in ((0, 2), (1,))[cp]:
                    at = (2 * (1 - a // 2) + 1 - c // 2) * OPIX
                    part = dot_rhs_t(xs[1, 0, at:at + OPIX, :], wbuf[3 * a + c])
                    total = part if total is None else total + part
            pre = own_f[2 * rp + cp, 0:OPIX, :]
            grad = jax.vjp(gelu_tanh, pre)[1](total)[0].astype(BF16).astype(F32)
            for i in range(OUT_R):
                for k in range(5):
                    grid[k, 2 * i + rp + 1, pl.ds(EDGE + cp, OUT_C, stride=2), :] = grad[i * OUT_C:(i + 1) * OUT_C, k * 128:(k + 1) * 128]

    def pack(r, _):
        for k in range(5):
            da[pl.ds(pl.multiple_of(r * COLS, COLS), COLS), lane(k)] = grid[k, r + 1, EDGE:EDGE + COLS, :].astype(BF16)
        return 0
    lax.fori_loop(0, ROWS, pack, 0)
    share = pltpu.make_async_remote_copy(src_ref=da, dst_ref=da_pair, send_sem=pair_sems.at[0], recv_sem=pair_sems.at[1], device_id=dev['c'], device_id_type=MESH)
    share.start()

    last_r, last_c = ROWS, EDGE + COLS - 1
    for k in range(5):
        for side, r in enumerate((1, last_r)):
            row_send[side, :, lane(k)] = grid[k, r, EDGE:EDGE + COLS, :]
        for side, c in enumerate((EDGE, last_c)):
            for r in range(ROWS):
                col_send[side, r:r + 1, lane(k)] = grid[k, r + 1, c:c + 1, :]
            for vert, r in enumerate((1, last_r)):
                cor_send[2 * vert + side, :, lane(k)] = jnp.broadcast_to(grid[k, r, c:c + 1, :], (8, 128))
    borders = []
    for i, (dw, dh) in enumerate(NEAR):
        if dw == 0:
            src, dst = row_send.at[(dh + 1) // 2], row_land.at[(1 - dh) // 2]
        elif dh == 0:
            src, dst = col_send.at[(dw + 1) // 2], col_land.at[(1 - dw) // 2]
        else:
            src = cor_send.at[2 * ((dh + 1) // 2) + (dw + 1) // 2]
            dst = cor_land.at[2 * ((1 - dh) // 2) + (1 - dw) // 2]
        peer = ((w + dw + 4) % 4, (h + dh + 4) % 4)
        copy = pltpu.make_async_remote_copy(src_ref=src, dst_ref=dst, send_sem=near_sems.at[0, i], recv_sem=near_sems.at[1, i], device_id=peer, device_id_type=MESH)
        copy.start()
        borders.append(copy)

    loads['x'].wait()
    shift_columns(ext, xs.at[0])
    pair_load = pltpu.make_async_copy(xp_in, ext, load_sems.at[6])
    pair_load.start()

    loads['t'].wait()
    for t in range(9):
        part = dot(taps[t], wbuf[t])
        acc[0:OPIX, :] = part if t == 0 else acc[0:OPIX, :] + part
    y_stage = taps.at[0]
    y_stage[...] = acc[0:OPIX, :].astype(BF16)
    y_copy = pltpu.make_async_copy(y_stage, y_out, out_sems.at[0])
    y_copy.start()
    w_copy = pltpu.make_async_copy(w_first, wbuf, load_sems.at[7])
    w_copy.start()

    pair_load.wait()
    shift_columns(ext, xs.at[1])
    share.wait()

    def first_tap(j, _):
        t = 4 * core + j
        a, c = t // 3, t % 3
        rows = pl.ds(pl.multiple_of(a * COLS, COLS), PIX)
        res = dot_lhs_t(xs[0, c, rows, :], da[...]) + dot_lhs_t(xs[1, c, rows, :], da_pair[...])
        own_f[2 * j] = res[:HALF]
        own_f[2 * j + 1] = res[HALF:]
        return 0
    lax.fori_loop(0, 4, first_tap, 0)
    down.move(R1, (R2,), add=True)
    first_tap(4, 0)
    first.begin()

    for copy in borders:
        copy.wait()
    for side, edge in enumerate((h == 0, h == 3)):
        for k in range(5):
            grid[k, side * (ROWS + 1), EDGE:EDGE + COLS, :] = jnp.where(edge, 0.0, row_land[side, :, lane(k)])
    for side, edge in enumerate((w == 0, w == 3)):
        c = (EDGE - 1, EDGE + COLS)[side]
        for k in range(5):
            for r in range(ROWS):
                grid[k, r + 1, c:c + 1, :] = jnp.where(edge, 0.0, col_land[side, r:r + 1, lane(k)])
            for vert, far in enumerate((h == 0, h == 3)):
                grid[k, vert * (ROWS + 1), c:c + 1, :] = jnp.where(jnp.logical_or(edge, far), 0.0, cor_land[2 * vert + side, 0:1, lane(k)])

    def spread(r, _):
        for c in range(3):
            for k in range(5):
                xs[0, c, pl.ds(pl.multiple_of(r * COLS, COLS), COLS), lane(k)] = grid[k, r, EDGE - 1 + c:EDGE - 1 + c + COLS, :].astype(BF16)
        return 0
    lax.fori_loop(0, ROWS + 2, spread, 0)
    w_copy.wait()
    block = 8 * COLS

    def image_rows(i, _):
        for t in range(9):
            a, c = t // 3, t % 3
            rows = pl.ds(pl.multiple_of(i * block + (2 - a) * COLS, COLS), block)
            part = dot_rhs_t(xs[0, 2 - c, rows, :], wbuf[t])
            acc[...] = part if t == 0 else acc[...] + part
        da_pair[pl.ds(pl.multiple_of(i * block, block), block), :] = acc[...].astype(BF16)
        return 0
    lax.fori_loop(0, 3, image_rows, 0)
    dx_copy = pltpu.make_async_copy(da_pair, dx_out, out_sems.at[1])
    dx_copy.start()

    down.move(R2, (R3,), add=True)
    first.move(R1, (R2,), add=True)
    down.move(R3, (A1,), add=True)
    first.move(R2, (R3,), add=True)
    down.move(A1, (A2, A3A))
    first.move(R3, (A1,), add=True)
    down.move(A2, (A3B, DA, LA))
    first.move(A1, (A2, A3A))
    down.move(A3A, (DB, LB))
    first.move(A2, (A3B, DA, LA))
    down.move(A3B, (DC, LC))
    first.move(A3A, (DB, LB))
    first.move(A3B, (DC, LC))
    y_copy.wait()
    dx_copy.wait()
    for one in both:
        one.finish()


def back_call(p_down, taps, g_ext, a_own, w_down, w_first, x_own, x_pair):
    total = jax.ShapeDtypeStruct((18, HALF, C), F32)
    line = ((ROWS + 2) * COLS, C)
    dma = pltpu.SemaphoreType.DMA
    return pl.pallas_call(
        back_kernel,
        out_shape=[jax.ShapeDtypeStruct((OPIX, C), BF16), jax.ShapeDtypeStruct((PIX, C), BF16), total, total],
        in_specs=[ANY] * 8, out_specs=[ANY] * 4,
        scratch_shapes=[pltpu.VMEM((10, HALF, C), F32)] * 2 + [pltpu.VMEM((9, 280, C), F32)] * 2
        + [pltpu.VMEM((9, C, C), BF16), pltpu.VMEM((2, 3) + line, BF16)]
        + [pltpu.VMEM((ROWS + 2, COLS + 2, C), BF16)]
        + [pltpu.VMEM((9, OPIX, C), BF16), pltpu.VMEM((OUT_R + 1, OUT_C + 1, C), F32)]
        + [pltpu.VMEM((PIX, C), BF16)] * 2
        + [pltpu.VMEM((5, ROWS + 2, COLS + 2 * EDGE, 128), F32), pltpu.VMEM((8 * COLS, C), F32)]
        + [pltpu.VMEM((2, COLS, C), F32), pltpu.VMEM((2, ROWS, C), F32), pltpu.VMEM((4, 8, C), F32)] * 2
        + [dma((8,)), dma((2,)), dma((2, 8)), dma((2,)), dma((2, 3, 13)), dma((2, 3, 13)), pltpu.SemaphoreType.REGULAR((2, 3, 3))],
        compiler_params=pltpu.CompilerParams(collective_id=1, has_side_effects=True, vmem_limit_bytes=67043328),
        cost_estimate=pl.CostEstimate(flops=2 * PIX * 90 * C * C, bytes_accessed=64 * MIB, transcendentals=0),
    )(p_down, taps, g_ext, a_own, w_down, w_first, x_own, x_pair)


def settle_kernel(in_a, in_b, out_a, out_b, buf, load_sems, store_sems):
    loads, stores = [], []
    for i, (src, dst) in enumerate(((in_a, out_a), (in_b, out_b))):
        for part in range(9):
            span = pl.ds(2 * part, 2)
            loads.append(pltpu.make_async_copy(src.at[span], buf.at[i, span], load_sems.at[i, part]))
            stores.append(pltpu.make_async_copy(buf.at[i, span], dst.at[span], store_sems.at[i, part]))
    for load in loads:
        load.start()
    for load, store in zip(loads, stores):
        load.wait()
        store.start()
    for store in stores:
        store.wait()


def settle(sum_a, sum_b):
    shape = jax.ShapeDtypeStruct((18, HALF, C), F32)
    return pl.pallas_call(
        settle_kernel, out_shape=[shape, shape], in_specs=[ANY] * 2, out_specs=[ANY] * 2,
        scratch_shapes=[pltpu.VMEM((2, 18, HALF, C), F32), pltpu.SemaphoreType.DMA((2, 9)), pltpu.SemaphoreType.DMA((2, 9))],
        compiler_params=pltpu.CompilerParams(vmem_limit_bytes=56 * MIB),
    )(sum_a, sum_b)


def solution(mesh):
    axis_len = {'h': mesh.shape['h'], 'w': mesh.shape['w']}

    def from_prev(edge, axis):
        return lax.ppermute(edge, axis, [(i, i + 1) for i in range(axis_len[axis] - 1)])

    def from_next(edge, axis):
        return lax.ppermute(edge, axis, [(i + 1, i) for i in range(axis_len[axis] - 1)])

    def swap_core(value):
        return lax.ppermute(value, 'h', [(i, i ^ 1) for i in range(axis_len['h'])])

    def frame(tile):
        rows = jnp.concatenate([from_prev(tile[-1:], 'h'), tile, from_next(tile[:1], 'h')], 0)
        return jnp.concatenate([from_prev(rows[:, -1:], 'w'), rows, from_next(rows[:, :1], 'w')], 1)

    def block_step(image, w_first, w_down, grad_out):
        image, grad_out = image[0], grad_out[0]
        x_own = frame(image)
        g_rows = jnp.concatenate([from_prev(grad_out[-1:], 'h'), grad_out], 0)
        g_own = jnp.concatenate([from_prev(g_rows[:, -1:], 'w'), g_rows], 1)
        x_pair, g_pair = swap_core(x_own), swap_core(g_own)
        a_own, z_tile = conv_first(x_own, w_first)
        z_rows = jnp.concatenate([z_tile, jnp.pad(from_next(z_tile[:1, :, :1], 'h'), ((0, 1),) + ((0, 0),) * 4)], 2)
        z_own = jnp.concatenate([z_rows, jnp.pad(from_next(z_rows[:, :1, :, :1], 'w'), ((0, 0), (0, 1)) + ((0, 0),) * 3)], 3)
        z_pair = swap_core(z_own)
        g_f32, gp_f32 = g_own.astype(F32), g_pair.astype(F32)
        p_down, taps = weight_down(z_own, z_pair, g_f32, gp_f32)
        block_out, grad_image, sum_down, sum_first = back_call(
            p_down, taps, g_f32, a_own.reshape(4, OPIX, C), w_down.reshape(9, C, C), w_first.reshape(9, C, C), x_own, x_pair)
        grad_w_down, grad_w_first = settle(sum_down, sum_first)
        return (block_out.reshape(1, OUT_R, OUT_C, C), grad_image.reshape(1, ROWS, COLS, C),
                grad_w_first.reshape(3, 3, C, C), grad_w_down.reshape(3, 3, C, C))

    img_spec = P(None, 'h', 'w', None)
    return jax.shard_map(block_step, mesh=mesh, in_specs=(img_spec, P(), P(), img_spec), out_specs=(img_spec, img_spec, P(), P()), check_vma=False)
```

```python
import jax
import jax.numpy as jnp
from jax import lax
from jax.sharding import PartitionSpec as P
from jax.experimental import pallas as pl
from jax.experimental.pallas import tpu as pltpu

MESH = pl.DeviceIdType.MESH
F32, BF16 = jnp.float32, jnp.bfloat16
C = 640
ROWS, COLS = 24, 48
OUT_R, OUT_C = 12, 24
PIX, OPIX = ROWS * COLS, OUT_R * OUT_C
HALF = 320
MIB = 2 ** 20
ORDERS = (('x', 'y', 'z'), ('y', 'z', 'x'), ('z', 'x', 'y'))
R1, R2, R3, A1, A2, A3A, A3B, DA, DB, DC, LA, LB, LC = range(13)


def gelu_tanh(values):
    return jax.nn.gelu(values, approximate=True)


def dot(lhs, rhs):
    return lax.dot_general(lhs, rhs, (((1,), (0,)), ((), ())), preferred_element_type=F32)


def dot_rhs_t(lhs, rhs):
    return lax.dot_general(lhs, rhs, (((1,), (1,)), ((), ())), preferred_element_type=F32)


def dot_lhs_t(lhs, rhs):
    return lax.dot_general(lhs, rhs, (((0,), (0,)), ((), ())), preferred_element_type=F32)


ANY = pl.BlockSpec(memory_space=pl.ANY)


def place():
    w, h = lax.axis_index('w'), lax.axis_index('h')
    bit = {'x': h // 2, 'c': h % 2, 'y': w % 2, 'z': w // 2}
    dev = {'x': (w, (h + 2) % 4), 'c': (w, h + 1 - 2 * (h % 2)), 'y': (w + 1 - 2 * (w % 2), h), 'z': ((w + 2) % 4, h)}
    return bit, dev


class Reducer:
    def __init__(self, index, own, land, out, sems, grants, bit, dev):
        self.index, self.own, self.land, self.out, self.sems, self.grants, self.bit, self.dev = index, own, land, out, sems, grants, bit, dev

    def starts(self, third):
        b = [self.bit[axis] for axis in ORDERS[third]]
        base2 = b[0] * 160
        base3 = base2 + b[1] * 80
        return b, base2, base3, base3 + b[2] * 40

    def copy(self, third, kind):
        b, base2, base3, base4 = self.starts(third)
        core = self.bit['c']
        far = (1 - b[0]) * 160
        src, size, axis = {
            R1: (far, 160, 0), R2: (base2 + (1 - b[1]) * 80, 80, 1), R3: (base3 + (1 - b[2]) * 40, 40, 2),
            A1: (base4, 40, 2), A2: (base3, 80, 1), A3A: (base3, 80, 0), A3B: (base2 + (1 - b[1]) * 80, 80, 0),
            DA: (base2, 160, 'c'), DB: (far + b[1] * 80, 80, 'c'), DC: (far + (1 - b[1]) * 80, 80, 'c'),
            LA: (base2, 160, None), LB: (far + b[1] * 80, 80, None), LC: (far + (1 - b[1]) * 80, 80, None),
        }[kind]
        rows = pl.ds(pl.multiple_of(src, 8), size)
        source = self.own.at[pl.ds(core + 3 * third, 3), rows]
        send, recv = (s.at[self.index, third, kind] for s in self.sems)
        if kind <= R3:
            target = self.land.at[pl.ds(3 * third, 3), pl.ds((0, 160, 240)[kind], size)]
        elif kind <= A3B:
            target = source
        else:
            target = self.out.at[pl.ds(9 * core + 3 * third, 3), rows]
        if axis is None:
            return pltpu.make_async_copy(source, target, recv)
        peer = self.dev[axis if axis == 'c' else ORDERS[third][axis]]
        return pltpu.make_async_remote_copy(src_ref=source, dst_ref=target, send_sem=send, recv_sem=recv, device_id=peer, device_id_type=MESH)

    def add(self, third, kind):
        _, base2, base3, base4 = self.starts(third)
        keep, size = ((base2, 160), (base3, 80), (base4, 40))[kind]
        land_at = (0, 160, 240)[kind]
        steps = size // 40

        def body(j, _):
            unit, row = 3 * third + j // steps, (j % steps) * 40
            rows = pl.ds(pl.multiple_of(keep + row, 8), 40)
            where = self.bit['c'] + unit
            self.own[where, rows, :] += self.land[unit, pl.ds(pl.multiple_of(land_at + row, 8), 40), :]
            return 0
        lax.fori_loop(0, 3 * steps, body, 0)

    def begin(self):
        for third in range(3):
            self.copy(third, R1).start()

    def move(self, wait_for, then, add=False):
        for third in range(3):
            self.copy(third, wait_for).wait()
            if add:
                pl.semaphore_signal(self.grants.at[self.index, third, wait_for], inc=1, device_id=self.dev[ORDERS[third][wait_for]], device_id_type=MESH)
                self.add(third, wait_for)
            for kind in then:
                if kind in (A1, A2, A3A):
                    pl.semaphore_wait(self.grants.at[self.index, third, {A1: R3, A2: R2, A3A: R1}[kind]], 1)
                self.copy(third, kind).start()

    def finish(self):
        for kind in (DA, DB, DC, LA, LB, LC):
            self.move(kind, ())


EDGE = 8
LINES = (ROWS + 2) * COLS
BLOCK = 8 * COLS
NEAR = [(dw, dh) for dw in (-1, 0, 1) for dh in (-1, 0, 1) if (dw, dh) != (0, 0)]
ABOVE = [(-1, -1), (-1, 0), (0, -1)]
BELOW = [(1, 1), (1, 0), (0, 1)]
G_AT, G_PAIR_AT, TAP_PAIR_AT = 3 * OPIX, 4 * OPIX, 5 * OPIX


def lane(k):
    return pl.ds(k * 128, 128)


def at(start, size):
    return pl.ds(pl.multiple_of(start, size), size)


class Border:
    def __init__(self, grid, row0, rows, cols, send, land, sems, send_to, take_from):
        self.grid, self.row0, self.rows, self.cols, self.sends, self.lands = grid, row0, rows, cols, send, land
        self.sems, self.send_to, self.take_from = sems, send_to, take_from
        self.w, self.h = lax.axis_index('w'), lax.axis_index('h')

    def edge(self, step, first, size, outside):
        return {-1: first - outside, 1: first + size - 1 + outside}[step]

    def copies(self):
        found = []
        for dw, dh in self.send_to:
            i = NEAR.index((dw, dh))
            if dw == 0:
                src, dst = self.sends[0].at[(dh + 1) // 2], self.lands[0].at[(1 - dh) // 2]
            elif dh == 0:
                src, dst = self.sends[1].at[(dw + 1) // 2], self.lands[1].at[(1 - dw) // 2]
            else:
                src = self.sends[2].at[2 * ((dh + 1) // 2) + (dw + 1) // 2]
                dst = self.lands[2].at[2 * ((1 - dh) // 2) + (1 - dw) // 2]
            peer = ((self.w + dw + 4) % 4, (self.h + dh + 4) % 4)
            found.append(pltpu.make_async_remote_copy(src_ref=src, dst_ref=dst, send_sem=self.sems.at[0, i], recv_sem=self.sems.at[1, i], device_id=peer, device_id_type=MESH))
        return found

    def start(self):
        grid, row0, rows, cols = self.grid, self.row0, self.rows, self.cols
        for dw, dh in self.send_to:
            r = None if dh == 0 else self.edge(dh, row0, rows, 0)
            c = None if dw == 0 else self.edge(dw, EDGE, cols, 0)
            for k in range(5):
                if dw == 0:
                    self.sends[0][(dh + 1) // 2, :, lane(k)] = grid[k, r, EDGE:EDGE + cols, :]
                elif dh == 0:
                    for row in range(rows):
                        self.sends[1][(dw + 1) // 2, row:row + 1, lane(k)] = grid[k, row0 + row, c:c + 1, :]
                else:
                    self.sends[2][2 * ((dh + 1) // 2) + (dw + 1) // 2, :, lane(k)] = jnp.broadcast_to(grid[k, r, c:c + 1, :], (8, 128))
        for copy in self.copies():
            copy.start()

    def finish(self):
        grid, row0, rows, cols = self.grid, self.row0, self.rows, self.cols
        for copy in self.copies():
            copy.wait()
        for dw, dh in self.take_from:
            r = None if dh == 0 else self.edge(dh, row0, rows, 1)
            c = None if dw == 0 else self.edge(dw, EDGE, cols, 1)
            out_w = {-1: self.w == 0, 0: False, 1: self.w == 3}[dw]
            out_h = {-1: self.h == 0, 0: False, 1: self.h == 3}[dh]
            for k in range(5):
                if dw == 0:
                    grid[k, r, EDGE:EDGE + cols, :] = jnp.where(out_h, 0.0, self.lands[0][(dh + 1) // 2, :, lane(k)])
                elif dh == 0:
                    for row in range(rows):
                        grid[k, row0 + row, c:c + 1, :] = jnp.where(out_w, 0.0, self.lands[1][(dw + 1) // 2, row:row + 1, lane(k)])
                else:
                    out = jnp.logical_or(out_w, out_h)
                    grid[k, r, c:c + 1, :] = jnp.where(out, 0.0, self.lands[2][2 * ((dh + 1) // 2) + (dw + 1) // 2, 0:1, lane(k)])


def spread(grid, xs):
    def one_row(r, _):
        for c in range(3):
            for k in range(5):
                xs[0, at(c * LINES + r * COLS, COLS), lane(k)] = grid[k, r, EDGE - 1 + c:EDGE - 1 + c + COLS, :].astype(BF16)
        return 0
    lax.fori_loop(0, ROWS + 2, one_row, 0)


def accumulate(acc, rows, part, first):
    for k in range(5):
        piece = part[:, k * 128:(k + 1) * 128]
        acc[k, 0:rows, :] = piece if first else acc[k, 0:rows, :] + piece


def block_kernel(x_in, g_in, w_first, w_down, y_out, dx_out, o_down, o_first, x_land,
                 own_d, own_f, land_d, land_f, wbuf, xs, taps, g_tile, g_grid, da, da_pair, grid, acc,
                 send_r, send_c, send_k, x_r, x_c, x_k, z_r, z_c, z_k, d_r, d_c, d_k, gs_r, gs_c, gs_k, gl_r, gl_c, gl_k,
                 load_sems, pair_sems, near_sems, out_sems, send_sems, recv_sems, grants):
    bit, dev = place()
    w, h = lax.axis_index('w'), lax.axis_index('h')
    core = bit['c']
    x_tile = xs.at[0, pl.ds(0, PIX)]
    load_x = pltpu.make_async_copy(x_in, x_tile, load_sems.at[0])
    load_g = pltpu.make_async_copy(g_in, g_tile, load_sems.at[1])
    load_w = pltpu.make_async_copy(w_first, wbuf, load_sems.at[2])
    for load in (load_x, load_g, load_w):
        load.start()
    barrier = pltpu.get_barrier_semaphore()
    for axis in 'xyzc':
        pl.semaphore_signal(barrier, inc=1, device_id=dev[axis], device_id_type=MESH)
    for dw, dh in NEAR:
        pl.semaphore_signal(barrier, inc=1, device_id=((w + dw + 4) % 4, (h + dh + 4) % 4), device_id_type=MESH)
    sends = (send_r, send_c, send_k)
    x_border = Border(grid, 1, ROWS, COLS, sends, (x_r, x_c, x_k), near_sems.at[0], NEAR, NEAR)
    z_border = Border(grid, 0, ROWS, COLS, sends, (z_r, z_c, z_k), near_sems.at[1], ABOVE, BELOW)
    d_border = Border(grid, 1, ROWS, COLS, sends, (d_r, d_c, d_k), near_sems.at[2], NEAR, NEAR)
    g_border = Border(g_grid, 1, OUT_R, OUT_C, (gs_r, gs_c, gs_k), (gl_r, gl_c, gl_k), near_sems.at[3], BELOW, ABOVE)
    sems = (send_sems, recv_sems)
    down = Reducer(0, own_d, land_d, o_down, sems, grants, bit, dev)
    first = Reducer(1, own_f, land_f, o_first, sems, grants, bit, dev)

    def to_pair(src, dst, i):
        return pltpu.make_async_remote_copy(src_ref=src, dst_ref=dst, send_sem=pair_sems.at[0, i], recv_sem=pair_sems.at[1, i], device_id=dev['c'], device_id_type=MESH)

    load_x.wait()

    def place_row(r, _):
        for k in range(5):
            grid[k, r + 1, EDGE:EDGE + COLS, :] = x_tile[at(r * COLS, COLS), lane(k)].astype(F32)
        return 0
    lax.fori_loop(0, ROWS, place_row, 0)
    pl.semaphore_wait(barrier, 12)
    x_border.start()
    load_g.wait()
    for r in range(OUT_R):
        for k in range(5):
            g_grid[k, r + 1, EDGE:EDGE + OUT_C, :] = g_tile[r, :, lane(k)].astype(F32)
    g_border.start()
    x_border.finish()
    spread(grid, xs)
    x_share = to_pair(xs.at[0], x_land, 0)
    x_share.start()
    load_w.wait()

    def pre_rows(i, _):
        for t in range(9):
            a, c = t // 3, t % 3
            rows = pl.ds(pl.multiple_of(c * LINES + i * BLOCK + a * COLS, COLS), BLOCK)
            accumulate(acc, BLOCK, dot(xs[0, rows, :], wbuf[t]), t == 0)
        for k in range(5):
            pre = acc[k].astype(BF16).astype(F32)
            acc[k] = pre
            act = gelu_tanh(pre).astype(BF16).astype(F32)
            for r in range(8):
                grid[k, 8 * i + r, EDGE:EDGE + COLS, :] = act[r * COLS:(r + 1) * COLS]
        for r in range(8):
            for cp in range(2):
                for k in range(5):
                    own_f[2 * (r % 2) + cp, pl.ds(pl.multiple_of((4 * i + r // 2) * OUT_C, 8), OUT_C), lane(k)] = acc[k, pl.ds(r * COLS + cp, OUT_C, stride=2), :]
        return 0
    lax.fori_loop(0, 3, pre_rows, 0)
    load_w2 = pltpu.make_async_copy(w_down, wbuf, load_sems.at[3])
    load_w2.start()
    z_border.start()

    g_border.finish()
    for di in range(2):
        for dj in range(2):
            for k in range(5):
                part = g_grid[k, di:di + OUT_R, EDGE - 1 + dj:EDGE - 1 + dj + OUT_C, :]
                xs[1, (2 * di + dj) * OPIX:(2 * di + dj + 1) * OPIX, lane(k)] = part.reshape(OPIX, 128).astype(BF16)
    g_share = to_pair(xs.at[1, pl.ds(G_AT, OPIX)], xs.at[1, pl.ds(G_PAIR_AT, OPIX)], 1)
    g_share.start()
    z_border.finish()

    def tap_rows(p, _):
        for t in range(9):
            a, c = t // 3, t % 3
            for k in range(5):
                cols = pl.ds(EDGE + c, OUT_C, stride=2)
                two = jnp.concatenate([grid[k, 4 * p + a, cols, :], grid[k, 4 * p + 2 + a, cols, :]], 0)
                taps[t, at(p * 2 * OUT_C, 2 * OUT_C), lane(k)] = two.astype(BF16)
        return 0
    lax.fori_loop(0, OUT_R // 2, tap_rows, 0)
    tap_shares = [to_pair(taps.at[4 * (1 - core) + j], xs.at[1, pl.ds(TAP_PAIR_AT + j * OPIX, OPIX)], 2 + j) for j in range(5)]
    for share in tap_shares:
        share.start()

    def down_tap(j, _):
        res = dot_lhs_t(taps[4 * core + j], xs[1, G_AT:G_AT + OPIX, :])
        own_d[2 * j] = res[:HALF]
        own_d[2 * j + 1] = res[HALF:]
        return 0
    lax.fori_loop(0, 5, down_tap, 0)
    g_share.wait()
    for share in tap_shares:
        share.wait()

    def down_tap_pair(j, _):
        rows = pl.ds(pl.multiple_of(TAP_PAIR_AT + j * OPIX, 32), OPIX)
        res = dot_lhs_t(xs[1, rows, :], xs[1, G_PAIR_AT:G_PAIR_AT + OPIX, :])
        own_d[2 * j] += res[:HALF]
        own_d[2 * j + 1] += res[HALF:]
        return 0
    lax.fori_loop(0, 5, down_tap_pair, 0)
    down.begin()

    load_w2.wait()
    for rp in range(2):
        for cp in range(2):
            total = None
            for a in ((0, 2), (1,))[rp]:
                for c in ((0, 2), (1,))[cp]:
                    row = (2 * (1 - a // 2) + 1 - c // 2) * OPIX
                    part = dot_rhs_t(xs[1, row:row + OPIX, :], wbuf[3 * a + c])
                    total = part if total is None else total + part
            pre = own_f[2 * rp + cp, 0:OPIX, :]
            grad = jax.vjp(gelu_tanh, pre)[1](total)[0].astype(BF16).astype(F32)
            for i in range(OUT_R):
                for k in range(5):
                    grid[k, 2 * i + rp + 1, pl.ds(EDGE + cp, OUT_C, stride=2), :] = grad[i * OUT_C:(i + 1) * OUT_C, k * 128:(k + 1) * 128]

    def pack(r, _):
        for k in range(5):
            da[at(r * COLS, COLS), lane(k)] = grid[k, r + 1, EDGE:EDGE + COLS, :].astype(BF16)
        return 0
    lax.fori_loop(0, ROWS, pack, 0)
    da_share = to_pair(da, da_pair, 7)
    da_share.start()
    d_border.start()
    x_share.wait()
    pair_load = pltpu.make_async_copy(x_land, xs.at[1], load_sems.at[4])
    pair_load.start()

    for t in range(9):
        accumulate(acc, OPIX, dot(taps[t], wbuf[t]), t == 0)
    for k in range(5):
        taps[0, :, lane(k)] = acc[k, 0:OPIX, :].astype(BF16)
    y_copy = pltpu.make_async_copy(taps.at[0], y_out, out_sems.at[0])
    y_copy.start()
    load_w1 = pltpu.make_async_copy(w_first, wbuf, load_sems.at[5])
    load_w1.start()
    pair_load.wait()
    da_share.wait()

    def first_tap(j, _):
        t = 4 * core + j
        a, c = t // 3, t % 3
        rows = pl.ds(pl.multiple_of(c * LINES + a * COLS, COLS), PIX)
        res = dot_lhs_t(xs[0, rows, :], da[...]) + dot_lhs_t(xs[1, rows, :], da_pair[...])
        own_f[2 * j] = res[:HALF]
        own_f[2 * j + 1] = res[HALF:]
        return 0
    lax.fori_loop(0, 4, first_tap, 0)
    down.move(R1, (R2,), add=True)
    first_tap(4, 0)
    first.begin()

    d_border.finish()
    spread(grid, xs)
    load_w1.wait()

    def image_rows(i, _):
        for t in range(9):
            a, c = t // 3, t % 3
            rows = pl.ds(pl.multiple_of((2 - c) * LINES + i * BLOCK + (2 - a) * COLS, COLS), BLOCK)
            accumulate(acc, BLOCK, dot_rhs_t(xs[0, rows, :], wbuf[t]), t == 0)
        for k in range(5):
            da_pair[at(i * BLOCK, BLOCK), lane(k)] = acc[k].astype(BF16)
        return 0
    lax.fori_loop(0, 3, image_rows, 0)
    dx_copy = pltpu.make_async_copy(da_pair, dx_out, out_sems.at[1])
    dx_copy.start()

    down.move(R2, (R3,), add=True)
    first.move(R1, (R2,), add=True)
    down.move(R3, (A1,), add=True)
    first.move(R2, (R3,), add=True)
    down.move(A1, (A2, A3A))
    first.move(R3, (A1,), add=True)
    down.move(A2, (A3B, DA, LA))
    first.move(A1, (A2, A3A))
    down.move(A3A, (DB, LB))
    first.move(A2, (A3B, DA, LA))
    down.move(A3B, (DC, LC))
    first.move(A3A, (DB, LB))
    first.move(A3B, (DC, LC))
    y_copy.wait()
    dx_copy.wait()
    down.finish()
    first.finish()


def block_call(image, grad_out, w_first, w_down):
    total = jax.ShapeDtypeStruct((18, HALF, C), F32)
    dma = pltpu.SemaphoreType.DMA
    edges = [pltpu.VMEM((2, COLS, C), F32), pltpu.VMEM((2, ROWS, C), F32), pltpu.VMEM((4, 8, C), F32)]
    small = [pltpu.VMEM((2, OUT_C, C), F32), pltpu.VMEM((2, OUT_R, C), F32), pltpu.VMEM((4, 8, C), F32)]
    return pl.pallas_call(
        block_kernel,
        out_shape=[jax.ShapeDtypeStruct((OPIX, C), BF16), jax.ShapeDtypeStruct((PIX, C), BF16), total, total,
                   jax.ShapeDtypeStruct((3 * LINES, C), BF16)],
        in_specs=[ANY] * 4, out_specs=[ANY] * 5,
        scratch_shapes=[pltpu.VMEM((10, HALF, C), F32)] * 2 + [pltpu.VMEM((9, 280, C), F32)] * 2
        + [pltpu.VMEM((9, C, C), BF16), pltpu.VMEM((2, 3 * LINES, C), BF16), pltpu.VMEM((9, OPIX, C), BF16)]
        + [pltpu.VMEM((OUT_R, OUT_C, C), BF16), pltpu.VMEM((5, OUT_R + 1, OUT_C + EDGE, 128), F32)]
        + [pltpu.VMEM((PIX, C), BF16)] * 2
        + [pltpu.VMEM((5, ROWS + 2, COLS + 2 * EDGE, 128), F32), pltpu.VMEM((5, BLOCK, 128), F32)]
        + edges * 4 + small * 2
        + [dma((6,)), dma((2, 8)), dma((4, 2, 8)), dma((2,)), dma((2, 3, 13)), dma((2, 3, 13)), pltpu.SemaphoreType.REGULAR((2, 3, 3))],
        compiler_params=pltpu.CompilerParams(collective_id=1, has_side_effects=True, vmem_limit_bytes=67043328),
        cost_estimate=pl.CostEstimate(flops=2 * PIX * 90 * C * C, bytes_accessed=64 * MIB, transcendentals=0),
    )(image.reshape(PIX, C), grad_out, w_first, w_down)


def settle_kernel(in_a, in_b, out_a, out_b, buf, load_sems, store_sems):
    loads, stores = [], []
    for i, (src, dst) in enumerate(((in_a, out_a), (in_b, out_b))):
        for part in range(9):
            span = pl.ds(2 * part, 2)
            loads.append(pltpu.make_async_copy(src.at[span], buf.at[i, span], load_sems.at[i, part]))
            stores.append(pltpu.make_async_copy(buf.at[i, span], dst.at[span], store_sems.at[i, part]))
    for load in loads:
        load.start()
    for load, store in zip(loads, stores):
        load.wait()
        store.start()
    for store in stores:
        store.wait()


def settle(sum_a, sum_b):
    shape = jax.ShapeDtypeStruct((18, HALF, C), F32)
    return pl.pallas_call(
        settle_kernel, out_shape=[shape, shape], in_specs=[ANY] * 2, out_specs=[ANY] * 2,
        scratch_shapes=[pltpu.VMEM((2, 18, HALF, C), F32), pltpu.SemaphoreType.DMA((2, 9)), pltpu.SemaphoreType.DMA((2, 9))],
        compiler_params=pltpu.CompilerParams(vmem_limit_bytes=56 * MIB),
    )(sum_a, sum_b)


def solution(mesh):
    def block_step(image, w_first, w_down, grad_out):
        block_out, grad_image, sum_down, sum_first, _ = block_call(image[0], grad_out[0], w_first.reshape(9, C, C), w_down.reshape(9, C, C))
        grad_w_down, grad_w_first = settle(sum_down, sum_first)
        return (block_out.reshape(1, OUT_R, OUT_C, C), grad_image.reshape(1, ROWS, COLS, C),
                grad_w_first.reshape(3, 3, C, C), grad_w_down.reshape(3, 3, C, C))

    img_spec = P(None, 'h', 'w', None)
    return jax.shard_map(block_step, mesh=mesh, in_specs=(img_spec, P(), P(), img_spec), out_specs=(img_spec, img_spec, P(), P()), check_vma=False)
```

```python
import jax
import jax.numpy as jnp
from jax import lax
from jax.sharding import PartitionSpec as P
from jax.experimental import pallas as pl
from jax.experimental.pallas import tpu as pltpu

MESH = pl.DeviceIdType.MESH
F32, BF16 = jnp.float32, jnp.bfloat16
C = 640
ROWS, COLS = 24, 48
OUT_R, OUT_C = 12, 24
PIX, OPIX = ROWS * COLS, OUT_R * OUT_C
HALF = 320
MIB = 2 ** 20
OWN_SPACE = 50462720
ORDERS = (('x', 'y', 'z'), ('y', 'z', 'x'), ('z', 'x', 'y'))
R1, R2, R3, A1, A2, A3A, A3B, DA, DB, DC = range(10)
QUARTER = HALF // 2
EIGHTH = QUARTER // 2
LEAST = EIGHTH // 2
LAND_AT = (0, QUARTER, QUARTER + EIGHTH)
LANES = range(C // 128)
TAPS = [(t, t // 3, t % 3) for t in range(9)]
THIRDS = range(3)


def gelu_tanh(values):
    return jax.nn.gelu(values, approximate=True)


def dot(lhs, rhs):
    return lax.dot_general(lhs, rhs, (((1,), (0,)), ((), ())), preferred_element_type=F32)


def dot_rhs_t(lhs, rhs):
    return lax.dot_general(lhs, rhs, (((1,), (1,)), ((), ())), preferred_element_type=F32)


def dot_lhs_t(lhs, rhs):
    return lax.dot_general(lhs, rhs, (((0,), (0,)), ((), ())), preferred_element_type=F32)


ANY = pl.BlockSpec(memory_space=pl.ANY)


def place():
    w, h = lax.axis_index('w'), lax.axis_index('h')
    bit = {'x': h // 2, 'c': h % 2, 'y': w % 2, 'z': w // 2}
    dev = {'x': (w, (h + 2) % 4), 'c': (w, h + 1 - 2 * (h % 2)), 'y': (w + 1 - 2 * (w % 2), h), 'z': ((w + 2) % 4, h)}
    return bit, dev


class Reducer:
    def __init__(self, index, own, land, out, sems, grants, bit, dev):
        self.index, self.own, self.land, self.out, self.sems, self.grants, self.bit, self.dev = index, own, land, out, sems, grants, bit, dev

    def starts(self, third):
        b = [self.bit[axis] for axis in ORDERS[third]]
        base2 = b[0] * QUARTER
        base3 = base2 + b[1] * EIGHTH
        return b, base2, base3, base3 + b[2] * LEAST

    def copy(self, third, kind):
        (b0, b1, b2), base2, base3, base4 = self.starts(third)
        axis0, axis1, axis2 = ORDERS[third]
        far = (1 - b0) * QUARTER
        near1, far1 = b1 * EIGHTH, (1 - b1) * EIGHTH
        src, size, axis = {
            R1: (far, QUARTER, axis0), R2: (base2 + far1, EIGHTH, axis1), R3: (base3 + (1 - b2) * LEAST, LEAST, axis2),
            A1: (base4, LEAST, axis2), A2: (base3, EIGHTH, axis1), A3A: (base3, EIGHTH, axis0), A3B: (base2 + far1, EIGHTH, axis0),
            DA: (base2, QUARTER, 'c'), DB: (far + near1, EIGHTH, 'c'), DC: (far + far1, EIGHTH, 'c'),
        }[kind]
        rows = pl.ds(pl.multiple_of(src, 8), size)
        units = pl.ds(3 * third, 3)
        source = self.own.at[pl.ds(self.bit['c'] + 3 * third, 3), rows]
        send, recv = (s.at[self.index, third, kind] for s in self.sems)
        if kind <= R3:
            target = self.land.at[units, pl.ds(LAND_AT[kind], size)]
        elif kind <= A3B:
            target = source
        else:
            target = self.out.at[units, rows]
        return pltpu.make_async_remote_copy(src_ref=source, dst_ref=target, send_sem=send, recv_sem=recv, device_id=self.dev[axis], device_id_type=MESH)

    def add(self, third, kind):
        _, base2, base3, base4 = self.starts(third)
        keep, size = ((base2, QUARTER), (base3, EIGHTH), (base4, LEAST))[kind]
        steps = size // LEAST

        def body(j):
            unit, row = 3 * third + j // steps, (j % steps) * LEAST
            rows = pl.ds(pl.multiple_of(keep + row, 8), LEAST)
            self.own[self.bit['c'] + unit, rows, :] += self.land[unit, pl.ds(pl.multiple_of(LAND_AT[kind] + row, 8), LEAST), :]
        run(3 * steps, body)

    def begin(self):
        for third in THIRDS:
            self.copy(third, R1).start()

    def move(self, wait_for, then, add=False):
        for third in THIRDS:
            self.copy(third, wait_for).wait()
            if add:
                pl.semaphore_signal(self.grants.at[self.index, third, wait_for], inc=1, device_id=self.dev[ORDERS[third][wait_for]], device_id_type=MESH)
                self.add(third, wait_for)
            for kind in then:
                if kind in (A1, A2, A3A):
                    pl.semaphore_wait(self.grants.at[self.index, third, {A1: R3, A2: R2, A3A: R1}[kind]], 1)
                self.copy(third, kind).start()

    def finish(self):
        for kind in (DA, DB, DC):
            self.move(kind, ())


EDGE = 8
LINES = (ROWS + 2) * COLS
BLOCK = 8 * COLS
NEAR = [(dw, dh) for dw in (-1, 0, 1) for dh in (-1, 0, 1) if (dw, dh) != (0, 0)]
ABOVE = [(-1, -1), (-1, 0), (0, -1)]
BELOW = [(1, 1), (1, 0), (0, 1)]
G_AT, G_PAIR_AT, TAP_PAIR_AT = 3 * OPIX, 4 * OPIX, 5 * OPIX


def lane(k):
    return slice(k * 128, k * 128 + 128)


def run(steps, body):
    lax.fori_loop(0, steps, lambda i, _: body(i), None)


def clear_of(flag, value):
    return jnp.where(flag, 0.0, value)


def at(start, size):
    return pl.ds(pl.multiple_of(start, size), size)


class Border:
    def __init__(self, grid, row0, rows, cols, send, land, sems, send_to, take_from):
        self.grid, self.row0, self.rows, self.cols, self.sends, self.lands = grid, row0, rows, cols, send, land
        self.sems, self.send_to, self.take_from = sems, send_to, take_from
        self.w, self.h = lax.axis_index('w'), lax.axis_index('h')

    def edge(self, step, first, size, outside):
        return {-1: first - outside, 1: first + size - 1 + outside}[step]

    def copies(self):
        found = []
        for dw, dh in self.send_to:
            i = NEAR.index((dw, dh))
            if dw == 0:
                src, dst = self.sends[0].at[(dh + 1) // 2], self.lands[0].at[(1 - dh) // 2]
            elif dh == 0:
                src, dst = self.sends[1].at[(dw + 1) // 2], self.lands[1].at[(1 - dw) // 2]
            else:
                src = self.sends[2].at[2 * ((dh + 1) // 2) + (dw + 1) // 2]
                dst = self.lands[2].at[2 * ((1 - dh) // 2) + (1 - dw) // 2]
            peer = ((self.w + dw + 4) % 4, (self.h + dh + 4) % 4)
            found.append(pltpu.make_async_remote_copy(src_ref=src, dst_ref=dst, send_sem=self.sems.at[0, i], recv_sem=self.sems.at[1, i], device_id=peer, device_id_type=MESH))
        return found

    def start(self):
        grid, row0, rows, cols = self.grid, self.row0, self.rows, self.cols
        for dw, dh in self.send_to:
            r = None if dh == 0 else self.edge(dh, row0, rows, 0)
            c = None if dw == 0 else self.edge(dw, EDGE, cols, 0)
            for k in LANES:
                if dw == 0:
                    self.sends[0][(dh + 1) // 2, :, lane(k)] = grid[k, r, EDGE:EDGE + cols, :]
                elif dh == 0:
                    for row in range(rows):
                        self.sends[1][(dw + 1) // 2, row:row + 1, lane(k)] = grid[k, row0 + row, c:c + 1, :]
                else:
                    self.sends[2][2 * ((dh + 1) // 2) + (dw + 1) // 2, :, lane(k)] = jnp.broadcast_to(grid[k, r, c:c + 1, :], (8, 128))
        for copy in self.copies():
            copy.start()

    def finish(self):
        grid, row0, rows, cols = self.grid, self.row0, self.rows, self.cols
        for copy in self.copies():
            copy.wait()
        for dw, dh in self.take_from:
            r = None if dh == 0 else self.edge(dh, row0, rows, 1)
            c = None if dw == 0 else self.edge(dw, EDGE, cols, 1)
            out_w = {-1: self.w == 0, 0: False, 1: self.w == 3}[dw]
            out_h = {-1: self.h == 0, 0: False, 1: self.h == 3}[dh]
            for k in LANES:
                if dw == 0:
                    grid[k, r, EDGE:EDGE + cols, :] = clear_of(out_h, self.lands[0][(dh + 1) // 2, :, lane(k)])
                elif dh == 0:
                    for row in range(rows):
                        grid[k, row0 + row, c:c + 1, :] = clear_of(out_w, self.lands[1][(dw + 1) // 2, row:row + 1, lane(k)])
                else:
                    out = jnp.logical_or(out_w, out_h)
                    grid[k, r, c:c + 1, :] = clear_of(out, self.lands[2][2 * ((dh + 1) // 2) + (dw + 1) // 2, 0:1, lane(k)])


def spread(grid, xs):
    def one_row(r):
        for c in range(3):
            for k in LANES:
                xs[0, at(c * LINES + r * COLS, COLS), lane(k)] = grid[k, r, EDGE - 1 + c:EDGE - 1 + c + COLS, :].astype(BF16)
    run(ROWS + 2, one_row)


def accumulate(acc, rows, part, first):
    for k in LANES:
        piece = part[:, lane(k)]
        acc[k, 0:rows, :] = piece if first else acc[k, 0:rows, :] + piece


def block_kernel(x_in, g_in, w_first, w_down, y_out, dx_out, own_d, own_f, o_down, o_first, x_land,
                 land_d, land_f, wbuf, xs, taps, g_tile, g_grid, da, da_pair, grid, acc,
                 send_r, send_c, send_k, x_r, x_c, x_k, z_r, z_c, z_k, d_r, d_c, d_k, gs_r, gs_c, gs_k, gl_r, gl_c, gl_k,
                 load_sems, pair_sems, near_sems, out_sems, send_sems, recv_sems, grants):
    bit, dev = place()
    w, h = lax.axis_index('w'), lax.axis_index('h')
    core = bit['c']
    x_tile = xs.at[0, pl.ds(0, PIX)]
    load_x = pltpu.make_async_copy(x_in, x_tile, load_sems.at[0])
    load_g = pltpu.make_async_copy(g_in, g_tile, load_sems.at[1])
    load_w = pltpu.make_async_copy(w_first, wbuf, load_sems.at[2])
    for load in (load_x, load_g, load_w):
        load.start()
    barrier = pltpu.get_barrier_semaphore()
    for axis in 'xyzc':
        pl.semaphore_signal(barrier, inc=1, device_id=dev[axis], device_id_type=MESH)
    for dw, dh in NEAR:
        pl.semaphore_signal(barrier, inc=1, device_id=((w + dw + 4) % 4, (h + dh + 4) % 4), device_id_type=MESH)
    sends = (send_r, send_c, send_k)
    x_border = Border(grid, 1, ROWS, COLS, sends, (x_r, x_c, x_k), near_sems.at[0], NEAR, NEAR)
    z_border = Border(grid, 0, ROWS, COLS, sends, (z_r, z_c, z_k), near_sems.at[1], ABOVE, BELOW)
    d_border = Border(grid, 1, ROWS, COLS, sends, (d_r, d_c, d_k), near_sems.at[2], NEAR, NEAR)
    g_border = Border(g_grid, 1, OUT_R, OUT_C, (gs_r, gs_c, gs_k), (gl_r, gl_c, gl_k), near_sems.at[3], BELOW, ABOVE)
    sems = (send_sems, recv_sems)
    down = Reducer(0, own_d, land_d, o_down, sems, grants, bit, dev)
    first = Reducer(1, own_f, land_f, o_first, sems, grants, bit, dev)

    def to_pair(src, dst, i):
        return pltpu.make_async_remote_copy(src_ref=src, dst_ref=dst, send_sem=pair_sems.at[0, i], recv_sem=pair_sems.at[1, i], device_id=dev['c'], device_id_type=MESH)

    load_x.wait()

    def place_row(r):
        for k in LANES:
            grid[k, r + 1, EDGE:EDGE + COLS, :] = x_tile[at(r * COLS, COLS), lane(k)].astype(F32)
    run(ROWS, place_row)
    pl.semaphore_wait(barrier, 12)
    x_border.start()
    load_g.wait()
    for r in range(OUT_R):
        for k in LANES:
            g_grid[k, r + 1, EDGE:EDGE + OUT_C, :] = g_tile[r, :, lane(k)].astype(F32)
    g_border.start()
    x_border.finish()
    spread(grid, xs)
    x_share = to_pair(xs.at[0], x_land, 0)
    x_share.start()
    load_w.wait()

    def pre_rows(i):
        for t, a, c in TAPS:
            rows = pl.ds(pl.multiple_of(c * LINES + i * BLOCK + a * COLS, COLS), BLOCK)
            accumulate(acc, BLOCK, dot(xs[0, rows, :], wbuf[t]), t == 0)
        for k in LANES:
            pre = acc[k].astype(BF16).astype(F32)
            acc[k] = pre
            act = gelu_tanh(pre).astype(BF16).astype(F32)
            for r in range(8):
                grid[k, 8 * i + r, EDGE:EDGE + COLS, :] = act[r * COLS:(r + 1) * COLS]
        for r in range(8):
            for cp in range(2):
                for k in LANES:
                    own_f[2 * (r % 2) + cp, pl.ds(pl.multiple_of((4 * i + r // 2) * OUT_C, 8), OUT_C), lane(k)] = acc[k, pl.ds(r * COLS + cp, OUT_C, stride=2), :]
    run(3, pre_rows)
    load_w2 = pltpu.make_async_copy(w_down, wbuf, load_sems.at[3])
    load_w2.start()
    z_border.start()

    g_border.finish()
    for di in range(2):
        for dj in range(2):
            for k in LANES:
                part = g_grid[k, di:di + OUT_R, EDGE - 1 + dj:EDGE - 1 + dj + OUT_C, :]
                xs[1, (2 * di + dj) * OPIX:(2 * di + dj + 1) * OPIX, lane(k)] = part.reshape(OPIX, 128).astype(BF16)
    g_share = to_pair(xs.at[1, pl.ds(G_AT, OPIX)], xs.at[1, pl.ds(G_PAIR_AT, OPIX)], 1)
    g_share.start()
    z_border.finish()

    def tap_rows(p):
        for t, a, c in TAPS:
            for k in LANES:
                cols = pl.ds(EDGE + c, OUT_C, stride=2)
                two = jnp.concatenate([grid[k, 4 * p + a, cols, :], grid[k, 4 * p + 2 + a, cols, :]], 0)
                taps[t, at(p * 2 * OUT_C, 2 * OUT_C), lane(k)] = two.astype(BF16)
    run(OUT_R // 2, tap_rows)
    tap_shares = [to_pair(taps.at[4 * (1 - core) + j], xs.at[1, pl.ds(TAP_PAIR_AT + j * OPIX, OPIX)], 2 + j) for j in range(5)]
    for share in tap_shares:
        share.start()

    def down_tap(j):
        res = dot_lhs_t(taps[4 * core + j], xs[1, G_AT:G_AT + OPIX, :])
        own_d[2 * j] = res[:HALF]
        own_d[2 * j + 1] = res[HALF:]
    run(5, down_tap)
    g_share.wait()
    for share in tap_shares:
        share.wait()

    def down_tap_pair(j):
        rows = pl.ds(pl.multiple_of(TAP_PAIR_AT + j * OPIX, 32), OPIX)
        res = dot_lhs_t(xs[1, rows, :], xs[1, G_PAIR_AT:G_PAIR_AT + OPIX, :])
        own_d[2 * j] += res[:HALF]
        own_d[2 * j + 1] += res[HALF:]
    run(5, down_tap_pair)
    down.begin()

    load_w2.wait()
    for rp in range(2):
        for cp in range(2):
            total = None
            for a in ((0, 2), (1,))[rp]:
                for c in ((0, 2), (1,))[cp]:
                    row = (2 * (1 - a // 2) + 1 - c // 2) * OPIX
                    part = dot_rhs_t(xs[1, row:row + OPIX, :], wbuf[3 * a + c])
                    total = part if total is None else total + part
            pre = own_f[2 * rp + cp, 0:OPIX, :]
            grad = jax.vjp(gelu_tanh, pre)[1](total)[0].astype(BF16).astype(F32)
            for i in range(OUT_R):
                for k in LANES:
                    grid[k, 2 * i + rp + 1, pl.ds(EDGE + cp, OUT_C, stride=2), :] = grad[i * OUT_C:(i + 1) * OUT_C, lane(k)]

    def pack(r):
        for k in LANES:
            da[at(r * COLS, COLS), lane(k)] = grid[k, r + 1, EDGE:EDGE + COLS, :].astype(BF16)
    run(ROWS, pack)
    da_share = to_pair(da, da_pair, 7)
    da_share.start()
    d_border.start()
    x_share.wait()
    pair_load = pltpu.make_async_copy(x_land, xs.at[1], load_sems.at[4])
    pair_load.start()

    for t in range(9):
        accumulate(acc, OPIX, dot(taps[t], wbuf[t]), t == 0)
    for k in LANES:
        taps[0, :, lane(k)] = acc[k, 0:OPIX, :].astype(BF16)
    y_copy = pltpu.make_async_copy(taps.at[0], y_out, out_sems.at[0])
    y_copy.start()
    load_w1 = pltpu.make_async_copy(w_first, wbuf, load_sems.at[5])
    load_w1.start()
    pair_load.wait()
    da_share.wait()

    def first_tap(j):
        t = 4 * core + j
        a, c = t // 3, t % 3
        rows = pl.ds(pl.multiple_of(c * LINES + a * COLS, COLS), PIX)
        res = dot_lhs_t(xs[0, rows, :], da[...]) + dot_lhs_t(xs[1, rows, :], da_pair[...])
        own_f[2 * j] = res[:HALF]
        own_f[2 * j + 1] = res[HALF:]
    run(4, first_tap)
    down.move(R1, (R2,), add=True)
    first_tap(4)
    first.begin()

    d_border.finish()
    spread(grid, xs)
    load_w1.wait()

    def image_rows(i):
        for t, a, c in TAPS:
            rows = pl.ds(pl.multiple_of((2 - c) * LINES + i * BLOCK + (2 - a) * COLS, COLS), BLOCK)
            accumulate(acc, BLOCK, dot_rhs_t(xs[0, rows, :], wbuf[t]), t == 0)
        for k in LANES:
            da_pair[at(i * BLOCK, BLOCK), lane(k)] = acc[k].astype(BF16)
    run(3, image_rows)
    dx_copy = pltpu.make_async_copy(da_pair, dx_out, out_sems.at[1])
    dx_copy.start()

    down.move(R2, (R3,), add=True)
    first.move(R1, (R2,), add=True)
    down.move(R3, (A1,), add=True)
    first.move(R2, (R3,), add=True)
    down.move(A1, (A2, A3A))
    first.move(R3, (A1,), add=True)
    down.move(A2, (A3B, DA))
    first.move(A1, (A2, A3A))
    down.move(A3A, (DB,))
    first.move(A2, (A3B, DA))
    down.move(A3B, (DC,))
    first.move(A3A, (DB,))
    first.move(A3B, (DC,))
    y_copy.wait()
    dx_copy.wait()
    down.finish()
    first.finish()


def block_call(image, grad_out, w_first, w_down):
    total = jax.ShapeDtypeStruct((9, HALF, C), F32)
    kept = pltpu.VMEM((10, HALF, C), F32)
    dma = pltpu.SemaphoreType.DMA
    edges = [pltpu.VMEM((2, COLS, C), F32), pltpu.VMEM((2, ROWS, C), F32), pltpu.VMEM((4, 8, C), F32)]
    small = [pltpu.VMEM((2, OUT_C, C), F32), pltpu.VMEM((2, OUT_R, C), F32), pltpu.VMEM((4, 8, C), F32)]
    return pl.pallas_call(
        block_kernel,
        out_shape=[jax.ShapeDtypeStruct((OPIX, C), BF16), jax.ShapeDtypeStruct((PIX, C), BF16), kept, kept, total, total,
                   jax.ShapeDtypeStruct((3 * LINES, C), BF16)],
        in_specs=[ANY] * 4, out_specs=[ANY] * 2 + [pl.BlockSpec(memory_space=pltpu.VMEM)] * 2 + [ANY] * 3,
        scratch_shapes=[pltpu.VMEM((9, 280, C), F32)] * 2
        + [pltpu.VMEM((9, C, C), BF16), pltpu.VMEM((2, 3 * LINES, C), BF16), pltpu.VMEM((9, OPIX, C), BF16)]
        + [pltpu.VMEM((OUT_R, OUT_C, C), BF16), pltpu.VMEM((5, OUT_R + 1, OUT_C + EDGE, 128), F32)]
        + [pltpu.VMEM((PIX, C), BF16)] * 2
        + [pltpu.VMEM((5, ROWS + 2, COLS + 2 * EDGE, 128), F32), pltpu.VMEM((5, BLOCK, 128), F32)]
        + edges * 4 + small * 2
        + [dma((6,)), dma((2, 8)), dma((4, 2, 8)), dma((2,)), dma((2, 3, 10)), dma((2, 3, 10)), pltpu.SemaphoreType.REGULAR((2, 3, 3))],
        compiler_params=pltpu.CompilerParams(collective_id=1, has_side_effects=True, vmem_limit_bytes=OWN_SPACE),
        cost_estimate=pl.CostEstimate(flops=2 * PIX * 90 * C * C, bytes_accessed=64 * MIB, transcendentals=0),
    )(image.reshape(PIX, C), grad_out, w_first, w_down)


def settle_kernel(y_in, dx_in, own_d, own_f, pair_d, pair_f, y_out, dx_out, down_out, first_out, y_buf, dx_buf, buf, load_sems, store_sems):
    core = lax.axis_index('h') % 2
    loads, stores = [], []
    for i, (src, via, dst) in enumerate(((y_in, y_buf, y_out), (dx_in, dx_buf, dx_out))):
        loads.append(pltpu.make_async_copy(src, via, load_sems.at[2, i]))
        stores.append(pltpu.make_async_copy(via, dst, store_sems.at[2, i]))
    kept = []
    for i, (own, pair, out) in enumerate(((own_d, pair_d, down_out), (own_f, pair_f, first_out))):
        kept.append(pltpu.make_async_copy(own.at[pl.ds(core, 9)], out.at[pl.ds(9 * core, 9)], store_sems.at[i, 9]))
        for part in range(9):
            loads.append(pltpu.make_async_copy(pair.at[part], buf.at[i, part], load_sems.at[i, part]))
            stores.append(pltpu.make_async_copy(buf.at[i, part], out.at[9 * (1 - core) + part], store_sems.at[i, part]))
    for copy in loads + kept:
        copy.start()
    for load, store in zip(loads, stores):
        load.wait()
        store.start()
    for copy in kept + stores:
        copy.wait()


def settle(*made):
    total = jax.ShapeDtypeStruct((18, HALF, C), F32)
    dma = pltpu.SemaphoreType.DMA
    return pl.pallas_call(
        settle_kernel, out_shape=[jax.ShapeDtypeStruct((OPIX, C), BF16), jax.ShapeDtypeStruct((PIX, C), BF16), total, total],
        in_specs=[pl.BlockSpec(memory_space=pltpu.HBM)] * 2 + [pl.BlockSpec(memory_space=pltpu.VMEM)] * 2 + [pl.BlockSpec(memory_space=pltpu.HBM)] * 2,
        out_specs=[ANY] * 4,
        scratch_shapes=[pltpu.VMEM((OPIX, C), BF16), pltpu.VMEM((PIX, C), BF16), pltpu.VMEM((2, 9, HALF, C), F32), dma((3, 9)), dma((3, 10))],
        compiler_params=pltpu.CompilerParams(vmem_limit_bytes=OWN_SPACE),
    )(*made[:2], *(pltpu.with_memory_space_constraint(own, pltpu.VMEM) for own in made[2:4]), *made[4:])


def solution(mesh):
    def block_step(image, w_first, w_down, grad_out):
        made = block_call(image[0], grad_out[0], w_first.reshape(9, C, C), w_down.reshape(9, C, C))
        block_out, grad_image, grad_w_down, grad_w_first = settle(*made[:6])
        return (block_out.reshape(1, OUT_R, OUT_C, C), grad_image.reshape(1, ROWS, COLS, C),
                grad_w_first.reshape(3, 3, C, C), grad_w_down.reshape(3, 3, C, C))

    img_spec = P(None, 'h', 'w', None)
    return jax.shard_map(block_step, mesh=mesh, in_specs=(img_spec, P(), P(), img_spec), out_specs=(img_spec, img_spec, P(), P()), check_vma=False)
```

```python
import jax
import jax.numpy as jnp
from jax import lax
from jax.sharding import PartitionSpec as P
from jax.experimental import pallas as pl
from jax.experimental.pallas import tpu as pltpu

MESH = pl.DeviceIdType.MESH
F32, BF16 = jnp.float32, jnp.bfloat16
C = 640
ROWS, COLS = 24, 48
OUT_R, OUT_C = 12, 24
PIX, OPIX = ROWS * COLS, OUT_R * OUT_C
HALF = 320
MIB = 2 ** 20
SCRATCH = 36000000
ORDERS = (('x', 'y', 'z'), ('y', 'z', 'x'), ('z', 'x', 'y'))
R1, R2, R3, A1, A2, A3A, A3B, DA, DB, DC = range(10)
QUARTER = HALF // 2
EIGHTH = QUARTER // 2
LEAST = EIGHTH // 2
LAND_AT = (0, QUARTER, QUARTER + EIGHTH)
LANES = range(C // 128)
TAPS = [(t, t // 3, t % 3) for t in range(9)]
THIRDS = range(3)


def gelu_tanh(values):
    return jax.nn.gelu(values, approximate=True)


def dot(lhs, rhs):
    return lax.dot_general(lhs, rhs, (((1,), (0,)), ((), ())), preferred_element_type=F32)


def dot_rhs_t(lhs, rhs):
    return lax.dot_general(lhs, rhs, (((1,), (1,)), ((), ())), preferred_element_type=F32)


def dot_lhs_t(lhs, rhs):
    return lax.dot_general(lhs, rhs, (((0,), (0,)), ((), ())), preferred_element_type=F32)


ANY = pl.BlockSpec(memory_space=pl.ANY)
VM = pl.BlockSpec(memory_space=pltpu.VMEM)


def place():
    w, h = lax.axis_index('w'), lax.axis_index('h')
    bit = {'x': h // 2, 'c': h % 2, 'y': w % 2, 'z': w // 2}
    dev = {'x': (w, (h + 2) % 4), 'c': (w, h + 1 - 2 * (h % 2)), 'y': (w + 1 - 2 * (w % 2), h), 'z': ((w + 2) % 4, h)}
    return bit, dev


class Reducer:
    def __init__(self, index, own, pair, sems, grants, bit, dev):
        self.index, self.own, self.pair, self.sems, self.grants, self.bit, self.dev = index, own, pair, sems, grants, bit, dev

    def starts(self, third):
        b = [self.bit[axis] for axis in ORDERS[third]]
        base2 = b[0] * QUARTER
        base3 = base2 + b[1] * EIGHTH
        return b, base2, base3, base3 + b[2] * LEAST

    def copy(self, third, kind):
        (b0, b1, b2), base2, base3, base4 = self.starts(third)
        axis0, axis1, axis2 = ORDERS[third]
        far = (1 - b0) * QUARTER
        near1, far1 = b1 * EIGHTH, (1 - b1) * EIGHTH
        src, size, axis = {
            R1: (far, QUARTER, axis0), R2: (base2 + far1, EIGHTH, axis1), R3: (base3 + (1 - b2) * LEAST, LEAST, axis2),
            A1: (base4, LEAST, axis2), A2: (base3, EIGHTH, axis1), A3A: (base3, EIGHTH, axis0), A3B: (base2 + far1, EIGHTH, axis0),
            DA: (base2, QUARTER, 'c'), DB: (far + near1, EIGHTH, 'c'), DC: (far + far1, EIGHTH, 'c'),
        }[kind]
        rows = pl.ds(pl.multiple_of(src, 8), size)
        units = pl.ds(3 * third, 3)
        source = self.own.at[units, rows]
        send, recv = (s.at[self.index, third, kind] for s in self.sems)
        if kind <= R3:
            target = self.pair.at[units, pl.ds(LAND_AT[kind], size)]
        elif kind <= A3B:
            target = source
        else:
            target = self.pair.at[units, rows]
        return pltpu.make_async_remote_copy(src_ref=source, dst_ref=target, send_sem=send, recv_sem=recv, device_id=self.dev[axis], device_id_type=MESH)

    def add(self, third, kind):
        _, base2, base3, base4 = self.starts(third)
        keep, size = ((base2, QUARTER), (base3, EIGHTH), (base4, LEAST))[kind]
        steps = size // LEAST

        def body(j):
            unit, row = 3 * third + j // steps, (j % steps) * LEAST
            rows = pl.ds(pl.multiple_of(keep + row, 8), LEAST)
            self.own[unit, rows, :] += self.pair[unit, pl.ds(pl.multiple_of(LAND_AT[kind] + row, 8), LEAST), :]
        run(3 * steps, body)

    def begin(self):
        for third in THIRDS:
            self.copy(third, R1).start()

    def move(self, wait_for, then, add=False):
        for third in THIRDS:
            self.copy(third, wait_for).wait()
            if add:
                pl.semaphore_signal(self.grants.at[self.index, third, wait_for], inc=1, device_id=self.dev[ORDERS[third][wait_for]], device_id_type=MESH)
                self.add(third, wait_for)
            if wait_for == R3 and third == THIRDS[-1]:
                pl.semaphore_signal(self.grants.at[self.index, 0, 3], inc=1, device_id=self.dev['c'], device_id_type=MESH)
            for kind in then:
                if kind == DA and third == 0:
                    pl.semaphore_wait(self.grants.at[self.index, 0, 3], 1)
                if kind in (A1, A2, A3A):
                    pl.semaphore_wait(self.grants.at[self.index, third, {A1: R3, A2: R2, A3A: R1}[kind]], 1)
                self.copy(third, kind).start()

    def finish(self):
        for kind in (DA, DB, DC):
            self.move(kind, ())


EDGE = 8
LINES = (ROWS + 2) * COLS
BLOCK_ROWS = 6
BLOCK = BLOCK_ROWS * COLS
NEAR = [(dw, dh) for dw in (-1, 0, 1) for dh in (-1, 0, 1) if (dw, dh) != (0, 0)]
ABOVE = [(-1, -1), (-1, 0), (0, -1)]
BELOW = [(1, 1), (1, 0), (0, 1)]
G_AT, G_PAIR_AT, TAP_PAIR_AT = 3 * OPIX, 4 * OPIX, 5 * OPIX


def lane(k):
    return slice(k * 128, k * 128 + 128)


def run(steps, body):
    lax.fori_loop(0, steps, lambda i, _: body(i), None)


def clear_of(flag, value):
    return jnp.where(flag, 0.0, value)


def at(start, size):
    return pl.ds(pl.multiple_of(start, size), size)


class Border:
    def __init__(self, grid, row0, rows, cols, send, land, sems, send_to, take_from):
        self.grid, self.row0, self.rows, self.cols, self.sends, self.lands = grid, row0, rows, cols, send, land
        self.sems, self.send_to, self.take_from = sems, send_to, take_from
        self.w, self.h = lax.axis_index('w'), lax.axis_index('h')

    def edge(self, step, first, size, outside):
        return {-1: first - outside, 1: first + size - 1 + outside}[step]

    def copies(self):
        found = []
        for dw, dh in self.send_to:
            i = NEAR.index((dw, dh))
            if dw == 0:
                src, dst = self.sends[0].at[(dh + 1) // 2], self.lands[0].at[(1 - dh) // 2]
            elif dh == 0:
                src, dst = self.sends[1].at[(dw + 1) // 2], self.lands[1].at[(1 - dw) // 2]
            else:
                src = self.sends[2].at[2 * ((dh + 1) // 2) + (dw + 1) // 2]
                dst = self.lands[2].at[2 * ((1 - dh) // 2) + (1 - dw) // 2]
            peer = ((self.w + dw + 4) % 4, (self.h + dh + 4) % 4)
            found.append(pltpu.make_async_remote_copy(src_ref=src, dst_ref=dst, send_sem=self.sems.at[0, i], recv_sem=self.sems.at[1, i], device_id=peer, device_id_type=MESH))
        return found

    def start(self):
        grid, row0, rows, cols = self.grid, self.row0, self.rows, self.cols
        for dw, dh in self.send_to:
            r = None if dh == 0 else self.edge(dh, row0, rows, 0)
            c = None if dw == 0 else self.edge(dw, EDGE, cols, 0)
            for k in LANES:
                if dw == 0:
                    self.sends[0][(dh + 1) // 2, :, lane(k)] = grid[k, r, EDGE:EDGE + cols, :]
                elif dh == 0:
                    for row in range(rows):
                        self.sends[1][(dw + 1) // 2, row:row + 1, lane(k)] = grid[k, row0 + row, c:c + 1, :]
                else:
                    self.sends[2][2 * ((dh + 1) // 2) + (dw + 1) // 2, :, lane(k)] = jnp.broadcast_to(grid[k, r, c:c + 1, :], (8, 128))
        for copy in self.copies():
            copy.start()

    def finish(self):
        grid, row0, rows, cols = self.grid, self.row0, self.rows, self.cols
        for copy in self.copies():
            copy.wait()
        for dw, dh in self.take_from:
            r = None if dh == 0 else self.edge(dh, row0, rows, 1)
            c = None if dw == 0 else self.edge(dw, EDGE, cols, 1)
            out_w = {-1: self.w == 0, 0: False, 1: self.w == 3}[dw]
            out_h = {-1: self.h == 0, 0: False, 1: self.h == 3}[dh]
            for k in LANES:
                if dw == 0:
                    grid[k, r, EDGE:EDGE + cols, :] = clear_of(out_h, self.lands[0][(dh + 1) // 2, :, lane(k)])
                elif dh == 0:
                    for row in range(rows):
                        grid[k, row0 + row, c:c + 1, :] = clear_of(out_w, self.lands[1][(dw + 1) // 2, row:row + 1, lane(k)])
                else:
                    out = jnp.logical_or(out_w, out_h)
                    grid[k, r, c:c + 1, :] = clear_of(out, self.lands[2][2 * ((dh + 1) // 2) + (dw + 1) // 2, 0:1, lane(k)])


def spread(grid, xs):
    def one_row(r):
        for c in range(3):
            for k in LANES:
                xs[0, at(c * LINES + r * COLS, COLS), lane(k)] = grid[k, r, EDGE - 1 + c:EDGE - 1 + c + COLS, :].astype(BF16)
    run(ROWS + 2, one_row)


def accumulate(acc, rows, part, first):
    for k in LANES:
        piece = part[:, lane(k)]
        acc[k, 0:rows, :] = piece if first else acc[k, 0:rows, :] + piece


def block_kernel(x_in, g_in, w_first, w_down, y_out, da_pair, own_d, own_f, other_d, other_f, x_land,
                 wbuf, xs, taps, g_tile, g_grid, da, grid, acc,
                 send_r, send_c, send_k, x_r, x_c, x_k, z_r, z_c, z_k, d_r, d_c, d_k, gs_r, gs_c, gs_k, gl_r, gl_c, gl_k,
                 load_sems, pair_sems, near_sems, out_sems, send_sems, recv_sems, grants):
    bit, dev = place()
    w, h = lax.axis_index('w'), lax.axis_index('h')
    core = bit['c']
    x_tile = xs.at[0, pl.ds(0, PIX)]
    load_x = pltpu.make_async_copy(x_in, x_tile, load_sems.at[0])
    load_g = pltpu.make_async_copy(g_in, g_tile, load_sems.at[1])
    load_w = pltpu.make_async_copy(w_first, wbuf, load_sems.at[2])
    for load in (load_x, load_g, load_w):
        load.start()
    barrier = pltpu.get_barrier_semaphore()
    for axis in 'xyzc':
        pl.semaphore_signal(barrier, inc=1, device_id=dev[axis], device_id_type=MESH)
    for dw, dh in NEAR:
        pl.semaphore_signal(barrier, inc=1, device_id=((w + dw + 4) % 4, (h + dh + 4) % 4), device_id_type=MESH)
    sends = (send_r, send_c, send_k)
    x_border = Border(grid, 1, ROWS, COLS, sends, (x_r, x_c, x_k), near_sems.at[0], NEAR, NEAR)
    z_border = Border(grid, 0, ROWS, COLS, sends, (z_r, z_c, z_k), near_sems.at[1], ABOVE, BELOW)
    d_border = Border(grid, 1, ROWS, COLS, sends, (d_r, d_c, d_k), near_sems.at[2], NEAR, NEAR)
    g_border = Border(g_grid, 1, OUT_R, OUT_C, (gs_r, gs_c, gs_k), (gl_r, gl_c, gl_k), near_sems.at[3], BELOW, ABOVE)
    sems = (send_sems, recv_sems)
    down = Reducer(0, own_d, other_d, sems, grants, bit, dev)
    first = Reducer(1, own_f, other_f, sems, grants, bit, dev)

    def to_pair(src, dst, i):
        return pltpu.make_async_remote_copy(src_ref=src, dst_ref=dst, send_sem=pair_sems.at[0, i], recv_sem=pair_sems.at[1, i], device_id=dev['c'], device_id_type=MESH)

    def put(own, j, res, more):
        for side in range(2):
            unit = 2 * j + side - core
            part = res[side * HALF:(side + 1) * HALF]

            @pl.when(jnp.logical_and(unit >= 0, unit < 9))
            def _():
                own[unit] = own[unit] + part if more else part

    load_x.wait()

    def place_row(r):
        for k in LANES:
            grid[k, r + 1, EDGE:EDGE + COLS, :] = x_tile[at(r * COLS, COLS), lane(k)].astype(F32)
    run(ROWS, place_row)
    pl.semaphore_wait(barrier, 12)
    x_border.start()
    load_g.wait()
    for r in range(OUT_R):
        for k in LANES:
            g_grid[k, r + 1, EDGE:EDGE + OUT_C, :] = g_tile[r, :, lane(k)].astype(F32)
    g_border.start()
    x_border.finish()
    spread(grid, xs)
    x_share = to_pair(xs.at[0], x_land, 0)
    x_share.start()
    load_w.wait()

    def pre_rows(i):
        for t, a, c in TAPS:
            rows = pl.ds(pl.multiple_of(c * LINES + i * BLOCK + a * COLS, COLS), BLOCK)
            accumulate(acc, BLOCK, dot(xs[0, rows, :], wbuf[t]), t == 0)
        for k in LANES:
            pre = acc[k].astype(BF16).astype(F32)
            acc[k] = pre
            act = gelu_tanh(pre).astype(BF16).astype(F32)
            for r in range(BLOCK_ROWS):
                grid[k, BLOCK_ROWS * i + r, EDGE:EDGE + COLS, :] = act[r * COLS:(r + 1) * COLS]
        for r in range(BLOCK_ROWS):
            for cp in range(2):
                for k in LANES:
                    own_f[2 * (r % 2) + cp, pl.ds(pl.multiple_of((BLOCK_ROWS // 2 * i + r // 2) * OUT_C, 8), OUT_C), lane(k)] = acc[k, pl.ds(r * COLS + cp, OUT_C, stride=2), :]
    run(ROWS // BLOCK_ROWS, pre_rows)
    load_w2 = pltpu.make_async_copy(w_down, wbuf, load_sems.at[3])
    load_w2.start()
    z_border.start()

    g_border.finish()
    for di in range(2):
        for dj in range(2):
            for k in LANES:
                part = g_grid[k, di:di + OUT_R, EDGE - 1 + dj:EDGE - 1 + dj + OUT_C, :]
                xs[1, (2 * di + dj) * OPIX:(2 * di + dj + 1) * OPIX, lane(k)] = part.reshape(OPIX, 128).astype(BF16)
    g_share = to_pair(xs.at[1, pl.ds(G_AT, OPIX)], xs.at[1, pl.ds(G_PAIR_AT, OPIX)], 1)
    g_share.start()
    z_border.finish()

    def tap_rows(p):
        for t, a, c in TAPS:
            for k in LANES:
                cols = pl.ds(EDGE + c, OUT_C, stride=2)
                two = jnp.concatenate([grid[k, 4 * p + a, cols, :], grid[k, 4 * p + 2 + a, cols, :]], 0)
                taps[t, at(p * 2 * OUT_C, 2 * OUT_C), lane(k)] = two.astype(BF16)
    run(OUT_R // 2, tap_rows)
    tap_shares = [to_pair(taps.at[4 * (1 - core) + j], xs.at[1, pl.ds(TAP_PAIR_AT + j * OPIX, OPIX)], 2 + j) for j in range(5)]
    for share in tap_shares:
        share.start()

    def down_tap(j):
        res = dot_lhs_t(taps[4 * core + j], xs[1, G_AT:G_AT + OPIX, :])
        put(own_d, j, res, False)
    run(5, down_tap)
    g_share.wait()
    for share in tap_shares:
        share.wait()

    def down_tap_pair(j):
        rows = pl.ds(pl.multiple_of(TAP_PAIR_AT + j * OPIX, 32), OPIX)
        res = dot_lhs_t(xs[1, rows, :], xs[1, G_PAIR_AT:G_PAIR_AT + OPIX, :])
        put(own_d, j, res, True)
    run(5, down_tap_pair)
    down.begin()

    load_w2.wait()
    for rp in range(2):
        for cp in range(2):
            total = None
            for a in ((0, 2), (1,))[rp]:
                for c in ((0, 2), (1,))[cp]:
                    row = (2 * (1 - a // 2) + 1 - c // 2) * OPIX
                    part = dot_rhs_t(xs[1, row:row + OPIX, :], wbuf[3 * a + c])
                    total = part if total is None else total + part
            pre = own_f[2 * rp + cp, 0:OPIX, :]
            grad = jax.vjp(gelu_tanh, pre)[1](total)[0].astype(BF16).astype(F32)
            for i in range(OUT_R):
                for k in LANES:
                    grid[k, 2 * i + rp + 1, pl.ds(EDGE + cp, OUT_C, stride=2), :] = grad[i * OUT_C:(i + 1) * OUT_C, lane(k)]

    def pack(r):
        for k in LANES:
            da[at(r * COLS, COLS), lane(k)] = grid[k, r + 1, EDGE:EDGE + COLS, :].astype(BF16)
    run(ROWS, pack)
    da_share = to_pair(da, da_pair, 7)
    da_share.start()
    d_border.start()
    x_share.wait()
    pair_load = pltpu.make_async_copy(x_land, xs.at[1], load_sems.at[4])
    pair_load.start()

    for t in range(9):
        accumulate(acc, OPIX, dot(taps[t], wbuf[t]), t == 0)
    for k in LANES:
        taps[0, :, lane(k)] = acc[k, 0:OPIX, :].astype(BF16)
    y_copy = pltpu.make_async_copy(taps.at[0], y_out, out_sems.at[0])
    y_copy.start()
    load_w1 = pltpu.make_async_copy(w_first, wbuf, load_sems.at[5])
    load_w1.start()
    pair_load.wait()
    da_share.wait()

    def first_tap(j):
        t = 4 * core + j
        a, c = t // 3, t % 3
        rows = pl.ds(pl.multiple_of(c * LINES + a * COLS, COLS), PIX)
        res = dot_lhs_t(xs[0, rows, :], da[...]) + dot_lhs_t(xs[1, rows, :], da_pair[...])
        put(own_f, j, res, False)
    run(4, first_tap)
    down.move(R1, (R2,), add=True)
    first_tap(4)
    first.begin()

    d_border.finish()
    spread(grid, xs)
    load_w1.wait()

    def image_rows(i):
        for t, a, c in TAPS:
            rows = pl.ds(pl.multiple_of((2 - c) * LINES + i * BLOCK + (2 - a) * COLS, COLS), BLOCK)
            accumulate(acc, BLOCK, dot_rhs_t(xs[0, rows, :], wbuf[t]), t == 0)
        for k in LANES:
            da_pair[at(i * BLOCK, BLOCK), lane(k)] = acc[k].astype(BF16)
    run(ROWS // BLOCK_ROWS, image_rows)

    down.move(R2, (R3,), add=True)
    first.move(R1, (R2,), add=True)
    down.move(R3, (A1,), add=True)
    first.move(R2, (R3,), add=True)
    down.move(A1, (A2, A3A))
    first.move(R3, (A1,), add=True)
    down.move(A2, (A3B, DA))
    first.move(A1, (A2, A3A))
    down.move(A3A, (DB,))
    first.move(A2, (A3B, DA))
    down.move(A3B, (DC,))
    first.move(A3A, (DB,))
    first.move(A3B, (DC,))
    y_copy.wait()
    down.finish()
    first.finish()


def block_call(image, grad_out, w_first, w_down):
    kept = pltpu.VMEM((9, HALF, C), F32)
    dma = pltpu.SemaphoreType.DMA
    edges = [pltpu.VMEM((2, COLS, C), F32), pltpu.VMEM((2, ROWS, C), F32), pltpu.VMEM((4, 8, C), F32)]
    small = [pltpu.VMEM((2, OUT_C, C), F32), pltpu.VMEM((2, OUT_R, C), F32), pltpu.VMEM((4, 8, C), F32)]
    return pl.pallas_call(
        block_kernel,
        out_shape=[jax.ShapeDtypeStruct((OPIX, C), BF16), pltpu.VMEM((PIX, C), BF16), kept, kept, kept, kept,
                   jax.ShapeDtypeStruct((3 * LINES, C), BF16)],
        in_specs=[ANY] * 4, out_specs=[ANY] + [VM] * 5 + [ANY],
        scratch_shapes=[pltpu.VMEM((9, C, C), BF16), pltpu.VMEM((2, 3 * LINES, C), BF16), pltpu.VMEM((9, OPIX, C), BF16)]
        + [pltpu.VMEM((OUT_R, OUT_C, C), BF16), pltpu.VMEM((5, OUT_R + 1, OUT_C + EDGE, 128), F32)]
        + [pltpu.VMEM((PIX, C), BF16)]
        + [pltpu.VMEM((5, ROWS + 2, COLS + 2 * EDGE, 128), F32), pltpu.VMEM((5, BLOCK, 128), F32)]
        + edges * 4 + small * 2
        + [dma((6,)), dma((2, 8)), dma((4, 2, 8)), dma((2,)), dma((2, 3, 10)), dma((2, 3, 10)), pltpu.SemaphoreType.REGULAR((2, 3, 4))],
        compiler_params=pltpu.CompilerParams(collective_id=1, has_side_effects=True, vmem_limit_bytes=SCRATCH),
        cost_estimate=pl.CostEstimate(flops=2 * PIX * 90 * C * C, bytes_accessed=64 * MIB, transcendentals=0),
    )(image.reshape(PIX, C), grad_out, w_first, w_down)


def settle_kernel(y_in, dx_in, own_d, own_f, other_d, other_f, y_out, dx_out, down_out, first_out, y_buf, load_sem, sems):
    core = lax.axis_index('h') % 2
    load = pltpu.make_async_copy(y_in, y_buf, load_sem)
    load.start()
    pieces = [(dx_in, dx_out)]
    for own, other, out in ((own_d, other_d, down_out), (own_f, other_f, first_out)):
        for part in THIRDS:
            for side, src in ((core, own), (1 - core, other)):
                pieces.append((src.at[pl.ds(3 * part, 3)], out.at[pl.ds(9 * side + 3 * part, 3)]))
    copies = [pltpu.make_async_copy(src, dst, sems.at[i]) for i, (src, dst) in enumerate(pieces)]
    for copy in copies:
        copy.start()
    load.wait()
    last = pltpu.make_async_copy(y_buf, y_out, sems.at[len(copies)])
    last.start()
    for copy in copies + [last]:
        copy.wait()


def settle(*made):
    total = jax.ShapeDtypeStruct((18, HALF, C), F32)
    dma = pltpu.SemaphoreType.DMA
    return pl.pallas_call(
        settle_kernel, out_shape=[jax.ShapeDtypeStruct((OPIX, C), BF16), jax.ShapeDtypeStruct((PIX, C), BF16), total, total],
        in_specs=[pl.BlockSpec(memory_space=pltpu.HBM)] + [VM] * 5, out_specs=[ANY] * 4,
        scratch_shapes=[pltpu.VMEM((OPIX, C), BF16), dma, dma((14,))],
        compiler_params=pltpu.CompilerParams(vmem_limit_bytes=SCRATCH),
    )(made[0], *(pltpu.with_memory_space_constraint(one, pltpu.VMEM) for one in made[1:]))


def solution(mesh):
    def block_step(image, w_first, w_down, grad_out):
        made = block_call(image[0], grad_out[0], w_first.reshape(9, C, C), w_down.reshape(9, C, C))
        block_out, grad_image, grad_w_down, grad_w_first = settle(*made[:6])
        return (block_out.reshape(1, OUT_R, OUT_C, C), grad_image.reshape(1, ROWS, COLS, C),
                grad_w_first.reshape(3, 3, C, C), grad_w_down.reshape(3, 3, C, C))

    img_spec = P(None, 'h', 'w', None)
    return jax.shard_map(block_step, mesh=mesh, in_specs=(img_spec, P(), P(), img_spec), out_specs=(img_spec, img_spec, P(), P()), check_vma=False)
```

```python
import jax
import jax.numpy as jnp
from jax import lax
from jax.sharding import PartitionSpec as P
from jax.experimental import pallas as pl
from jax.experimental.pallas import tpu as pltpu

MESH = pl.DeviceIdType.MESH
F32, BF16 = jnp.float32, jnp.bfloat16
C = 640
ROWS, COLS = 24, 48
OUT_R, OUT_C = 12, 24
PIX, OPIX = ROWS * COLS, OUT_R * OUT_C
HALF = 320
MIB = 2 ** 20
SCRATCH = 36000000
ORDERS = (('x', 'y', 'z'), ('y', 'z', 'x'), ('z', 'x', 'y'))
R1, R2, R3, A1, A2, A3A, A3B, DA, DB, DC = range(10)
QUARTER = HALF // 2
EIGHTH = QUARTER // 2
LEAST = EIGHTH // 2
LAND_AT = (0, QUARTER, QUARTER + EIGHTH)
LANES = range(C // 128)
TAPS = [(t, t // 3, t % 3) for t in range(9)]
THIRDS = range(3)


def gelu_tanh(values):
    return jax.nn.gelu(values, approximate=True)


def dot(lhs, rhs):
    return lax.dot_general(lhs, rhs, (((1,), (0,)), ((), ())), preferred_element_type=F32)


def dot_rhs_t(lhs, rhs):
    return lax.dot_general(lhs, rhs, (((1,), (1,)), ((), ())), preferred_element_type=F32)


def dot_lhs_t(lhs, rhs):
    return lax.dot_general(lhs, rhs, (((0,), (0,)), ((), ())), preferred_element_type=F32)


ANY = pl.BlockSpec(memory_space=pl.ANY)
VM = pl.BlockSpec(memory_space=pltpu.VMEM)


def place():
    w, h = lax.axis_index('w'), lax.axis_index('h')
    bit = {'x': h // 2, 'c': h % 2, 'y': w % 2, 'z': w // 2}
    dev = {'x': (w, (h + 2) % 4), 'c': (w, h + 1 - 2 * (h % 2)), 'y': (w + 1 - 2 * (w % 2), h), 'z': ((w + 2) % 4, h)}
    return bit, dev


class Reducer:
    def __init__(self, index, own, pair, sems, grants, bit, dev):
        self.index, self.own, self.pair, self.sems, self.grants, self.bit, self.dev = index, own, pair, sems, grants, bit, dev

    def starts(self, third):
        b = [self.bit[axis] for axis in ORDERS[third]]
        base2 = b[0] * QUARTER
        base3 = base2 + b[1] * EIGHTH
        return b, base2, base3, base3 + b[2] * LEAST

    def copy(self, third, kind):
        (b0, b1, b2), base2, base3, base4 = self.starts(third)
        axis0, axis1, axis2 = ORDERS[third]
        far = (1 - b0) * QUARTER
        near1, far1 = b1 * EIGHTH, (1 - b1) * EIGHTH
        src, size, axis = {
            R1: (far, QUARTER, axis0), R2: (base2 + far1, EIGHTH, axis1), R3: (base3 + (1 - b2) * LEAST, LEAST, axis2),
            A1: (base4, LEAST, axis2), A2: (base3, EIGHTH, axis1), A3A: (base3, EIGHTH, axis0), A3B: (base2 + far1, EIGHTH, axis0),
            DA: (base2, QUARTER, 'c'), DB: (far + near1, EIGHTH, 'c'), DC: (far + far1, EIGHTH, 'c'),
        }[kind]
        rows = pl.ds(pl.multiple_of(src, 8), size)
        units = pl.ds(3 * third, 3)
        source = self.own.at[units, rows]
        send, recv = (s.at[self.index, third, kind] for s in self.sems)
        if kind <= R3:
            target = self.pair.at[units, pl.ds(LAND_AT[kind], size)]
        elif kind <= A3B:
            target = source
        else:
            target = self.pair.at[units, rows]
        return pltpu.make_async_remote_copy(src_ref=source, dst_ref=target, send_sem=send, recv_sem=recv, device_id=self.dev[axis], device_id_type=MESH)

    def add(self, third, kind):
        _, base2, base3, base4 = self.starts(third)
        keep, size = ((base2, QUARTER), (base3, EIGHTH), (base4, LEAST))[kind]
        steps = size // LEAST

        def body(j):
            unit, row = 3 * third + j // steps, (j % steps) * LEAST
            rows = pl.ds(pl.multiple_of(keep + row, 8), LEAST)
            self.own[unit, rows, :] += self.pair[unit, pl.ds(pl.multiple_of(LAND_AT[kind] + row, 8), LEAST), :]
        run(3 * steps, body)

    def begin(self):
        for third in THIRDS:
            self.copy(third, R1).start()

    def move(self, wait_for, then, add=False):
        for third in THIRDS:
            self.copy(third, wait_for).wait()
            if add:
                pl.semaphore_signal(self.grants.at[self.index, third, wait_for], inc=1, device_id=self.dev[ORDERS[third][wait_for]], device_id_type=MESH)
                self.add(third, wait_for)
            if wait_for == R3 and third == THIRDS[-1]:
                pl.semaphore_signal(self.grants.at[self.index, 0, 3], inc=1, device_id=self.dev['c'], device_id_type=MESH)
            for kind in then:
                if kind == DA and third == 0:
                    pl.semaphore_wait(self.grants.at[self.index, 0, 3], 1)
                if kind in (A1, A2, A3A):
                    pl.semaphore_wait(self.grants.at[self.index, third, {A1: R3, A2: R2, A3A: R1}[kind]], 1)
                self.copy(third, kind).start()

    def finish(self):
        for kind in (DA, DB, DC):
            self.move(kind, ())


EDGE = 8
LINES = (ROWS + 2) * COLS
BLOCK_ROWS = 6
BLOCK = BLOCK_ROWS * COLS
NEAR = [(dw, dh) for dw in (-1, 0, 1) for dh in (-1, 0, 1) if (dw, dh) != (0, 0)]
ABOVE = [(-1, -1), (-1, 0), (0, -1)]
BELOW = [(1, 1), (1, 0), (0, 1)]
G_AT, G_PAIR_AT, TAP_PAIR_AT = 3 * OPIX, 4 * OPIX, 5 * OPIX


def lane(k):
    return slice(k * 128, k * 128 + 128)


def run(steps, body):
    lax.fori_loop(0, steps, lambda i, _: body(i), None)


def clear_of(flag, value):
    return jnp.where(flag, 0.0, value)


def at(start, size):
    return pl.ds(pl.multiple_of(start, size), size)


class Border:
    def __init__(self, grid, row0, rows, cols, send, land, sems, send_to, take_from, row_sources=None):
        self.grid, self.row0, self.rows, self.cols, self.sends, self.lands = grid, row0, rows, cols, send, land
        self.sems, self.send_to, self.take_from, self.row_sources = sems, send_to, take_from, row_sources
        self.w, self.h = lax.axis_index('w'), lax.axis_index('h')

    def edge(self, step, first, size, outside):
        return {-1: first - outside, 1: first + size - 1 + outside}[step]

    def inside(self, dw, dh):
        w, h = self.w + dw, self.h + dh
        return jnp.logical_and(jnp.logical_and(w >= 0, w < 4), jnp.logical_and(h >= 0, h < 4))

    def copy(self, dw, dh):
        i, up, side = NEAR.index((dw, dh)), (dh + 1) // 2, (dw + 1) // 2
        if dw == 0:
            src = self.row_sources[up] if self.row_sources else self.sends[0].at[up]
            dst = self.lands[0].at[1 - up]
        elif dh == 0:
            src, dst = self.sends[1].at[side], self.lands[1].at[1 - side]
        else:
            src, dst = self.sends[2].at[2 * up + side], self.lands[2].at[2 * (1 - up) + 1 - side]
        peer = ((self.w + dw + 4) % 4, (self.h + dh + 4) % 4)
        return pltpu.make_async_remote_copy(src_ref=src, dst_ref=dst, send_sem=self.sems.at[0, i], recv_sem=self.sems.at[1, i], device_id=peer, device_id_type=MESH)

    def start(self, straight):
        grid, row0, rows, cols = self.grid, self.row0, self.rows, self.cols
        for dw, dh in self.send_to:
            if (dw == 0) != straight:
                continue
            up, side = (dh + 1) // 2, (dw + 1) // 2
            r = None if dh == 0 else self.edge(dh, row0, rows, 0)
            c = None if dw == 0 else self.edge(dw, EDGE, cols, 0)
            for k in LANES:
                if dw == 0:
                    if not self.row_sources:
                        self.sends[0][up, :, lane(k)] = grid[k, r, EDGE:EDGE + cols, :].astype(self.sends[0].dtype)
                elif dh == 0:
                    for row in range(rows):
                        self.sends[1][side, row:row + 1, lane(k)] = grid[k, row0 + row, c:c + 1, :]
                else:
                    self.sends[2][2 * up + side, :, lane(k)] = jnp.broadcast_to(grid[k, r, c:c + 1, :], (8, 128))

            @pl.when(self.inside(dw, dh))
            def _():
                self.copy(dw, dh).start()

    def finish(self):
        grid, row0, rows, cols = self.grid, self.row0, self.rows, self.cols
        for dw, dh in self.send_to:
            @pl.when(self.inside(dw, dh))
            def _():
                self.copy(dw, dh).wait_send()

            @pl.when(self.inside(-dw, -dh))
            def _():
                self.copy(dw, dh).wait_recv()
        for dw, dh in self.take_from:
            up, side = (dh + 1) // 2, (dw + 1) // 2
            r = None if dh == 0 else self.edge(dh, row0, rows, 1)
            c = None if dw == 0 else self.edge(dw, EDGE, cols, 1)
            out = jnp.logical_not(self.inside(dw, dh))
            for k in LANES:
                if dw == 0:
                    grid[k, r, EDGE:EDGE + cols, :] = clear_of(out, self.lands[0][up, :, lane(k)].astype(F32))
                elif dh == 0:
                    for row in range(rows):
                        grid[k, row0 + row, c:c + 1, :] = clear_of(out, self.lands[1][side, row:row + 1, lane(k)])
                else:
                    grid[k, r, c:c + 1, :] = clear_of(out, self.lands[2][2 * up + side, 0:1, lane(k)])


def spread(grid, xs):
    def one_row(r):
        for c in range(3):
            for k in LANES:
                xs[0, at(c * LINES + r * COLS, COLS), lane(k)] = grid[k, r, EDGE - 1 + c:EDGE - 1 + c + COLS, :].astype(BF16)
    run(ROWS + 2, one_row)


def accumulate(acc, rows, part, first):
    for k in LANES:
        piece = part[:, lane(k)]
        acc[k, 0:rows, :] = piece if first else acc[k, 0:rows, :] + piece


def block_kernel(x_in, g_in, w_first, w_down, y_out, da_pair, own_d, own_f, other_d, other_f, x_land,
                 wbuf, xs, taps, g_tile, g_grid, da, grid, acc,
                 send_r, send_c, send_k, x_r, x_c, x_k, z_r, z_c, z_k, d_r, d_c, d_k, gs_r, gs_c, gs_k, gl_r, gl_c, gl_k,
                 load_sems, pair_sems, near_sems, out_sems, send_sems, recv_sems, grants):
    bit, dev = place()
    w, h = lax.axis_index('w'), lax.axis_index('h')
    core = bit['c']
    x_tile = xs.at[0, pl.ds(0, PIX)]
    load_x = pltpu.make_async_copy(x_in, x_tile, load_sems.at[0])
    load_g = pltpu.make_async_copy(g_in, g_tile, load_sems.at[1])
    load_w = pltpu.make_async_copy(w_first, wbuf, load_sems.at[2])
    for load in (load_x, load_g, load_w):
        load.start()
    barrier = pltpu.get_barrier_semaphore()
    for axis in 'xyzc':
        pl.semaphore_signal(barrier, inc=1, device_id=dev[axis], device_id_type=MESH)
    for dw, dh in NEAR:
        pl.semaphore_signal(barrier, inc=1, device_id=((w + dw + 4) % 4, (h + dh + 4) % 4), device_id_type=MESH)
    sends = (send_r, send_c, send_k)
    x_border = Border(grid, 1, ROWS, COLS, sends, (x_r, x_c, x_k), near_sems.at[0], NEAR, NEAR,
                      [x_tile.at[pl.ds(0, COLS)], x_tile.at[pl.ds(PIX - COLS, COLS)]])
    z_border = Border(grid, 0, ROWS, COLS, sends, (z_r, z_c, z_k), near_sems.at[1], ABOVE, BELOW)
    d_border = Border(grid, 1, ROWS, COLS, sends, (d_r, d_c, d_k), near_sems.at[2], NEAR, NEAR)
    g_border = Border(g_grid, 1, OUT_R, OUT_C, (gs_r, gs_c, gs_k), (gl_r, gl_c, gl_k), near_sems.at[3], BELOW, ABOVE)
    sems = (send_sems, recv_sems)
    down = Reducer(0, own_d, other_d, sems, grants, bit, dev)
    first = Reducer(1, own_f, other_f, sems, grants, bit, dev)

    def to_pair(src, dst, i):
        return pltpu.make_async_remote_copy(src_ref=src, dst_ref=dst, send_sem=pair_sems.at[0, i], recv_sem=pair_sems.at[1, i], device_id=dev['c'], device_id_type=MESH)

    def put(own, j, res, more):
        for side in range(2):
            unit = 2 * j + side - core
            part = res[side * HALF:(side + 1) * HALF]

            @pl.when(jnp.logical_and(unit >= 0, unit < 9))
            def _():
                own[unit] = own[unit] + part if more else part

    load_x.wait()
    pl.semaphore_wait(barrier, 12)
    x_border.start(True)

    def place_row(r):
        for k in LANES:
            grid[k, r + 1, EDGE:EDGE + COLS, :] = x_tile[at(r * COLS, COLS), lane(k)].astype(F32)
    run(ROWS, place_row)
    x_border.start(False)
    load_g.wait()
    for r in range(OUT_R):
        for k in LANES:
            g_grid[k, r + 1, EDGE:EDGE + OUT_C, :] = g_tile[r, :, lane(k)].astype(F32)
    g_border.start(True)
    g_border.start(False)
    x_border.finish()
    spread(grid, xs)
    x_share = to_pair(xs.at[0], x_land, 0)
    x_share.start()
    load_w.wait()

    def pre_rows(i):
        for t, a, c in TAPS:
            rows = pl.ds(pl.multiple_of(c * LINES + i * BLOCK + a * COLS, COLS), BLOCK)
            accumulate(acc, BLOCK, dot(xs[0, rows, :], wbuf[t]), t == 0)
        for k in LANES:
            pre = acc[k].astype(BF16).astype(F32)
            acc[k] = pre
            act = gelu_tanh(pre).astype(BF16).astype(F32)
            for r in range(BLOCK_ROWS):
                grid[k, BLOCK_ROWS * i + r, EDGE:EDGE + COLS, :] = act[r * COLS:(r + 1) * COLS]
        for r in range(BLOCK_ROWS):
            for cp in range(2):
                for k in LANES:
                    own_f[2 * (r % 2) + cp, pl.ds(pl.multiple_of((BLOCK_ROWS // 2 * i + r // 2) * OUT_C, 8), OUT_C), lane(k)] = acc[k, pl.ds(r * COLS + cp, OUT_C, stride=2), :]
    run(ROWS // BLOCK_ROWS, pre_rows)
    load_w2 = pltpu.make_async_copy(w_down, wbuf, load_sems.at[3])
    load_w2.start()
    z_border.start(True)
    z_border.start(False)

    g_border.finish()
    for di in range(2):
        for dj in range(2):
            for k in LANES:
                part = g_grid[k, di:di + OUT_R, EDGE - 1 + dj:EDGE - 1 + dj + OUT_C, :]
                xs[1, (2 * di + dj) * OPIX:(2 * di + dj + 1) * OPIX, lane(k)] = part.reshape(OPIX, 128).astype(BF16)
    g_share = to_pair(xs.at[1, pl.ds(G_AT, OPIX)], xs.at[1, pl.ds(G_PAIR_AT, OPIX)], 1)
    g_share.start()
    z_border.finish()

    def tap_rows(p):
        for t, a, c in TAPS:
            for k in LANES:
                cols = pl.ds(EDGE + c, OUT_C, stride=2)
                two = jnp.concatenate([grid[k, 4 * p + a, cols, :], grid[k, 4 * p + 2 + a, cols, :]], 0)
                taps[t, at(p * 2 * OUT_C, 2 * OUT_C), lane(k)] = two.astype(BF16)
    run(OUT_R // 2, tap_rows)
    tap_shares = [to_pair(taps.at[4 * (1 - core) + j], xs.at[1, pl.ds(TAP_PAIR_AT + j * OPIX, OPIX)], 2 + j) for j in range(5)]
    for share in tap_shares:
        share.start()

    def down_tap(j):
        res = dot_lhs_t(taps[4 * core + j], xs[1, G_AT:G_AT + OPIX, :])
        put(own_d, j, res, False)
    run(5, down_tap)
    g_share.wait()
    for share in tap_shares:
        share.wait()

    def down_tap_pair(j):
        rows = pl.ds(pl.multiple_of(TAP_PAIR_AT + j * OPIX, 32), OPIX)
        res = dot_lhs_t(xs[1, rows, :], xs[1, G_PAIR_AT:G_PAIR_AT + OPIX, :])
        put(own_d, j, res, True)
    run(5, down_tap_pair)
    down.begin()

    load_w2.wait()
    for rp in range(2):
        for cp in range(2):
            total = None
            for a in ((0, 2), (1,))[rp]:
                for c in ((0, 2), (1,))[cp]:
                    row = (2 * (1 - a // 2) + 1 - c // 2) * OPIX
                    part = dot_rhs_t(xs[1, row:row + OPIX, :], wbuf[3 * a + c])
                    total = part if total is None else total + part
            pre = own_f[2 * rp + cp, 0:OPIX, :]
            grad = jax.vjp(gelu_tanh, pre)[1](total)[0].astype(BF16).astype(F32)
            for i in range(OUT_R):
                for k in LANES:
                    grid[k, 2 * i + rp + 1, pl.ds(EDGE + cp, OUT_C, stride=2), :] = grad[i * OUT_C:(i + 1) * OUT_C, lane(k)]

    def pack(r):
        for k in LANES:
            da[at(r * COLS, COLS), lane(k)] = grid[k, r + 1, EDGE:EDGE + COLS, :].astype(BF16)
    run(ROWS, pack)
    da_share = to_pair(da, da_pair, 7)
    da_share.start()
    d_border.start(True)
    d_border.start(False)
    x_share.wait()
    pair_load = pltpu.make_async_copy(x_land, xs.at[1], load_sems.at[4])
    pair_load.start()

    for t in range(9):
        accumulate(acc, OPIX, dot(taps[t], wbuf[t]), t == 0)
    for k in LANES:
        taps[0, :, lane(k)] = acc[k, 0:OPIX, :].astype(BF16)
    y_copy = pltpu.make_async_copy(taps.at[0], y_out, out_sems.at[0])
    y_copy.start()
    load_w1 = pltpu.make_async_copy(w_first, wbuf, load_sems.at[5])
    load_w1.start()
    pair_load.wait()
    da_share.wait()

    def first_tap(j):
        t = 4 * core + j
        a, c = t // 3, t % 3
        rows = pl.ds(pl.multiple_of(c * LINES + a * COLS, COLS), PIX)
        res = dot_lhs_t(xs[0, rows, :], da[...]) + dot_lhs_t(xs[1, rows, :], da_pair[...])
        put(own_f, j, res, False)
    run(4, first_tap)
    down.move(R1, (R2,), add=True)
    first_tap(4)
    first.begin()

    d_border.finish()
    spread(grid, xs)
    load_w1.wait()

    def image_rows(i):
        for t, a, c in TAPS:
            rows = pl.ds(pl.multiple_of((2 - c) * LINES + i * BLOCK + (2 - a) * COLS, COLS), BLOCK)
            accumulate(acc, BLOCK, dot_rhs_t(xs[0, rows, :], wbuf[t]), t == 0)
        for k in LANES:
            da_pair[at(i * BLOCK, BLOCK), lane(k)] = acc[k].astype(BF16)
    run(ROWS // BLOCK_ROWS, image_rows)

    down.move(R2, (R3,), add=True)
    first.move(R1, (R2,), add=True)
    down.move(R3, (A1,), add=True)
    first.move(R2, (R3,), add=True)
    down.move(A1, (A2, A3A))
    first.move(R3, (A1,), add=True)
    down.move(A2, (A3B, DA))
    first.move(A1, (A2, A3A))
    down.move(A3A, (DB,))
    first.move(A2, (A3B, DA))
    down.move(A3B, (DC,))
    first.move(A3A, (DB,))
    first.move(A3B, (DC,))
    y_copy.wait()
    down.finish()
    first.finish()


def block_call(image, grad_out, w_first, w_down):
    kept = pltpu.VMEM((9, HALF, C), F32)
    dma = pltpu.SemaphoreType.DMA
    edges = [pltpu.VMEM((2, COLS, C), BF16), pltpu.VMEM((2, ROWS, C), F32), pltpu.VMEM((4, 8, C), F32)]
    small = [pltpu.VMEM((2, OUT_C, C), F32), pltpu.VMEM((2, OUT_R, C), F32), pltpu.VMEM((4, 8, C), F32)]
    return pl.pallas_call(
        block_kernel,
        out_shape=[jax.ShapeDtypeStruct((OPIX, C), BF16), pltpu.VMEM((PIX, C), BF16), kept, kept, kept, kept,
                   jax.ShapeDtypeStruct((3 * LINES, C), BF16)],
        in_specs=[ANY] * 4, out_specs=[ANY] + [VM] * 5 + [ANY],
        scratch_shapes=[pltpu.VMEM((9, C, C), BF16), pltpu.VMEM((2, 3 * LINES, C), BF16), pltpu.VMEM((9, OPIX, C), BF16)]
        + [pltpu.VMEM((OUT_R, OUT_C, C), BF16), pltpu.VMEM((5, OUT_R + 1, OUT_C + EDGE, 128), F32)]
        + [pltpu.VMEM((PIX, C), BF16)]
        + [pltpu.VMEM((5, ROWS + 2, COLS + 2 * EDGE, 128), F32), pltpu.VMEM((5, BLOCK, 128), F32)]
        + edges * 4 + small * 2
        + [dma((6,)), dma((2, 8)), dma((4, 2, 8)), dma((2,)), dma((2, 3, 10)), dma((2, 3, 10)), pltpu.SemaphoreType.REGULAR((2, 3, 4))],
        compiler_params=pltpu.CompilerParams(collective_id=1, has_side_effects=True, vmem_limit_bytes=SCRATCH),
        cost_estimate=pl.CostEstimate(flops=2 * PIX * 90 * C * C, bytes_accessed=64 * MIB, transcendentals=0),
    )(image.reshape(PIX, C), grad_out, w_first, w_down)


def settle_kernel(y_in, dx_in, own_d, own_f, other_d, other_f, y_out, dx_out, down_out, first_out, y_buf, load_sem, sems):
    core = lax.axis_index('h') % 2
    load = pltpu.make_async_copy(y_in, y_buf, load_sem)
    load.start()
    pieces = [(dx_in, dx_out)]
    for own, other, out in ((own_d, other_d, down_out), (own_f, other_f, first_out)):
        for part in THIRDS:
            for side, src in ((core, own), (1 - core, other)):
                pieces.append((src.at[pl.ds(3 * part, 3)], out.at[pl.ds(9 * side + 3 * part, 3)]))
    copies = [pltpu.make_async_copy(src, dst, sems.at[i]) for i, (src, dst) in enumerate(pieces)]
    for copy in copies:
        copy.start()
    load.wait()
    last = pltpu.make_async_copy(y_buf, y_out, sems.at[len(copies)])
    last.start()
    for copy in copies + [last]:
        copy.wait()


def settle(*made):
    total = jax.ShapeDtypeStruct((18, HALF, C), F32)
    dma = pltpu.SemaphoreType.DMA
    return pl.pallas_call(
        settle_kernel, out_shape=[jax.ShapeDtypeStruct((OPIX, C), BF16), jax.ShapeDtypeStruct((PIX, C), BF16), total, total],
        in_specs=[pl.BlockSpec(memory_space=pltpu.HBM)] + [VM] * 5, out_specs=[ANY] * 4,
        scratch_shapes=[pltpu.VMEM((OPIX, C), BF16), dma, dma((14,))],
        compiler_params=pltpu.CompilerParams(vmem_limit_bytes=SCRATCH),
    )(made[0], *(pltpu.with_memory_space_constraint(one, pltpu.VMEM) for one in made[1:]))


def solution(mesh):
    def block_step(image, w_first, w_down, grad_out):
        made = block_call(image[0], grad_out[0], w_first.reshape(9, C, C), w_down.reshape(9, C, C))
        block_out, grad_image, grad_w_down, grad_w_first = settle(*made[:6])
        return (block_out.reshape(1, OUT_R, OUT_C, C), grad_image.reshape(1, ROWS, COLS, C),
                grad_w_first.reshape(3, 3, C, C), grad_w_down.reshape(3, 3, C, C))

    img_spec = P(None, 'h', 'w', None)
    return jax.shard_map(block_step, mesh=mesh, in_specs=(img_spec, P(), P(), img_spec), out_specs=(img_spec, img_spec, P(), P()), check_vma=False)
```

```python
import jax
import jax.numpy as jnp
from jax import lax
from jax.sharding import PartitionSpec as P
from jax.experimental import pallas as pl
from jax.experimental.pallas import tpu as pltpu

MESH = pl.DeviceIdType.MESH
F32, BF16 = jnp.float32, jnp.bfloat16
C = 640
ROWS, COLS = 24, 48
OUT_R, OUT_C = 12, 24
PIX, OPIX = ROWS * COLS, OUT_R * OUT_C
HALF = 320
MIB = 2 ** 20
SCRATCH = 36000000
ORDERS = (('x', 'y', 'z'), ('y', 'z', 'x'), ('z', 'x', 'y'))
R1, R2, R3, A1, A2, A3A, A3B, DA, DB, DC = range(10)
QUARTER = HALF // 2
EIGHTH = QUARTER // 2
LEAST = EIGHTH // 2
LAND_AT = (0, QUARTER, QUARTER + EIGHTH)
LANES = range(C // 128)
TAPS = [(t, t // 3, t % 3) for t in range(9)]
THIRDS = range(3)


def gelu_tanh(values):
    return jax.nn.gelu(values, approximate=True)


def dot(lhs, rhs):
    return lax.dot_general(lhs, rhs, (((1,), (0,)), ((), ())), preferred_element_type=F32)


def dot_rhs_t(lhs, rhs):
    return lax.dot_general(lhs, rhs, (((1,), (1,)), ((), ())), preferred_element_type=F32)


def dot_lhs_t(lhs, rhs):
    return lax.dot_general(lhs, rhs, (((0,), (0,)), ((), ())), preferred_element_type=F32)


ANY = pl.BlockSpec(memory_space=pl.ANY)
VM = pl.BlockSpec(memory_space=pltpu.VMEM)


def place():
    w, h = lax.axis_index('w'), lax.axis_index('h')
    bit = {'x': h // 2, 'c': h % 2, 'y': w % 2, 'z': w // 2}
    dev = {'x': (w, (h + 2) % 4), 'c': (w, h + 1 - 2 * (h % 2)), 'y': (w + 1 - 2 * (w % 2), h), 'z': ((w + 2) % 4, h)}
    return bit, dev


class Reducer:
    def __init__(self, index, own, pair, sems, grants, bit, dev):
        self.index, self.own, self.pair, self.sems, self.grants, self.bit, self.dev = index, own, pair, sems, grants, bit, dev

    def starts(self, third):
        b = [self.bit[axis] for axis in ORDERS[third]]
        base2 = b[0] * QUARTER
        base3 = base2 + b[1] * EIGHTH
        return b, base2, base3, base3 + b[2] * LEAST

    def copy(self, third, kind):
        (b0, b1, b2), base2, base3, base4 = self.starts(third)
        axis0, axis1, axis2 = ORDERS[third]
        far = (1 - b0) * QUARTER
        near1, far1 = b1 * EIGHTH, (1 - b1) * EIGHTH
        src, size, axis = {
            R1: (far, QUARTER, axis0), R2: (base2 + far1, EIGHTH, axis1), R3: (base3 + (1 - b2) * LEAST, LEAST, axis2),
            A1: (base4, LEAST, axis2), A2: (base3, EIGHTH, axis1), A3A: (base3, EIGHTH, axis0), A3B: (base2 + far1, EIGHTH, axis0),
            DA: (base2, QUARTER, 'c'), DB: (far + near1, EIGHTH, 'c'), DC: (far + far1, EIGHTH, 'c'),
        }[kind]
        rows = pl.ds(pl.multiple_of(src, 8), size)
        units = pl.ds(3 * third, 3)
        source = self.own.at[units, rows]
        send, recv = (s.at[self.index, third, kind] for s in self.sems)
        if kind <= R3:
            target = self.pair.at[units, pl.ds(LAND_AT[kind], size)]
        elif kind <= A3B:
            target = source
        else:
            target = self.pair.at[units, rows]
        return pltpu.make_async_remote_copy(src_ref=source, dst_ref=target, send_sem=send, recv_sem=recv, device_id=self.dev[axis], device_id_type=MESH)

    def add(self, third, kind):
        _, base2, base3, base4 = self.starts(third)
        keep, size = ((base2, QUARTER), (base3, EIGHTH), (base4, LEAST))[kind]
        steps = size // LEAST

        def body(j):
            unit, row = 3 * third + j // steps, (j % steps) * LEAST
            rows = pl.ds(pl.multiple_of(keep + row, 8), LEAST)
            self.own[unit, rows, :] += self.pair[unit, pl.ds(pl.multiple_of(LAND_AT[kind] + row, 8), LEAST), :]
        run(3 * steps, body)

    def begin(self):
        for third in THIRDS:
            self.copy(third, R1).start()

    def move(self, wait_for, then, add=False):
        for third in THIRDS:
            self.copy(third, wait_for).wait()
            if add:
                pl.semaphore_signal(self.grants.at[self.index, third, wait_for], inc=1, device_id=self.dev[ORDERS[third][wait_for]], device_id_type=MESH)
                self.add(third, wait_for)
            if wait_for == R3 and third == THIRDS[-1]:
                pl.semaphore_signal(self.grants.at[self.index, 0, 3], inc=1, device_id=self.dev['c'], device_id_type=MESH)
            for kind in then:
                if kind == DA and third == 0:
                    pl.semaphore_wait(self.grants.at[self.index, 0, 3], 1)
                if kind in (A1, A2, A3A):
                    pl.semaphore_wait(self.grants.at[self.index, third, {A1: R3, A2: R2, A3A: R1}[kind]], 1)
                self.copy(third, kind).start()

    def finish(self):
        for kind in (DA, DB, DC):
            self.move(kind, ())


EDGE = 8
ALL_PARTS = ROW, COLUMN, CORNER = range(3)
LINES = (ROWS + 2) * COLS
BLOCK_ROWS = 6
BLOCK = BLOCK_ROWS * COLS
NEAR = [(dw, dh) for dw in (-1, 0, 1) for dh in (-1, 0, 1) if (dw, dh) != (0, 0)]
ABOVE = [(-1, -1), (-1, 0), (0, -1)]
BELOW = [(1, 1), (1, 0), (0, 1)]
G_AT, G_PAIR_AT, TAP_PAIR_AT = 3 * OPIX, 4 * OPIX, 5 * OPIX


def lane(k):
    return slice(k * 128, k * 128 + 128)


def run(steps, body):
    lax.fori_loop(0, steps, lambda i, _: body(i), None)


def clear_of(flag, value):
    return jnp.where(flag, 0.0, value)


def at(start, size):
    return pl.ds(pl.multiple_of(start, size), size)


class Border:
    def __init__(self, grid, row0, rows, cols, send, land, sems, send_to, take_from, row_sources=None):
        self.grid, self.row0, self.rows, self.cols, self.sends, self.lands = grid, row0, rows, cols, send, land
        self.sems, self.send_to, self.take_from, self.row_sources = sems, send_to, take_from, row_sources
        self.w, self.h = lax.axis_index('w'), lax.axis_index('h')

    def edge(self, step, first, size, outside):
        return {-1: first - outside, 1: first + size - 1 + outside}[step]

    def inside(self, dw, dh):
        w, h = self.w + dw, self.h + dh
        return jnp.logical_and(jnp.logical_and(w >= 0, w < 4), jnp.logical_and(h >= 0, h < 4))

    def copy(self, dw, dh):
        i, up, side = NEAR.index((dw, dh)), (dh + 1) // 2, (dw + 1) // 2
        if dw == 0:
            src = self.row_sources[up] if self.row_sources else self.sends[0].at[up]
            dst = self.lands[0].at[1 - up]
        elif dh == 0:
            src, dst = self.sends[1].at[side], self.lands[1].at[1 - side]
        else:
            src, dst = self.sends[2].at[2 * up + side], self.lands[2].at[2 * (1 - up) + 1 - side]
        peer = ((self.w + dw + 4) % 4, (self.h + dh + 4) % 4)
        return pltpu.make_async_remote_copy(src_ref=src, dst_ref=dst, send_sem=self.sems.at[0, i], recv_sem=self.sems.at[1, i], device_id=peer, device_id_type=MESH)

    def chosen(self, ways, parts):
        return [(dw, dh) for dw, dh in ways if (ROW if dw == 0 else COLUMN if dh == 0 else CORNER) in parts]

    def start(self, *parts):
        grid, row0, rows, cols = self.grid, self.row0, self.rows, self.cols
        for dw, dh in self.chosen(self.send_to, parts):
            up, side = (dh + 1) // 2, (dw + 1) // 2
            r = None if dh == 0 else self.edge(dh, row0, rows, 0)
            c = None if dw == 0 else self.edge(dw, EDGE, cols, 0)
            for k in LANES:
                if dw == 0:
                    if not self.row_sources:
                        self.sends[0][up, :, lane(k)] = grid[k, r, EDGE:EDGE + cols, :].astype(self.sends[0].dtype)
                elif dh == 0:
                    for row in range(rows):
                        self.sends[1][side, row:row + 1, lane(k)] = grid[k, row0 + row, c:c + 1, :]
                else:
                    self.sends[2][2 * up + side, :, lane(k)] = jnp.broadcast_to(grid[k, r, c:c + 1, :], (8, 128))

            @pl.when(self.inside(dw, dh))
            def _():
                self.copy(dw, dh).start()

    def finish(self, *parts):
        grid, row0, rows, cols = self.grid, self.row0, self.rows, self.cols
        for dw, dh in self.chosen(self.send_to, parts):
            @pl.when(self.inside(dw, dh))
            def _():
                self.copy(dw, dh).wait_send()

            @pl.when(self.inside(-dw, -dh))
            def _():
                self.copy(dw, dh).wait_recv()
        for dw, dh in self.chosen(self.take_from, parts):
            up, side = (dh + 1) // 2, (dw + 1) // 2
            r = None if dh == 0 else self.edge(dh, row0, rows, 1)
            c = None if dw == 0 else self.edge(dw, EDGE, cols, 1)
            out = jnp.logical_not(self.inside(dw, dh))
            for k in LANES:
                if dw == 0:
                    grid[k, r, EDGE:EDGE + cols, :] = clear_of(out, self.lands[0][up, :, lane(k)].astype(F32))
                elif dh == 0:
                    for row in range(rows):
                        grid[k, row0 + row, c:c + 1, :] = clear_of(out, self.lands[1][side, row:row + 1, lane(k)])
                else:
                    grid[k, r, c:c + 1, :] = clear_of(out, self.lands[2][2 * up + side, 0:1, lane(k)])


def spread(grid, xs):
    def one_row(r):
        for c in range(3):
            for k in LANES:
                xs[0, at(c * LINES + r * COLS, COLS), lane(k)] = grid[k, r, EDGE - 1 + c:EDGE - 1 + c + COLS, :].astype(BF16)
    run(ROWS + 2, one_row)


def accumulate(acc, rows, part, first):
    for k in LANES:
        piece = part[:, lane(k)]
        acc[k, 0:rows, :] = piece if first else acc[k, 0:rows, :] + piece


def block_kernel(x_in, g_in, w_first, w_down, y_out, da_pair, own_d, own_f, other_d, other_f, x_land,
                 wbuf, xs, taps, g_tile, g_grid, da, grid, acc,
                 send_r, send_c, send_k, x_r, x_c, x_k, z_r, z_c, z_k, d_r, d_c, d_k, gs_r, gs_c, gs_k, gl_r, gl_c, gl_k,
                 load_sems, pair_sems, near_sems, out_sems, send_sems, recv_sems, grants):
    bit, dev = place()
    w, h = lax.axis_index('w'), lax.axis_index('h')
    core = bit['c']
    x_tile = xs.at[0, pl.ds(0, PIX)]
    load_x = pltpu.make_async_copy(x_in, x_tile, load_sems.at[0])
    load_g = pltpu.make_async_copy(g_in, g_tile, load_sems.at[1])
    load_w = pltpu.make_async_copy(w_first, wbuf, load_sems.at[2])
    for load in (load_x, load_g, load_w):
        load.start()
    barrier = pltpu.get_barrier_semaphore()
    for axis in 'xyzc':
        pl.semaphore_signal(barrier, inc=1, device_id=dev[axis], device_id_type=MESH)
    for dw, dh in NEAR:
        pl.semaphore_signal(barrier, inc=1, device_id=((w + dw + 4) % 4, (h + dh + 4) % 4), device_id_type=MESH)
    sends = (send_r, send_c, send_k)
    x_border = Border(grid, 1, ROWS, COLS, sends, (x_r, x_c, x_k), near_sems.at[0], NEAR, NEAR,
                      [x_tile.at[pl.ds(0, COLS)], x_tile.at[pl.ds(PIX - COLS, COLS)]])
    z_border = Border(grid, 0, ROWS, COLS, sends, (z_r, z_c, z_k), near_sems.at[1], ABOVE, BELOW)
    d_border = Border(grid, 1, ROWS, COLS, sends, (d_r, d_c, d_k), near_sems.at[2], NEAR, NEAR)
    g_border = Border(g_grid, 1, OUT_R, OUT_C, (gs_r, gs_c, gs_k), (gl_r, gl_c, gl_k), near_sems.at[3], BELOW, ABOVE)
    sems = (send_sems, recv_sems)
    down = Reducer(0, own_d, other_d, sems, grants, bit, dev)
    first = Reducer(1, own_f, other_f, sems, grants, bit, dev)

    def to_pair(src, dst, i):
        return pltpu.make_async_remote_copy(src_ref=src, dst_ref=dst, send_sem=pair_sems.at[0, i], recv_sem=pair_sems.at[1, i], device_id=dev['c'], device_id_type=MESH)

    def put(own, j, res, more):
        for side in range(2):
            unit = 2 * j + side - core
            part = res[side * HALF:(side + 1) * HALF]

            @pl.when(jnp.logical_and(unit >= 0, unit < 9))
            def _():
                own[unit] = own[unit] + part if more else part

    load_x.wait()
    pl.semaphore_wait(barrier, 12)
    x_border.start(ROW)

    def place_row(r):
        for k in LANES:
            grid[k, r + 1, EDGE:EDGE + COLS, :] = x_tile[at(r * COLS, COLS), lane(k)].astype(F32)
    run(ROWS, place_row)
    x_border.start(COLUMN, CORNER)
    load_g.wait()
    for r in range(OUT_R):
        for k in LANES:
            g_grid[k, r + 1, EDGE:EDGE + OUT_C, :] = g_tile[r, :, lane(k)].astype(F32)
    g_border.start(*ALL_PARTS)
    x_border.finish(*ALL_PARTS)
    spread(grid, xs)
    x_share = to_pair(xs.at[0], x_land, 0)
    x_share.start()
    load_w.wait()

    def pre_rows(i):
        for t, a, c in TAPS:
            rows = pl.ds(pl.multiple_of(c * LINES + i * BLOCK + a * COLS, COLS), BLOCK)
            accumulate(acc, BLOCK, dot(xs[0, rows, :], wbuf[t]), t == 0)
        for k in LANES:
            pre = acc[k].astype(BF16).astype(F32)
            acc[k] = pre
            act = gelu_tanh(pre).astype(BF16).astype(F32)
            for r in range(BLOCK_ROWS):
                grid[k, BLOCK_ROWS * i + r, EDGE:EDGE + COLS, :] = act[r * COLS:(r + 1) * COLS]
        for r in range(BLOCK_ROWS):
            for cp in range(2):
                for k in LANES:
                    own_f[2 * (r % 2) + cp, pl.ds(pl.multiple_of((BLOCK_ROWS // 2 * i + r // 2) * OUT_C, 8), OUT_C), lane(k)] = acc[k, pl.ds(r * COLS + cp, OUT_C, stride=2), :]
    pre_rows(0)
    z_border.start(ROW, CORNER)
    run(ROWS // BLOCK_ROWS - 1, lambda i: pre_rows(i + 1))
    z_border.start(COLUMN)
    load_w2 = pltpu.make_async_copy(w_down, wbuf, load_sems.at[3])
    load_w2.start()

    g_border.finish(*ALL_PARTS)
    for di in range(2):
        for dj in range(2):
            for k in LANES:
                part = g_grid[k, di:di + OUT_R, EDGE - 1 + dj:EDGE - 1 + dj + OUT_C, :]
                xs[1, (2 * di + dj) * OPIX:(2 * di + dj + 1) * OPIX, lane(k)] = part.reshape(OPIX, 128).astype(BF16)
    g_share = to_pair(xs.at[1, pl.ds(G_AT, OPIX)], xs.at[1, pl.ds(G_PAIR_AT, OPIX)], 1)
    g_share.start()

    def tap_rows(p, columns):
        for t, a, c in TAPS:
            if c in columns:
                for k in LANES:
                    cols = pl.ds(EDGE + c, OUT_C, stride=2)
                    two = jnp.concatenate([grid[k, 4 * p + a, cols, :], grid[k, 4 * p + 2 + a, cols, :]], 0)
                    taps[t, at(p * 2 * OUT_C, 2 * OUT_C), lane(k)] = two.astype(BF16)

    def early(n, core):
        return n + n // 2 + core * (n % 2)

    def late(n, core):
        return 4 - 2 * n + core * (5 * n - 3)

    def share_tap(j, i):
        rows = pl.ds(pl.multiple_of(TAP_PAIR_AT + j * OPIX, 32), OPIX)
        share = to_pair(taps.at[4 * (1 - core) + j], xs.at[1, rows], 2 + i)
        share.start()
        return share

    def down_tap(j):
        put(own_d, j, dot_lhs_t(taps[4 * core + j], xs[1, G_AT:G_AT + OPIX, :]), False)

    z_border.finish(ROW)
    run(OUT_R // 2, lambda p: tap_rows(p, (0, 1)))
    tap_shares = [share_tap(early(n, 1 - core), n) for n in range(3)]
    run(3, lambda n: down_tap(early(n, core)))
    z_border.finish(COLUMN, CORNER)
    run(OUT_R // 2, lambda p: tap_rows(p, (2,)))
    tap_shares += [share_tap(late(n, 1 - core), 3 + n) for n in range(2)]
    run(2, lambda n: down_tap(late(n, core)))
    g_share.wait()
    for share in tap_shares:
        share.wait()

    def down_tap_pair(j):
        rows = pl.ds(pl.multiple_of(TAP_PAIR_AT + j * OPIX, 32), OPIX)
        res = dot_lhs_t(xs[1, rows, :], xs[1, G_PAIR_AT:G_PAIR_AT + OPIX, :])
        put(own_d, j, res, True)
    run(5, down_tap_pair)
    down.begin()

    load_w2.wait()
    for rp in range(2):
        for cp in range(2):
            total = None
            for a in ((0, 2), (1,))[rp]:
                for c in ((0, 2), (1,))[cp]:
                    row = (2 * (1 - a // 2) + 1 - c // 2) * OPIX
                    part = dot_rhs_t(xs[1, row:row + OPIX, :], wbuf[3 * a + c])
                    total = part if total is None else total + part
            pre = own_f[2 * rp + cp, 0:OPIX, :]
            grad = jax.vjp(gelu_tanh, pre)[1](total)[0].astype(BF16).astype(F32)
            for i in range(OUT_R):
                for k in LANES:
                    grid[k, 2 * i + rp + 1, pl.ds(EDGE + cp, OUT_C, stride=2), :] = grad[i * OUT_C:(i + 1) * OUT_C, lane(k)]

    def pack(r):
        for k in LANES:
            da[at(r * COLS, COLS), lane(k)] = grid[k, r + 1, EDGE:EDGE + COLS, :].astype(BF16)
    run(ROWS, pack)
    da_share = to_pair(da, da_pair, 7)
    da_share.start()
    d_border.start(*ALL_PARTS)
    x_share.wait()
    pair_load = pltpu.make_async_copy(x_land, xs.at[1], load_sems.at[4])
    pair_load.start()

    for t in range(9):
        accumulate(acc, OPIX, dot(taps[t], wbuf[t]), t == 0)
    for k in LANES:
        taps[0, :, lane(k)] = acc[k, 0:OPIX, :].astype(BF16)
    y_copy = pltpu.make_async_copy(taps.at[0], y_out, out_sems.at[0])
    y_copy.start()
    load_w1 = pltpu.make_async_copy(w_first, wbuf, load_sems.at[5])
    load_w1.start()
    pair_load.wait()
    da_share.wait()

    def first_tap(j):
        t = 4 * core + j
        a, c = t // 3, t % 3
        rows = pl.ds(pl.multiple_of(c * LINES + a * COLS, COLS), PIX)
        res = dot_lhs_t(xs[0, rows, :], da[...]) + dot_lhs_t(xs[1, rows, :], da_pair[...])
        put(own_f, j, res, False)
    run(4, first_tap)
    down.move(R1, (R2,), add=True)
    first_tap(4)
    first.begin()

    d_border.finish(*ALL_PARTS)
    spread(grid, xs)
    load_w1.wait()

    def image_rows(i):
        for t, a, c in TAPS:
            rows = pl.ds(pl.multiple_of((2 - c) * LINES + i * BLOCK + (2 - a) * COLS, COLS), BLOCK)
            accumulate(acc, BLOCK, dot_rhs_t(xs[0, rows, :], wbuf[t]), t == 0)
        for k in LANES:
            da_pair[at(i * BLOCK, BLOCK), lane(k)] = acc[k].astype(BF16)
    run(ROWS // BLOCK_ROWS, image_rows)

    down.move(R2, (R3,), add=True)
    first.move(R1, (R2,), add=True)
    down.move(R3, (A1,), add=True)
    first.move(R2, (R3,), add=True)
    down.move(A1, (A2, A3A))
    first.move(R3, (A1,), add=True)
    down.move(A2, (A3B, DA))
    first.move(A1, (A2, A3A))
    down.move(A3A, (DB,))
    first.move(A2, (A3B, DA))
    down.move(A3B, (DC,))
    first.move(A3A, (DB,))
    first.move(A3B, (DC,))
    y_copy.wait()
    down.finish()
    first.finish()


def block_call(image, grad_out, w_first, w_down):
    kept = pltpu.VMEM((9, HALF, C), F32)
    dma = pltpu.SemaphoreType.DMA
    edges = [pltpu.VMEM((2, COLS, C), BF16), pltpu.VMEM((2, ROWS, C), F32), pltpu.VMEM((4, 8, C), F32)]
    small = [pltpu.VMEM((2, OUT_C, C), F32), pltpu.VMEM((2, OUT_R, C), F32), pltpu.VMEM((4, 8, C), F32)]
    return pl.pallas_call(
        block_kernel,
        out_shape=[jax.ShapeDtypeStruct((OPIX, C), BF16), pltpu.VMEM((PIX, C), BF16), kept, kept, kept, kept,
                   jax.ShapeDtypeStruct((3 * LINES, C), BF16)],
        in_specs=[ANY] * 4, out_specs=[ANY] + [VM] * 5 + [ANY],
        scratch_shapes=[pltpu.VMEM((9, C, C), BF16), pltpu.VMEM((2, 3 * LINES, C), BF16), pltpu.VMEM((9, OPIX, C), BF16)]
        + [pltpu.VMEM((OUT_R, OUT_C, C), BF16), pltpu.VMEM((5, OUT_R + 1, OUT_C + EDGE, 128), F32)]
        + [pltpu.VMEM((PIX, C), BF16)]
        + [pltpu.VMEM((5, ROWS + 2, COLS + 2 * EDGE, 128), F32), pltpu.VMEM((5, BLOCK, 128), F32)]
        + edges * 4 + small * 2
        + [dma((6,)), dma((2, 8)), dma((4, 2, 8)), dma((2,)), dma((2, 3, 10)), dma((2, 3, 10)), pltpu.SemaphoreType.REGULAR((2, 3, 4))],
        compiler_params=pltpu.CompilerParams(collective_id=1, has_side_effects=True, vmem_limit_bytes=SCRATCH),
        cost_estimate=pl.CostEstimate(flops=2 * PIX * 90 * C * C, bytes_accessed=64 * MIB, transcendentals=0),
    )(image.reshape(PIX, C), grad_out, w_first, w_down)


def settle_kernel(y_in, dx_in, own_d, own_f, other_d, other_f, y_out, dx_out, down_out, first_out, y_buf, load_sem, sems):
    core = lax.axis_index('h') % 2
    load = pltpu.make_async_copy(y_in, y_buf, load_sem)
    load.start()
    pieces = [(dx_in, dx_out)]
    for own, other, out in ((own_d, other_d, down_out), (own_f, other_f, first_out)):
        for part in THIRDS:
            for side, src in ((core, own), (1 - core, other)):
                pieces.append((src.at[pl.ds(3 * part, 3)], out.at[pl.ds(9 * side + 3 * part, 3)]))
    copies = [pltpu.make_async_copy(src, dst, sems.at[i]) for i, (src, dst) in enumerate(pieces)]
    for copy in copies:
        copy.start()
    load.wait()
    last = pltpu.make_async_copy(y_buf, y_out, sems.at[len(copies)])
    last.start()
    for copy in copies + [last]:
        copy.wait()


def settle(*made):
    total = jax.ShapeDtypeStruct((18, HALF, C), F32)
    dma = pltpu.SemaphoreType.DMA
    return pl.pallas_call(
        settle_kernel, out_shape=[jax.ShapeDtypeStruct((OPIX, C), BF16), jax.ShapeDtypeStruct((PIX, C), BF16), total, total],
        in_specs=[pl.BlockSpec(memory_space=pltpu.HBM)] + [VM] * 5, out_specs=[ANY] * 4,
        scratch_shapes=[pltpu.VMEM((OPIX, C), BF16), dma, dma((14,))],
        compiler_params=pltpu.CompilerParams(vmem_limit_bytes=SCRATCH),
    )(made[0], *(pltpu.with_memory_space_constraint(one, pltpu.VMEM) for one in made[1:]))


def solution(mesh):
    def block_step(image, w_first, w_down, grad_out):
        made = block_call(image[0], grad_out[0], w_first.reshape(9, C, C), w_down.reshape(9, C, C))
        block_out, grad_image, grad_w_down, grad_w_first = settle(*made[:6])
        return (block_out.reshape(1, OUT_R, OUT_C, C), grad_image.reshape(1, ROWS, COLS, C),
                grad_w_first.reshape(3, 3, C, C), grad_w_down.reshape(3, 3, C, C))

    img_spec = P(None, 'h', 'w', None)
    return jax.shard_map(block_step, mesh=mesh, in_specs=(img_spec, P(), P(), img_spec), out_specs=(img_spec, img_spec, P(), P()), check_vma=False)
```

```python
import jax
import jax.numpy as jnp
from jax import lax
from jax.sharding import PartitionSpec as P
from jax.experimental import pallas as pl
from jax.experimental.pallas import tpu as pltpu

MESH = pl.DeviceIdType.MESH
F32, BF16 = jnp.float32, jnp.bfloat16
C = 640
ROWS, COLS = 24, 48
OUT_R, OUT_C = 12, 24
PIX, OPIX = ROWS * COLS, OUT_R * OUT_C
HALF = 320
MIB = 2 ** 20
SCRATCH = 36000000
ORDERS = (('x', 'y', 'z'), ('y', 'z', 'x'), ('z', 'x', 'y'))
R1, R2, R3, A1, A2, A3A, A3B, A3C, DA, DB, DC, DD = range(12)
QUARTER = HALF // 2
EIGHTH = QUARTER // 2
LEAST = EIGHTH // 2
LAND_AT = (0, QUARTER, QUARTER + EIGHTH)
LANES = range(C // 128)
TAPS = [(t, t // 3, t % 3) for t in range(9)]
THIRDS = range(3)


def gelu_tanh(values):
    return jax.nn.gelu(values, approximate=True)


def dot(lhs, rhs):
    return lax.dot_general(lhs, rhs, (((1,), (0,)), ((), ())), preferred_element_type=F32)


def dot_rhs_t(lhs, rhs):
    return lax.dot_general(lhs, rhs, (((1,), (1,)), ((), ())), preferred_element_type=F32)


def dot_lhs_t(lhs, rhs):
    return lax.dot_general(lhs, rhs, (((0,), (0,)), ((), ())), preferred_element_type=F32)


ANY = pl.BlockSpec(memory_space=pl.ANY)
VM = pl.BlockSpec(memory_space=pltpu.VMEM)


def place():
    w, h = lax.axis_index('w'), lax.axis_index('h')
    bit = {'x': h // 2, 'c': h % 2, 'y': w % 2, 'z': w // 2}
    dev = {'x': (w, (h + 2) % 4), 'c': (w, h + 1 - 2 * (h % 2)), 'y': (w + 1 - 2 * (w % 2), h), 'z': ((w + 2) % 4, h)}
    return bit, dev


class Reducer:
    def __init__(self, index, own, pair, sems, grants, bit, dev):
        self.index, self.own, self.pair, self.sems, self.grants, self.bit, self.dev = index, own, pair, sems, grants, bit, dev

    def starts(self, third):
        b = [self.bit[axis] for axis in ORDERS[third]]
        base2 = b[0] * QUARTER
        base3 = base2 + b[1] * EIGHTH
        return b, base2, base3, base3 + b[2] * LEAST

    def copy(self, third, kind):
        (b0, b1, b2), base2, base3, base4 = self.starts(third)
        axis0, axis1, axis2 = ORDERS[third]
        far = (1 - b0) * QUARTER
        near1, far1 = b1 * EIGHTH, (1 - b1) * EIGHTH
        src, size, axis = {
            R1: (far, QUARTER, axis0), R2: (base2 + far1, EIGHTH, axis1), R3: (base3 + (1 - b2) * LEAST, LEAST, axis2),
            A1: (base4, LEAST, axis2), A2: (base3, EIGHTH, axis1), A3A: (base3, EIGHTH, axis0), A3B: (base2 + far1, LEAST, axis0), A3C: (base2 + far1 + LEAST, LEAST, axis0),
            DA: (base2, QUARTER, 'c'), DB: (far + near1, EIGHTH, 'c'), DC: (far + far1, LEAST, 'c'), DD: (far + far1 + LEAST, LEAST, 'c'),
        }[kind]
        rows = pl.ds(pl.multiple_of(src, 8), size)
        units = pl.ds(3 * third, 3)
        source = self.own.at[units, rows]
        send, recv = (s.at[self.index, third, kind] for s in self.sems)
        if kind <= R3:
            target = self.pair.at[units, pl.ds(LAND_AT[kind], size)]
        elif kind <= A3C:
            target = source
        else:
            target = self.pair.at[units, rows]
        return pltpu.make_async_remote_copy(src_ref=source, dst_ref=target, send_sem=send, recv_sem=recv, device_id=self.dev[axis], device_id_type=MESH)

    def add(self, third, kind):
        _, base2, base3, base4 = self.starts(third)
        keep, size = ((base2, QUARTER), (base3, EIGHTH), (base4, LEAST))[kind]
        steps = size // LEAST

        def body(j):
            unit, row = 3 * third + j // steps, (j % steps) * LEAST
            rows = pl.ds(pl.multiple_of(keep + row, 8), LEAST)
            self.own[unit, rows, :] += self.pair[unit, pl.ds(pl.multiple_of(LAND_AT[kind] + row, 8), LEAST), :]
        run(3 * steps, body)

    def begin(self, *thirds):
        for third in thirds:
            self.copy(third, R1).start()

    def move(self, wait_for, then, add=False):
        for third in THIRDS:
            self.copy(third, wait_for).wait()
            if add:
                pl.semaphore_signal(self.grants.at[self.index, third, wait_for], inc=1, device_id=self.dev[ORDERS[third][wait_for]], device_id_type=MESH)
                self.add(third, wait_for)
            if wait_for == R3 and third == THIRDS[-1]:
                pl.semaphore_signal(self.grants.at[self.index, 0, 3], inc=1, device_id=self.dev['c'], device_id_type=MESH)
            for kind in then:
                if kind == DA and third == 0:
                    pl.semaphore_wait(self.grants.at[self.index, 0, 3], 1)
                if kind in (A1, A2, A3A):
                    pl.semaphore_wait(self.grants.at[self.index, third, {A1: R3, A2: R2, A3A: R1}[kind]], 1)
                self.copy(third, kind).start()

    def finish(self):
        for kind in (DA, DB, DC, DD):
            self.move(kind, ())


EDGE = 8
ALL_PARTS = ROW, COLUMN, CORNER = range(3)
LINES = (ROWS + 2) * COLS
BLOCK_ROWS = 6
BLOCK = BLOCK_ROWS * COLS
NEAR = [(dw, dh) for dw in (-1, 0, 1) for dh in (-1, 0, 1) if (dw, dh) != (0, 0)]
ABOVE = [(-1, -1), (-1, 0), (0, -1)]
BELOW = [(1, 1), (1, 0), (0, 1)]
G_AT, G_PAIR_AT, TAP_PAIR_AT = 3 * OPIX, 4 * OPIX, 5 * OPIX


def lane(k):
    return slice(k * 128, k * 128 + 128)


def run(steps, body):
    lax.fori_loop(0, steps, lambda i, _: body(i), None)


def clear_of(flag, value):
    return jnp.where(flag, 0.0, value)


def at(start, size):
    return pl.ds(pl.multiple_of(start, size), size)


class Border:
    def __init__(self, grid, row0, rows, cols, send, land, sems, send_to, take_from, row_sources=None):
        self.grid, self.row0, self.rows, self.cols, self.sends, self.lands = grid, row0, rows, cols, send, land
        self.sems, self.send_to, self.take_from, self.row_sources = sems, send_to, take_from, row_sources
        self.w, self.h = lax.axis_index('w'), lax.axis_index('h')

    def edge(self, step, first, size, outside):
        return {-1: first - outside, 1: first + size - 1 + outside}[step]

    def inside(self, dw, dh):
        w, h = self.w + dw, self.h + dh
        return jnp.logical_and(jnp.logical_and(w >= 0, w < 4), jnp.logical_and(h >= 0, h < 4))

    def copy(self, dw, dh):
        i, up, side = NEAR.index((dw, dh)), (dh + 1) // 2, (dw + 1) // 2
        if dw == 0:
            src = self.row_sources[up] if self.row_sources else self.sends[0].at[up]
            dst = self.lands[0].at[1 - up]
        elif dh == 0:
            src, dst = self.sends[1].at[side], self.lands[1].at[1 - side]
        else:
            src, dst = self.sends[2].at[2 * up + side], self.lands[2].at[2 * (1 - up) + 1 - side]
        peer = ((self.w + dw + 4) % 4, (self.h + dh + 4) % 4)
        return pltpu.make_async_remote_copy(src_ref=src, dst_ref=dst, send_sem=self.sems.at[0, i], recv_sem=self.sems.at[1, i], device_id=peer, device_id_type=MESH)

    def chosen(self, ways, parts):
        return [(dw, dh) for dw, dh in ways if (ROW if dw == 0 else COLUMN if dh == 0 else CORNER) in parts]

    def start(self, *parts):
        grid, row0, rows, cols = self.grid, self.row0, self.rows, self.cols
        for dw, dh in self.chosen(self.send_to, parts):
            up, side = (dh + 1) // 2, (dw + 1) // 2
            r = None if dh == 0 else self.edge(dh, row0, rows, 0)
            c = None if dw == 0 else self.edge(dw, EDGE, cols, 0)
            for k in LANES:
                if dw == 0:
                    if not self.row_sources:
                        self.sends[0][up, :, lane(k)] = grid[k, r, EDGE:EDGE + cols, :].astype(self.sends[0].dtype)
                elif dh == 0:
                    for row in range(rows):
                        self.sends[1][side, row:row + 1, lane(k)] = grid[k, row0 + row, c:c + 1, :]
                else:
                    self.sends[2][2 * up + side, :, lane(k)] = jnp.broadcast_to(grid[k, r, c:c + 1, :], (8, 128))

            @pl.when(self.inside(dw, dh))
            def _():
                self.copy(dw, dh).start()

    def finish(self, *parts):
        grid, row0, rows, cols = self.grid, self.row0, self.rows, self.cols
        for dw, dh in self.chosen(self.send_to, parts):
            @pl.when(self.inside(dw, dh))
            def _():
                self.copy(dw, dh).wait_send()

            @pl.when(self.inside(-dw, -dh))
            def _():
                self.copy(dw, dh).wait_recv()
        for dw, dh in self.chosen(self.take_from, parts):
            up, side = (dh + 1) // 2, (dw + 1) // 2
            r = None if dh == 0 else self.edge(dh, row0, rows, 1)
            c = None if dw == 0 else self.edge(dw, EDGE, cols, 1)
            out = jnp.logical_not(self.inside(dw, dh))
            for k in LANES:
                if dw == 0:
                    grid[k, r, EDGE:EDGE + cols, :] = clear_of(out, self.lands[0][up, :, lane(k)].astype(F32))
                elif dh == 0:
                    for row in range(rows):
                        grid[k, row0 + row, c:c + 1, :] = clear_of(out, self.lands[1][side, row:row + 1, lane(k)])
                else:
                    grid[k, r, c:c + 1, :] = clear_of(out, self.lands[2][2 * up + side, 0:1, lane(k)])


def spread(grid, xs):
    def one_row(r):
        for c in range(3):
            for k in LANES:
                xs[0, at(c * LINES + r * COLS, COLS), lane(k)] = grid[k, r, EDGE - 1 + c:EDGE - 1 + c + COLS, :].astype(BF16)
    run(ROWS + 2, one_row)


def accumulate(acc, rows, part, first):
    for k in LANES:
        piece = part[:, lane(k)]
        acc[k, 0:rows, :] = piece if first else acc[k, 0:rows, :] + piece


def block_kernel(x_in, g_in, w_first, w_down, y_out, da_pair, own_d, own_f, other_d, other_f, x_land,
                 wbuf, xs, taps, g_tile, g_grid, da, grid, acc,
                 send_r, send_c, send_k, x_r, x_c, x_k, z_r, z_c, z_k, d_r, d_c, d_k, gs_r, gs_c, gs_k, gl_r, gl_c, gl_k,
                 load_sems, pair_sems, near_sems, out_sems, send_sems, recv_sems, grants):
    bit, dev = place()
    w, h = lax.axis_index('w'), lax.axis_index('h')
    core = bit['c']
    x_tile = xs.at[0, pl.ds(0, PIX)]
    load_x = pltpu.make_async_copy(x_in, x_tile, load_sems.at[0])
    load_g = pltpu.make_async_copy(g_in, g_tile, load_sems.at[1])
    load_w = pltpu.make_async_copy(w_first, wbuf, load_sems.at[2])
    for load in (load_x, load_g, load_w):
        load.start()
    barrier = pltpu.get_barrier_semaphore()
    for axis in 'xyzc':
        pl.semaphore_signal(barrier, inc=1, device_id=dev[axis], device_id_type=MESH)
    for dw, dh in NEAR:
        pl.semaphore_signal(barrier, inc=1, device_id=((w + dw + 4) % 4, (h + dh + 4) % 4), device_id_type=MESH)
    sends = (send_r, send_c, send_k)
    x_border = Border(grid, 1, ROWS, COLS, sends, (x_r, x_c, x_k), near_sems.at[0], NEAR, NEAR,
                      [x_tile.at[pl.ds(0, COLS)], x_tile.at[pl.ds(PIX - COLS, COLS)]])
    z_border = Border(grid, 0, ROWS, COLS, sends, (z_r, z_c, z_k), near_sems.at[1], ABOVE, BELOW)
    d_border = Border(grid, 1, ROWS, COLS, sends, (d_r, d_c, d_k), near_sems.at[2], NEAR, NEAR)
    g_border = Border(g_grid, 1, OUT_R, OUT_C, (gs_r, gs_c, gs_k), (gl_r, gl_c, gl_k), near_sems.at[3], BELOW, ABOVE)
    sems = (send_sems, recv_sems)
    down = Reducer(0, own_d, other_d, sems, grants, bit, dev)
    first = Reducer(1, own_f, other_f, sems, grants, bit, dev)

    def to_pair(src, dst, i):
        return pltpu.make_async_remote_copy(src_ref=src, dst_ref=dst, send_sem=pair_sems.at[0, i], recv_sem=pair_sems.at[1, i], device_id=dev['c'], device_id_type=MESH)

    def put(own, j, res, more):
        for side in range(2):
            unit = 2 * j + side - core
            part = res[side * HALF:(side + 1) * HALF]

            @pl.when(jnp.logical_and(unit >= 0, unit < 9))
            def _():
                own[unit] = own[unit] + part if more else part

    load_x.wait()
    pl.semaphore_wait(barrier, 12)
    x_border.start(ROW)

    def place_row(r):
        for k in LANES:
            grid[k, r + 1, EDGE:EDGE + COLS, :] = x_tile[at(r * COLS, COLS), lane(k)].astype(F32)
    run(ROWS, place_row)
    x_border.start(COLUMN, CORNER)
    load_g.wait()
    for r in range(OUT_R):
        for k in LANES:
            g_grid[k, r + 1, EDGE:EDGE + OUT_C, :] = g_tile[r, :, lane(k)].astype(F32)
    g_border.start(*ALL_PARTS)
    x_border.finish(*ALL_PARTS)
    spread(grid, xs)
    x_share = to_pair(xs.at[0], x_land, 0)
    x_share.start()
    load_w.wait()

    def pre_rows(i):
        for t, a, c in TAPS:
            rows = pl.ds(pl.multiple_of(c * LINES + i * BLOCK + a * COLS, COLS), BLOCK)
            accumulate(acc, BLOCK, dot(xs[0, rows, :], wbuf[t]), t == 0)
        for k in LANES:
            pre = acc[k].astype(BF16).astype(F32)
            acc[k] = pre
            act = gelu_tanh(pre).astype(BF16).astype(F32)
            for r in range(BLOCK_ROWS):
                grid[k, BLOCK_ROWS * i + r, EDGE:EDGE + COLS, :] = act[r * COLS:(r + 1) * COLS]
        for r in range(BLOCK_ROWS):
            for cp in range(2):
                for k in LANES:
                    own_f[2 * (r % 2) + cp, pl.ds(pl.multiple_of((BLOCK_ROWS // 2 * i + r // 2) * OUT_C, 8), OUT_C), lane(k)] = acc[k, pl.ds(r * COLS + cp, OUT_C, stride=2), :]
    pre_rows(0)
    z_border.start(ROW, CORNER)
    run(ROWS // BLOCK_ROWS - 1, lambda i: pre_rows(i + 1))
    z_border.start(COLUMN)
    load_w2 = pltpu.make_async_copy(w_down, wbuf, load_sems.at[3])
    load_w2.start()

    g_border.finish(*ALL_PARTS)
    for di in range(2):
        for dj in range(2):
            for k in LANES:
                part = g_grid[k, di:di + OUT_R, EDGE - 1 + dj:EDGE - 1 + dj + OUT_C, :]
                xs[1, (2 * di + dj) * OPIX:(2 * di + dj + 1) * OPIX, lane(k)] = part.reshape(OPIX, 128).astype(BF16)
    g_share = to_pair(xs.at[1, pl.ds(G_AT, OPIX)], xs.at[1, pl.ds(G_PAIR_AT, OPIX)], 1)
    g_share.start()

    def tap_rows(p, columns):
        for t, a, c in TAPS:
            if c in columns:
                for k in LANES:
                    cols = pl.ds(EDGE + c, OUT_C, stride=2)
                    two = jnp.concatenate([grid[k, 4 * p + a, cols, :], grid[k, 4 * p + 2 + a, cols, :]], 0)
                    taps[t, at(p * 2 * OUT_C, 2 * OUT_C), lane(k)] = two.astype(BF16)

    def early(n, core):
        return n + n // 2 + core * (n % 2)

    def late(n, core):
        return 4 - 2 * n + core * (5 * n - 3)

    def share_tap(j, i):
        rows = pl.ds(pl.multiple_of(TAP_PAIR_AT + j * OPIX, 32), OPIX)
        share = to_pair(taps.at[4 * (1 - core) + j], xs.at[1, rows], 2 + i)
        share.start()
        return share

    def down_tap(j):
        put(own_d, j, dot_lhs_t(taps[4 * core + j], xs[1, G_AT:G_AT + OPIX, :]), False)

    z_border.finish(ROW)
    run(OUT_R // 2, lambda p: tap_rows(p, (0, 1)))
    tap_shares = [share_tap(early(n, 1 - core), n) for n in range(3)]
    run(3, lambda n: down_tap(early(n, core)))
    z_border.finish(COLUMN, CORNER)
    run(OUT_R // 2, lambda p: tap_rows(p, (2,)))
    tap_shares += [share_tap(late(n, 1 - core), 3 + n) for n in range(2)]
    run(2, lambda n: down_tap(late(n, core)))
    g_share.wait()
    for share in tap_shares:
        share.wait()

    def down_tap_pair(j):
        rows = pl.ds(TAP_PAIR_AT + j * OPIX, OPIX)
        res = dot_lhs_t(xs[1, rows, :], xs[1, G_PAIR_AT:G_PAIR_AT + OPIX, :])
        put(own_d, j, res, True)
    for j in range(5):
        down_tap_pair(j)
        down.begin(*{1: (0,), 3: (1,), 4: (2,)}.get(j, ()))

    load_w2.wait()
    for rp in range(2):
        for cp in range(2):
            total = None
            for a in ((0, 2), (1,))[rp]:
                for c in ((0, 2), (1,))[cp]:
                    row = (2 * (1 - a // 2) + 1 - c // 2) * OPIX
                    part = dot_rhs_t(xs[1, row:row + OPIX, :], wbuf[3 * a + c])
                    total = part if total is None else total + part
            pre = own_f[2 * rp + cp, 0:OPIX, :]
            grad = jax.vjp(gelu_tanh, pre)[1](total)[0].astype(BF16).astype(F32)
            for i in range(OUT_R):
                for k in LANES:
                    grid[k, 2 * i + rp + 1, pl.ds(EDGE + cp, OUT_C, stride=2), :] = grad[i * OUT_C:(i + 1) * OUT_C, lane(k)]

    def pack(r):
        for k in LANES:
            da[at(r * COLS, COLS), lane(k)] = grid[k, r + 1, EDGE:EDGE + COLS, :].astype(BF16)
    run(ROWS, pack)
    da_share = to_pair(da, da_pair, 7)
    da_share.start()
    d_border.start(*ALL_PARTS)
    x_share.wait()
    pair_load = pltpu.make_async_copy(x_land, xs.at[1], load_sems.at[4])
    pair_load.start()

    for t in range(9):
        accumulate(acc, OPIX, dot(taps[t], wbuf[t]), t == 0)
    for k in LANES:
        taps[0, :, lane(k)] = acc[k, 0:OPIX, :].astype(BF16)
    y_copy = pltpu.make_async_copy(taps.at[0], y_out, out_sems.at[0])
    y_copy.start()
    load_w1 = pltpu.make_async_copy(w_first, wbuf, load_sems.at[5])
    load_w1.start()
    pair_load.wait()
    da_share.wait()

    def first_tap(j):
        t = 4 * core + j
        a, c = t // 3, t % 3
        rows = pl.ds(pl.multiple_of(c * LINES + a * COLS, COLS), PIX)
        res = dot_lhs_t(xs[0, rows, :], da[...]) + dot_lhs_t(xs[1, rows, :], da_pair[...])
        put(own_f, j, res, False)
    run(4, first_tap)
    down.move(R1, (R2,), add=True)
    first_tap(4)
    first.begin(*THIRDS)

    d_border.finish(*ALL_PARTS)
    spread(grid, xs)
    load_w1.wait()

    def image_rows(i):
        for t, a, c in TAPS:
            rows = pl.ds(pl.multiple_of((2 - c) * LINES + i * BLOCK + (2 - a) * COLS, COLS), BLOCK)
            accumulate(acc, BLOCK, dot_rhs_t(xs[0, rows, :], wbuf[t]), t == 0)
        for k in LANES:
            da_pair[at(i * BLOCK, BLOCK), lane(k)] = acc[k].astype(BF16)
    run(ROWS // BLOCK_ROWS, image_rows)

    down.move(R2, (R3,), add=True)
    first.move(R1, (R2,), add=True)
    down.move(R3, (A1,), add=True)
    first.move(R2, (R3,), add=True)
    down.move(A1, (A2, A3A))
    first.move(R3, (A1,), add=True)
    down.move(A2, (A3B, A3C, DA))
    first.move(A1, (A2, A3A))
    down.move(A3A, (DB,))
    first.move(A2, (A3B, A3C, DA))
    down.move(A3B, (DC,))
    down.move(A3C, (DD,))
    first.move(A3A, (DB,))
    first.move(A3B, (DC,))
    first.move(A3C, (DD,))
    y_copy.wait()
    down.finish()
    first.finish()


def block_call(image, grad_out, w_first, w_down):
    kept = pltpu.VMEM((9, HALF, C), F32)
    dma = pltpu.SemaphoreType.DMA
    edges = [pltpu.VMEM((2, COLS, C), BF16), pltpu.VMEM((2, ROWS, C), F32), pltpu.VMEM((4, 8, C), F32)]
    small = [pltpu.VMEM((2, OUT_C, C), F32), pltpu.VMEM((2, OUT_R, C), F32), pltpu.VMEM((4, 8, C), F32)]
    return pl.pallas_call(
        block_kernel,
        out_shape=[jax.ShapeDtypeStruct((OPIX, C), BF16), pltpu.VMEM((PIX, C), BF16), kept, kept, kept, kept,
                   jax.ShapeDtypeStruct((3 * LINES, C), BF16)],
        in_specs=[ANY] * 4, out_specs=[ANY] + [VM] * 5 + [ANY],
        scratch_shapes=[pltpu.VMEM((9, C, C), BF16), pltpu.VMEM((2, 3 * LINES, C), BF16), pltpu.VMEM((9, OPIX, C), BF16)]
        + [pltpu.VMEM((OUT_R, OUT_C, C), BF16), pltpu.VMEM((5, OUT_R + 1, OUT_C + EDGE, 128), F32)]
        + [pltpu.VMEM((PIX, C), BF16)]
        + [pltpu.VMEM((5, ROWS + 2, COLS + 2 * EDGE, 128), F32), pltpu.VMEM((5, BLOCK, 128), F32)]
        + edges * 4 + small * 2
        + [dma((6,)), dma((2, 8)), dma((4, 2, 8)), dma((2,)), dma((2, 3, 12)), dma((2, 3, 12)), pltpu.SemaphoreType.REGULAR((2, 3, 4))],
        compiler_params=pltpu.CompilerParams(collective_id=1, has_side_effects=True, vmem_limit_bytes=SCRATCH),
        cost_estimate=pl.CostEstimate(flops=2 * PIX * 90 * C * C, bytes_accessed=64 * MIB, transcendentals=0),
    )(image.reshape(PIX, C), grad_out, w_first, w_down)


def settle_kernel(y_in, dx_in, own_d, own_f, other_d, other_f, y_out, dx_out, down_out, first_out, y_buf, load_sem, sems):
    core = lax.axis_index('h') % 2
    load = pltpu.make_async_copy(y_in, y_buf, load_sem)
    load.start()
    pieces = [(dx_in, dx_out)]
    for own, other, out in ((own_d, other_d, down_out), (own_f, other_f, first_out)):
        for part in THIRDS:
            for side, src in ((core, own), (1 - core, other)):
                pieces.append((src.at[pl.ds(3 * part, 3)], out.at[pl.ds(9 * side + 3 * part, 3)]))
    copies = [pltpu.make_async_copy(src, dst, sems.at[i]) for i, (src, dst) in enumerate(pieces)]
    for copy in copies:
        copy.start()
    load.wait()
    last = pltpu.make_async_copy(y_buf, y_out, sems.at[len(copies)])
    last.start()
    for copy in copies + [last]:
        copy.wait()


def settle(*made):
    total = jax.ShapeDtypeStruct((18, HALF, C), F32)
    dma = pltpu.SemaphoreType.DMA
    return pl.pallas_call(
        settle_kernel, out_shape=[jax.ShapeDtypeStruct((OPIX, C), BF16), jax.ShapeDtypeStruct((PIX, C), BF16), total, total],
        in_specs=[pl.BlockSpec(memory_space=pltpu.HBM)] + [VM] * 5, out_specs=[ANY] * 4,
        scratch_shapes=[pltpu.VMEM((OPIX, C), BF16), dma, dma((14,))],
        compiler_params=pltpu.CompilerParams(vmem_limit_bytes=SCRATCH),
    )(made[0], *(pltpu.with_memory_space_constraint(one, pltpu.VMEM) for one in made[1:]))


def solution(mesh):
    def block_step(image, w_first, w_down, grad_out):
        made = block_call(image[0], grad_out[0], w_first.reshape(9, C, C), w_down.reshape(9, C, C))
        block_out, grad_image, grad_w_down, grad_w_first = settle(*made[:6])
        return (block_out.reshape(1, OUT_R, OUT_C, C), grad_image.reshape(1, ROWS, COLS, C),
                grad_w_first.reshape(3, 3, C, C), grad_w_down.reshape(3, 3, C, C))

    img_spec = P(None, 'h', 'w', None)
    return jax.shard_map(block_step, mesh=mesh, in_specs=(img_spec, P(), P(), img_spec), out_specs=(img_spec, img_spec, P(), P()), check_vma=False)
```

```python
import jax
import jax.numpy as jnp
from jax import lax
from jax.sharding import PartitionSpec as P
from jax.experimental import pallas as pl
from jax.experimental.pallas import tpu as pltpu

MESH = pl.DeviceIdType.MESH
F32, BF16 = jnp.float32, jnp.bfloat16
C = 640
ROWS, COLS = 24, 48
OUT_R, OUT_C = 12, 24
PIX, OPIX = ROWS * COLS, OUT_R * OUT_C
HALF = 320
MIB = 2 ** 20
SCRATCH = 36000000
ORDERS = (('x', 'y', 'z'), ('y', 'z', 'x'), ('z', 'x', 'y'))
R1, R2, R3, A1, A2, A3A, A3B, A3C, DA, DB, DC, DD = range(12)
QUARTER = HALF // 2
EIGHTH = QUARTER // 2
LEAST = EIGHTH // 2
LAND_AT = (0, QUARTER, QUARTER + EIGHTH)
LANES = range(C // 128)
TAPS = [(t, t // 3, t % 3) for t in range(9)]
THIRDS = range(3)


def gelu_tanh(values):
    return jax.nn.gelu(values, approximate=True)


def dot(lhs, rhs):
    return lax.dot_general(lhs, rhs, (((1,), (0,)), ((), ())), preferred_element_type=F32)


def dot_rhs_t(lhs, rhs):
    return lax.dot_general(lhs, rhs, (((1,), (1,)), ((), ())), preferred_element_type=F32)


def dot_lhs_t(lhs, rhs):
    return lax.dot_general(lhs, rhs, (((0,), (0,)), ((), ())), preferred_element_type=F32)


ANY = pl.BlockSpec(memory_space=pl.ANY)
VM = pl.BlockSpec(memory_space=pltpu.VMEM)


def place():
    w, h = lax.axis_index('w'), lax.axis_index('h')
    bit = {'x': h // 2, 'c': h % 2, 'y': w % 2, 'z': w // 2}
    dev = {'x': (w, (h + 2) % 4), 'c': (w, h + 1 - 2 * (h % 2)), 'y': (w + 1 - 2 * (w % 2), h), 'z': ((w + 2) % 4, h)}
    return bit, dev


class Reducer:
    def __init__(self, index, own, pair, sems, grants, bit, dev):
        self.index, self.own, self.pair, self.sems, self.grants, self.bit, self.dev = index, own, pair, sems, grants, bit, dev

    def starts(self, third):
        b = [self.bit[axis] for axis in ORDERS[third]]
        base2 = b[0] * QUARTER
        base3 = base2 + b[1] * EIGHTH
        return b, base2, base3, base3 + b[2] * LEAST

    def copy(self, third, kind):
        (b0, b1, b2), base2, base3, base4 = self.starts(third)
        axis0, axis1, axis2 = ORDERS[third]
        far = (1 - b0) * QUARTER
        near1, far1 = b1 * EIGHTH, (1 - b1) * EIGHTH
        src, size, axis = {
            R1: (far, QUARTER, axis0), R2: (base2 + far1, EIGHTH, axis1), R3: (base3 + (1 - b2) * LEAST, LEAST, axis2),
            A1: (base4, LEAST, axis2), A2: (base3, EIGHTH, axis1), A3A: (base3, EIGHTH, axis0), A3B: (base2 + far1, LEAST, axis0), A3C: (base2 + far1 + LEAST, LEAST, axis0),
            DA: (base2, QUARTER, 'c'), DB: (far + near1, EIGHTH, 'c'), DC: (far + far1, LEAST, 'c'), DD: (far + far1 + LEAST, LEAST, 'c'),
        }[kind]
        rows = pl.ds(pl.multiple_of(src, 8), size)
        units = pl.ds(3 * third, 3)
        source = self.own.at[units, rows]
        send, recv = (s.at[self.index, third, kind] for s in self.sems)
        if kind <= R3:
            target = self.pair.at[units, pl.ds(LAND_AT[kind], size)]
        elif kind <= A3C:
            target = source
        else:
            target = self.pair.at[units, rows]
        return pltpu.make_async_remote_copy(src_ref=source, dst_ref=target, send_sem=send, recv_sem=recv, device_id=self.dev[axis], device_id_type=MESH)

    def add(self, third, kind):
        _, base2, base3, base4 = self.starts(third)
        keep, size = ((base2, QUARTER), (base3, EIGHTH), (base4, LEAST))[kind]
        steps = size // LEAST

        def body(j):
            unit, row = 3 * third + j // steps, (j % steps) * LEAST
            rows = pl.ds(pl.multiple_of(keep + row, 8), LEAST)
            self.own[unit, rows, :] += self.pair[unit, pl.ds(pl.multiple_of(LAND_AT[kind] + row, 8), LEAST), :]
        run(3 * steps, body)

    def begin(self, *thirds):
        for third in thirds:
            self.copy(third, R1).start()

    def move(self, wait_for, then, add=False):
        for third in THIRDS:
            self.copy(third, wait_for).wait()
            if add:
                pl.semaphore_signal(self.grants.at[self.index, third, wait_for], inc=1, device_id=self.dev[ORDERS[third][wait_for]], device_id_type=MESH)
                self.add(third, wait_for)
            if wait_for == R3 and third == THIRDS[-1]:
                pl.semaphore_signal(self.grants.at[self.index, 0, 3], inc=1, device_id=self.dev['c'], device_id_type=MESH)
            for kind in then:
                if kind == DA and third == 0:
                    pl.semaphore_wait(self.grants.at[self.index, 0, 3], 1)
                if kind in (A1, A2, A3A):
                    pl.semaphore_wait(self.grants.at[self.index, third, {A1: R3, A2: R2, A3A: R1}[kind]], 1)
                self.copy(third, kind).start()

    def finish(self):
        for kind in (DA, DB, DC, DD):
            self.move(kind, ())


EDGE = 8
ALL_PARTS = ROW, COLUMN, CORNER = range(3)
LINES = (ROWS + 2) * COLS
BLOCK_ROWS = 6
BLOCK = BLOCK_ROWS * COLS
NEAR = [(dw, dh) for dw in (-1, 0, 1) for dh in (-1, 0, 1) if (dw, dh) != (0, 0)]
ABOVE = [(-1, -1), (-1, 0), (0, -1)]
BELOW = [(1, 1), (1, 0), (0, 1)]
G_AT, G_PAIR_AT, TAP_PAIR_AT = 3 * OPIX, 4 * OPIX, 5 * OPIX


def lane(k):
    return slice(k * 128, k * 128 + 128)


def run(steps, body):
    lax.fori_loop(0, steps, lambda i, _: body(i), None)


def clear_of(flag, value):
    return jnp.where(flag, 0.0, value)


def at(start, size):
    return pl.ds(pl.multiple_of(start, size), size)


class Border:
    def __init__(self, grid, row0, rows, cols, send, land, sems, send_to, take_from, row_sources=None):
        self.grid, self.row0, self.rows, self.cols, self.sends, self.lands = grid, row0, rows, cols, send, land
        self.sems, self.send_to, self.take_from, self.row_sources = sems, send_to, take_from, row_sources
        self.w, self.h = lax.axis_index('w'), lax.axis_index('h')

    def edge(self, step, first, size, outside):
        return {-1: first - outside, 1: first + size - 1 + outside}[step]

    def inside(self, dw, dh):
        w, h = self.w + dw, self.h + dh
        return jnp.logical_and(jnp.logical_and(w >= 0, w < 4), jnp.logical_and(h >= 0, h < 4))

    def copy(self, dw, dh):
        i, up, side = NEAR.index((dw, dh)), (dh + 1) // 2, (dw + 1) // 2
        if dw == 0:
            src = self.row_sources[up] if self.row_sources else self.sends[0].at[up]
            dst = self.lands[0].at[1 - up]
        elif dh == 0:
            src, dst = self.sends[1].at[side], self.lands[1].at[1 - side]
        else:
            src, dst = self.sends[2].at[2 * up + side], self.lands[2].at[2 * (1 - up) + 1 - side]
        peer = ((self.w + dw + 4) % 4, (self.h + dh + 4) % 4)
        return pltpu.make_async_remote_copy(src_ref=src, dst_ref=dst, send_sem=self.sems.at[0, i], recv_sem=self.sems.at[1, i], device_id=peer, device_id_type=MESH)

    def chosen(self, ways, parts):
        return [(dw, dh) for dw, dh in ways if (ROW if dw == 0 else COLUMN if dh == 0 else CORNER) in parts]

    def start(self, *parts):
        grid, row0, rows, cols = self.grid, self.row0, self.rows, self.cols
        for dw, dh in self.chosen(self.send_to, parts):
            up, side = (dh + 1) // 2, (dw + 1) // 2
            r = None if dh == 0 else self.edge(dh, row0, rows, 0)
            c = None if dw == 0 else self.edge(dw, EDGE, cols, 0)
            for k in LANES:
                if dw == 0:
                    if not self.row_sources:
                        self.sends[0][up, :, lane(k)] = grid[k, r, EDGE:EDGE + cols, :].astype(self.sends[0].dtype)
                elif dh == 0:
                    for row in range(rows):
                        self.sends[1][side, row:row + 1, lane(k)] = grid[k, row0 + row, c:c + 1, :]
                else:
                    self.sends[2][2 * up + side, :, lane(k)] = jnp.broadcast_to(grid[k, r, c:c + 1, :], (8, 128))

            @pl.when(self.inside(dw, dh))
            def _():
                self.copy(dw, dh).start()

    def finish(self, *parts):
        grid, row0, rows, cols = self.grid, self.row0, self.rows, self.cols
        for dw, dh in self.chosen(self.send_to, parts):
            @pl.when(self.inside(dw, dh))
            def _():
                self.copy(dw, dh).wait_send()

            @pl.when(self.inside(-dw, -dh))
            def _():
                self.copy(dw, dh).wait_recv()
        for dw, dh in self.chosen(self.take_from, parts):
            up, side = (dh + 1) // 2, (dw + 1) // 2
            r = None if dh == 0 else self.edge(dh, row0, rows, 1)
            c = None if dw == 0 else self.edge(dw, EDGE, cols, 1)
            out = jnp.logical_not(self.inside(dw, dh))
            for k in LANES:
                if dw == 0:
                    grid[k, r, EDGE:EDGE + cols, :] = clear_of(out, self.lands[0][up, :, lane(k)].astype(F32))
                elif dh == 0:
                    for row in range(rows):
                        grid[k, row0 + row, c:c + 1, :] = clear_of(out, self.lands[1][side, row:row + 1, lane(k)])
                else:
                    grid[k, r, c:c + 1, :] = clear_of(out, self.lands[2][2 * up + side, 0:1, lane(k)])


def spread(grid, xs):
    def one_row(r):
        for c in range(3):
            for k in LANES:
                xs[0, at(c * LINES + r * COLS, COLS), lane(k)] = grid[k, r, EDGE - 1 + c:EDGE - 1 + c + COLS, :].astype(BF16)
    run(ROWS + 2, one_row)


def accumulate(acc, rows, part, first):
    for k in LANES:
        piece = part[:, lane(k)]
        acc[k, 0:rows, :] = piece if first else acc[k, 0:rows, :] + piece


def block_kernel(x_in, g_in, w_first, w_down, y_out, da_pair, own_d, own_f, other_d, other_f, x_land,
                 wbuf, xs, taps, g_tile, g_grid, da, grid, acc,
                 send_r, send_c, send_k, x_r, x_c, x_k, z_r, z_c, z_k, d_r, d_c, d_k, gs_r, gs_c, gs_k, gl_r, gl_c, gl_k,
                 load_sems, pair_sems, near_sems, out_sems, send_sems, recv_sems, grants):
    bit, dev = place()
    w, h = lax.axis_index('w'), lax.axis_index('h')
    core = bit['c']
    x_tile = xs.at[0, pl.ds(0, PIX)]
    load_x = pltpu.make_async_copy(x_in, x_tile, load_sems.at[0])
    load_g = pltpu.make_async_copy(g_in, g_tile, load_sems.at[1])
    load_w = pltpu.make_async_copy(w_first, wbuf, load_sems.at[2])
    for load in (load_x, load_g, load_w):
        load.start()
    barrier = pltpu.get_barrier_semaphore()
    for axis in 'xyzc':
        pl.semaphore_signal(barrier, inc=1, device_id=dev[axis], device_id_type=MESH)
    for dw, dh in NEAR:
        pl.semaphore_signal(barrier, inc=1, device_id=((w + dw + 4) % 4, (h + dh + 4) % 4), device_id_type=MESH)
    sends = (send_r, send_c, send_k)
    x_border = Border(grid, 1, ROWS, COLS, sends, (x_r, x_c, x_k), near_sems.at[0], NEAR, NEAR,
                      [x_tile.at[pl.ds(0, COLS)], x_tile.at[pl.ds(PIX - COLS, COLS)]])
    z_border = Border(grid, 0, ROWS, COLS, sends, (z_r, z_c, z_k), near_sems.at[1], ABOVE, BELOW)
    d_border = Border(grid, 1, ROWS, COLS, sends, (d_r, d_c, d_k), near_sems.at[2], NEAR, NEAR)
    g_border = Border(g_grid, 1, OUT_R, OUT_C, (gs_r, gs_c, gs_k), (gl_r, gl_c, gl_k), near_sems.at[3], BELOW, ABOVE)
    sems = (send_sems, recv_sems)
    down = Reducer(0, own_d, other_d, sems, grants, bit, dev)
    first = Reducer(1, own_f, other_f, sems, grants, bit, dev)

    def to_pair(src, dst, i):
        return pltpu.make_async_remote_copy(src_ref=src, dst_ref=dst, send_sem=pair_sems.at[0, i], recv_sem=pair_sems.at[1, i], device_id=dev['c'], device_id_type=MESH)

    def put(own, j, res, more):
        for side in range(2):
            unit = 2 * j + side - core
            part = res[side * HALF:(side + 1) * HALF]

            @pl.when(jnp.logical_and(unit >= 0, unit < 9))
            def _():
                own[unit] = own[unit] + part if more else part

    load_x.wait()
    pl.semaphore_wait(barrier, 12)
    x_border.start(ROW)

    def place_row(r):
        for k in LANES:
            grid[k, r + 1, EDGE:EDGE + COLS, :] = x_tile[at(r * COLS, COLS), lane(k)].astype(F32)
    run(ROWS, place_row)
    x_border.start(COLUMN, CORNER)
    load_g.wait()
    for r in range(OUT_R):
        for k in LANES:
            g_grid[k, r + 1, EDGE:EDGE + OUT_C, :] = g_tile[r, :, lane(k)].astype(F32)
    g_border.start(*ALL_PARTS)
    x_border.finish(*ALL_PARTS)
    spread(grid, xs)
    x_share = to_pair(xs.at[0], x_land, 0)
    x_share.start()
    load_w.wait()

    def pre_rows(i):
        for t, a, c in TAPS:
            rows = pl.ds(pl.multiple_of(c * LINES + i * BLOCK + a * COLS, COLS), BLOCK)
            accumulate(acc, BLOCK, dot(xs[0, rows, :], wbuf[t]), t == 0)
        for k in LANES:
            pre = acc[k].astype(BF16).astype(F32)
            acc[k] = pre
            act = gelu_tanh(pre).astype(BF16).astype(F32)
            for r in range(BLOCK_ROWS):
                grid[k, BLOCK_ROWS * i + r, EDGE:EDGE + COLS, :] = act[r * COLS:(r + 1) * COLS]
        for r in range(BLOCK_ROWS):
            for cp in range(2):
                for k in LANES:
                    own_f[2 * (r % 2) + cp, pl.ds(pl.multiple_of((BLOCK_ROWS // 2 * i + r // 2) * OUT_C, 8), OUT_C), lane(k)] = acc[k, pl.ds(r * COLS + cp, OUT_C, stride=2), :]
    pre_rows(0)
    z_border.start(ROW, CORNER)
    run(ROWS // BLOCK_ROWS - 1, lambda i: pre_rows(i + 1))
    z_border.start(COLUMN)
    load_w2 = pltpu.make_async_copy(w_down, wbuf, load_sems.at[3])
    load_w2.start()

    g_border.finish(*ALL_PARTS)
    for di in range(2):
        for dj in range(2):
            for k in LANES:
                part = g_grid[k, di:di + OUT_R, EDGE - 1 + dj:EDGE - 1 + dj + OUT_C, :]
                xs[1, (2 * di + dj) * OPIX:(2 * di + dj + 1) * OPIX, lane(k)] = part.reshape(OPIX, 128).astype(BF16)
    g_share = to_pair(xs.at[1, pl.ds(G_AT, OPIX)], xs.at[1, pl.ds(G_PAIR_AT, OPIX)], 1)
    g_share.start()

    def tap_rows(p, columns):
        for t, a, c in TAPS:
            if c in columns:
                for k in LANES:
                    cols = pl.ds(EDGE + c, OUT_C, stride=2)
                    two = jnp.concatenate([grid[k, 4 * p + a, cols, :], grid[k, 4 * p + 2 + a, cols, :]], 0)
                    taps[t, at(p * 2 * OUT_C, 2 * OUT_C), lane(k)] = two.astype(BF16)

    def early(n, core):
        return n + n // 2 + core * (n % 2)

    def late(n, core):
        return 4 - 2 * n + core * (5 * n - 3)

    def share_tap(j, i):
        rows = pl.ds(pl.multiple_of(TAP_PAIR_AT + j * OPIX, 32), OPIX)
        share = to_pair(taps.at[4 * (1 - core) + j], xs.at[1, rows], 2 + i)
        share.start()
        return share

    def down_tap(j):
        put(own_d, j, dot_lhs_t(taps[4 * core + j], xs[1, G_AT:G_AT + OPIX, :]), False)

    z_border.finish(ROW)
    run(OUT_R // 2, lambda p: tap_rows(p, (0, 1)))
    tap_shares = [share_tap(early(n, 1 - core), n) for n in range(3)]
    for n in range(3):
        down_tap(early(n, core))
    z_border.finish(COLUMN, CORNER)
    run(OUT_R // 2, lambda p: tap_rows(p, (2,)))
    tap_shares += [share_tap(late(n, 1 - core), 3 + n) for n in range(2)]
    for n in range(2):
        down_tap(late(n, core))
    g_share.wait()
    for share in tap_shares:
        share.wait()

    def down_tap_pair(j):
        rows = pl.ds(TAP_PAIR_AT + j * OPIX, OPIX)
        res = dot_lhs_t(xs[1, rows, :], xs[1, G_PAIR_AT:G_PAIR_AT + OPIX, :])
        put(own_d, j, res, True)
    for j in range(5):
        down_tap_pair(j)
        down.begin(*{1: (0,), 3: (1,), 4: (2,)}.get(j, ()))

    load_w2.wait()
    for rp in range(2):
        for cp in range(2):
            total = None
            for a in ((0, 2), (1,))[rp]:
                for c in ((0, 2), (1,))[cp]:
                    row = (2 * (1 - a // 2) + 1 - c // 2) * OPIX
                    part = dot_rhs_t(xs[1, row:row + OPIX, :], wbuf[3 * a + c])
                    total = part if total is None else total + part
            pre = own_f[2 * rp + cp, 0:OPIX, :]
            grad = jax.vjp(gelu_tanh, pre)[1](total)[0].astype(BF16).astype(F32)
            for i in range(OUT_R):
                for k in LANES:
                    grid[k, 2 * i + rp + 1, pl.ds(EDGE + cp, OUT_C, stride=2), :] = grad[i * OUT_C:(i + 1) * OUT_C, lane(k)]

    def pack(r):
        for k in LANES:
            da[at(r * COLS, COLS), lane(k)] = grid[k, r + 1, EDGE:EDGE + COLS, :].astype(BF16)
    run(ROWS, pack)
    da_share = to_pair(da, da_pair, 7)
    da_share.start()
    d_border.start(*ALL_PARTS)
    x_share.wait()
    pair_load = pltpu.make_async_copy(x_land, xs.at[1], load_sems.at[4])
    pair_load.start()

    for t in range(9):
        accumulate(acc, OPIX, dot(taps[t], wbuf[t]), t == 0)
    for k in LANES:
        taps[0, :, lane(k)] = acc[k, 0:OPIX, :].astype(BF16)
    y_copy = pltpu.make_async_copy(taps.at[0], y_out, out_sems.at[0])
    y_copy.start()
    load_w1 = pltpu.make_async_copy(w_first, wbuf, load_sems.at[5])
    load_w1.start()
    pair_load.wait()
    da_share.wait()

    def first_tap(j):
        t = 4 * core + j
        a, c = t // 3, t % 3
        rows = pl.ds(pl.multiple_of(c * LINES + a * COLS, COLS), PIX)
        res = dot_lhs_t(xs[0, rows, :], da[...]) + dot_lhs_t(xs[1, rows, :], da_pair[...])
        put(own_f, j, res, False)
    run(4, first_tap)
    down.move(R1, (R2,), add=True)
    first_tap(4)
    first.begin(*THIRDS)

    d_border.finish(*ALL_PARTS)
    spread(grid, xs)
    load_w1.wait()

    def image_rows(i):
        for t, a, c in TAPS:
            rows = pl.ds(pl.multiple_of((2 - c) * LINES + i * BLOCK + (2 - a) * COLS, COLS), BLOCK)
            accumulate(acc, BLOCK, dot_rhs_t(xs[0, rows, :], wbuf[t]), t == 0)
        for k in LANES:
            da_pair[at(i * BLOCK, BLOCK), lane(k)] = acc[k].astype(BF16)
    run(ROWS // BLOCK_ROWS, image_rows)

    down.move(R2, (R3,), add=True)
    first.move(R1, (R2,), add=True)
    down.move(R3, (A1,), add=True)
    first.move(R2, (R3,), add=True)
    down.move(A1, (A2, A3A))
    first.move(R3, (A1,), add=True)
    down.move(A2, (A3B, A3C, DA))
    first.move(A1, (A2, A3A))
    down.move(A3A, (DB,))
    first.move(A2, (A3B, A3C, DA))
    down.move(A3B, (DC,))
    down.move(A3C, (DD,))
    first.move(A3A, (DB,))
    first.move(A3B, (DC,))
    first.move(A3C, (DD,))
    y_copy.wait()
    down.finish()
    first.finish()


def block_call(image, grad_out, w_first, w_down):
    kept = pltpu.VMEM((9, HALF, C), F32)
    dma = pltpu.SemaphoreType.DMA
    edges = [pltpu.VMEM((2, COLS, C), BF16), pltpu.VMEM((2, ROWS, C), F32), pltpu.VMEM((4, 8, C), F32)]
    small = [pltpu.VMEM((2, OUT_C, C), F32), pltpu.VMEM((2, OUT_R, C), F32), pltpu.VMEM((4, 8, C), F32)]
    return pl.pallas_call(
        block_kernel,
        out_shape=[jax.ShapeDtypeStruct((OPIX, C), BF16), pltpu.VMEM((PIX, C), BF16), kept, kept, kept, kept,
                   jax.ShapeDtypeStruct((3 * LINES, C), BF16)],
        in_specs=[ANY] * 4, out_specs=[ANY] + [VM] * 5 + [ANY],
        scratch_shapes=[pltpu.VMEM((9, C, C), BF16), pltpu.VMEM((2, 3 * LINES, C), BF16), pltpu.VMEM((9, OPIX, C), BF16)]
        + [pltpu.VMEM((OUT_R, OUT_C, C), BF16), pltpu.VMEM((5, OUT_R + 1, OUT_C + EDGE, 128), F32)]
        + [pltpu.VMEM((PIX, C), BF16)]
        + [pltpu.VMEM((5, ROWS + 2, COLS + 2 * EDGE, 128), F32), pltpu.VMEM((5, BLOCK, 128), F32)]
        + edges * 4 + small * 2
        + [dma((6,)), dma((2, 8)), dma((4, 2, 8)), dma((2,)), dma((2, 3, 12)), dma((2, 3, 12)), pltpu.SemaphoreType.REGULAR((2, 3, 4))],
        compiler_params=pltpu.CompilerParams(collective_id=1, has_side_effects=True, vmem_limit_bytes=SCRATCH),
        cost_estimate=pl.CostEstimate(flops=2 * PIX * 90 * C * C, bytes_accessed=64 * MIB, transcendentals=0),
    )(image.reshape(PIX, C), grad_out, w_first, w_down)


def settle_kernel(y_in, dx_in, own_d, own_f, other_d, other_f, y_out, dx_out, down_out, first_out, y_buf, load_sem, sems):
    core = lax.axis_index('h') % 2
    load = pltpu.make_async_copy(y_in, y_buf, load_sem)
    load.start()
    pieces = [(dx_in, dx_out)]
    for own, other, out in ((own_d, other_d, down_out), (own_f, other_f, first_out)):
        for part in THIRDS:
            for side, src in ((core, own), (1 - core, other)):
                pieces.append((src.at[pl.ds(3 * part, 3)], out.at[pl.ds(9 * side + 3 * part, 3)]))
    copies = [pltpu.make_async_copy(src, dst, sems.at[i]) for i, (src, dst) in enumerate(pieces)]
    for copy in copies:
        copy.start()
    load.wait()
    last = pltpu.make_async_copy(y_buf, y_out, sems.at[len(copies)])
    last.start()
    for copy in copies + [last]:
        copy.wait()


def settle(*made):
    total = jax.ShapeDtypeStruct((18, HALF, C), F32)
    dma = pltpu.SemaphoreType.DMA
    return pl.pallas_call(
        settle_kernel, out_shape=[jax.ShapeDtypeStruct((OPIX, C), BF16), jax.ShapeDtypeStruct((PIX, C), BF16), total, total],
        in_specs=[pl.BlockSpec(memory_space=pltpu.HBM)] + [VM] * 5, out_specs=[ANY] * 4,
        scratch_shapes=[pltpu.VMEM((OPIX, C), BF16), dma, dma((14,))],
        compiler_params=pltpu.CompilerParams(vmem_limit_bytes=SCRATCH),
    )(made[0], *(pltpu.with_memory_space_constraint(one, pltpu.VMEM) for one in made[1:]))


def solution(mesh):
    def block_step(image, w_first, w_down, grad_out):
        made = block_call(image[0], grad_out[0], w_first.reshape(9, C, C), w_down.reshape(9, C, C))
        block_out, grad_image, grad_w_down, grad_w_first = settle(*made[:6])
        return (block_out.reshape(1, OUT_R, OUT_C, C), grad_image.reshape(1, ROWS, COLS, C),
                grad_w_first.reshape(3, 3, C, C), grad_w_down.reshape(3, 3, C, C))

    img_spec = P(None, 'h', 'w', None)
    return jax.shard_map(block_step, mesh=mesh, in_specs=(img_spec, P(), P(), img_spec), out_specs=(img_spec, img_spec, P(), P()), check_vma=False)
```
